8 devices in a mesh: data: 8 (over z, y, x, core).
Axes of the slice: x: 2, y: 2, z: 1, core: 2. Of those that a mesh axis runs over, the one named last changes fastest.
Arguments:
- z_one: bfloat16 [512, 256], P('data')
- z_two: bfloat16 [512, 256], P('data')
- z_small: bfloat16 [10, 512, 256], P(None, 'data')
- protos: bfloat16 [8192, 256], replicated
- live_mask: int32 [512], P('data')
Outputs:
- output 1: float32 [512, 8192], P('data')
- output 2: float32 [512, 8192], P('data')
- output 3: float32 [], replicated
- output 4: float32 [512, 256], P('data')
- output 5: float32 [512, 256], P('data')
- output 6: float32 [10, 512, 256], P(None, 'data')
- output 7: float32 [8192, 256], replicated
All inputs are finite; a program needn't handle non-finite values.
Results may differ from the reference program's by a relative error of at most 0.001.
Values are sent between devices in bfloat16 or wider.
A program may use at most 1 GiB of HBM per device.

```python
import jax
import jax.numpy as jnp
from jax import lax

ROWS_DEV = 64
NUM_GROUPS = 8
NUM_PROTOS = 8192
EMBED_DIM = 256
SMALL_CROPS = 10
ITERS = 3
NUM_ROWS = ROWS_DEV * NUM_GROUPS
EPS = 0.05
TAU = 0.1


def unit_rows(matrix):
    return matrix / jnp.sqrt(jnp.sum(matrix * matrix, axis=-1, keepdims=True))


def draw_mask(mask_key):
    k_count, k_full, k_one, k_perm = jax.random.split(mask_key, 4)
    counts = jax.random.randint(k_count, (NUM_GROUPS,), 1, ROWS_DEV + 1)
    full_grp = jax.random.randint(k_full, (), 0, NUM_GROUPS)
    one_grp = (full_grp + jax.random.randint(k_one, (), 1, NUM_GROUPS)) % NUM_GROUPS
    groups = jnp.arange(NUM_GROUPS)
    counts = jnp.where(groups == full_grp, ROWS_DEV, counts)
    counts = jnp.where(groups == one_grp, 1, counts)
    perm_keys = jax.random.split(k_perm, NUM_GROUPS)
    rank_vals = jax.vmap(lambda perm_key: jax.random.permutation(perm_key, ROWS_DEV))(perm_keys)
    return (rank_vals < counts[:, None]).astype(jnp.int32).reshape(NUM_ROWS)


def draw_views(view_key, protos_f):
    k_pick, k_noise = jax.random.split(view_key)
    win_width = max(NUM_PROTOS // 2, 1)
    offsets = jax.random.randint(k_pick, (NUM_ROWS,), 0, win_width)
    win_start = (jnp.arange(NUM_ROWS) // ROWS_DEV) * NUM_PROTOS // NUM_GROUPS
    pick_ids = (win_start + offsets) % NUM_PROTOS
    centers = protos_f[pick_ids]
    noise_vals = jax.random.normal(k_noise, (2 + SMALL_CROPS, NUM_ROWS, EMBED_DIM), jnp.float32)
    mixed = 0.6 * centers[None] + 0.8 * noise_vals * EMBED_DIM ** -0.5
    return unit_rows(mixed).astype(jnp.bfloat16)


def setup_inputs(seed: int = 0) -> dict:
    root_key = jax.random.key(seed)
    k_proto, k_views, k_mask = jax.random.split(root_key, 3)
    protos_f = unit_rows(jax.random.normal(k_proto, (NUM_PROTOS, EMBED_DIM), jnp.float32))
    crops_all = draw_views(k_views, protos_f)
    return {"z_one": crops_all[0], "z_two": crops_all[1], "z_small": crops_all[2:], "protos": protos_f.astype(jnp.bfloat16), "live_mask": draw_mask(k_mask)}


def sinkhorn(scores, live_f, live_total):
    live_col = live_f[:, None]

    def sk_step(weights, unused):
        col_sum = jnp.sum(weights, axis=0)
        weights = weights / (NUM_PROTOS * col_sum)
        row_sum = jnp.sum(weights, axis=1, keepdims=True)
        row_safe = jnp.where(live_col > 0, row_sum, 1.0)
        weights = weights * (live_col / (live_total * row_safe))
        return weights, None

    weights = lax.scan(sk_step, live_col * jnp.exp(scores / EPS), None, length=ITERS)[0]
    return live_total * weights


def reference(z_one, z_two, z_small, protos, live_mask):
    live_f = live_mask.astype(jnp.float32)
    live_col = live_f[:, None]
    live_total = jnp.sum(live_f)
    pair_count = 2 + 2 * SMALL_CROPS
    grad_scale = 1.0 / (TAU * live_total * pair_count)
    scores_one = jnp.dot(z_one, protos.T, preferred_element_type=jnp.float32)
    scores_two = jnp.dot(z_two, protos.T, preferred_element_type=jnp.float32)
    q_one = sinkhorn(scores_one, live_f, live_total)
    q_two = sinkhorn(scores_two, live_f, live_total)
    q_sum = q_one + q_two
    logp_one = jax.nn.log_softmax(scores_one / TAU, axis=-1)
    logp_two = jax.nn.log_softmax(scores_two / TAU, axis=-1)
    grad_one = ((live_col * jnp.exp(logp_one) - q_two) * grad_scale).astype(jnp.bfloat16)
    grad_two = ((live_col * jnp.exp(logp_two) - q_one) * grad_scale).astype(jnp.bfloat16)

    def small_view(z_crop):
        scores = jnp.dot(z_crop, protos.T, preferred_element_type=jnp.float32)
        logp_crop = jax.nn.log_softmax(scores / TAU, axis=-1)
        grad_crop = ((2.0 * live_col * jnp.exp(logp_crop) - q_sum) * grad_scale).astype(jnp.bfloat16)
        return (jnp.sum(q_sum * logp_crop), jnp.dot(grad_crop, protos, preferred_element_type=jnp.float32), jnp.dot(grad_crop.T, z_crop, preferred_element_type=jnp.float32))

    small_cross, dz_small, small_dc = lax.map(small_view, z_small)
    cross_sum = jnp.sum(q_two * logp_one) + jnp.sum(q_one * logp_two) + jnp.sum(small_cross)
    loss_total = -cross_sum / (live_total * pair_count)
    dz_one = jnp.dot(grad_one, protos, preferred_element_type=jnp.float32)
    dz_two = jnp.dot(grad_two, protos, preferred_element_type=jnp.float32)
    d_protos = jnp.dot(grad_one.T, z_one, preferred_element_type=jnp.float32) + jnp.dot(grad_two.T, z_two, preferred_element_type=jnp.float32) + jnp.sum(small_dc, axis=0)
    return (q_one, q_two, loss_total, dz_one, dz_two, dz_small, d_protos)
```

```python
import functools
import math

import jax
import jax.numpy as jnp
from jax import lax
from jax.experimental import pallas as pl
from jax.experimental.pallas import tpu as pltpu
from jax.sharding import PartitionSpec as P

EPS = 0.05
TAU = 0.1
ITERS = 3
DEVS = 8
ROWS = 64
NROW = ROWS * DEVS
PROTOS = 8192
DIM = 256
VIEWS = 12
OWN = PROTOS // DEVS
KC = 256
NCH = OWN // KC
PC = 512
MESH = pl.DeviceIdType.MESH
F32 = jnp.float32
BF16 = jnp.bfloat16
UNITS = ((0, 1), (1, 1), (2, 4), (6, 3), (9, 3))


def nt_dot(a, b):
    return lax.dot_general(a, b, (((1,), (1,)), ((), ())), preferred_element_type=F32)


def body(mask_ref, z1_ref, z2_ref, zs_ref, c_hbm,
         q1_hbm, q2_hbm, loss_ref, dz1_ref, dz2_ref, dzs_ref, dc_hbm,
         zall, zown, cv, et, a0, gq, gt, dcv, qbuf, vb, vx, rx, lx, mx, px,
         mvec, wvec, acf, cf, ct, ab, ssum_ref, dzacc,
         csem, zsend, zrecv, rsend, rrecv, lsend, lrecv, vsend, vrecv, psend, precv,
         asend, arecv, qsem, osem):
    me = lax.axis_index("data")
    core = me % 2
    xpos = (me // 2) % 2
    ypos = me // 4
    partner = me + 1 - 2 * core
    xn = me + 2 - 4 * xpos
    yn = me + 4 - 8 * ypos
    dg = xn + 4 - 8 * ypos

    def other(d):
        return d + 1 - 2 * core

    own0 = pl.multiple_of(me * OWN, OWN)
    c_own_copy = pltpu.make_async_copy(c_hbm.at[pl.ds(own0, OWN)], cv.at[pl.ds(own0, OWN)], csem.at[0])
    c_own_copy.start()

    barrier = pltpu.get_barrier_semaphore()
    for off in range(1, DEVS):
        pl.semaphore_signal(barrier, inc=1, device_id=((me + off) % DEVS,), device_id_type=MESH)

    mrow = mask_ref[...].astype(F32)
    sel = (lax.broadcasted_iota(jnp.int32, (ROWS, 128), 1)
           == lax.broadcasted_iota(jnp.int32, (ROWS, 128), 0) + ROWS * core)
    mplaced = jnp.dot(jnp.broadcast_to(mrow, (8, ROWS)).astype(BF16), sel.astype(BF16),
                      preferred_element_type=F32)
    mx[me] = mplaced[0:1, :]

    def zdst(unit, dev):
        lo, cnt = UNITS[unit]
        rows = pl.ds(pl.multiple_of(dev * ROWS, ROWS), ROWS)
        if cnt == 1:
            return zall.at[lo, rows]
        return zall.at[pl.ds(lo, cnt), rows]

    def zsrc(unit):
        lo, cnt = UNITS[unit]
        if unit == 0:
            return z1_ref
        if unit == 1:
            return z2_ref
        return zs_ref.at[pl.ds(lo - 2, cnt)]

    peers = (partner, xn, yn, dg)

    def zcopy(unit, kind):
        if kind < 4:
            return pltpu.make_async_remote_copy(
                src_ref=zsrc(unit), dst_ref=zdst(unit, me), send_sem=zsend.at[kind, unit],
                recv_sem=zrecv.at[kind, unit], device_id=(peers[kind],), device_id_type=MESH)
        dev = peers[kind - 3]
        return pltpu.make_async_remote_copy(
            src_ref=zdst(unit, dev), dst_ref=zdst(unit, dev), send_sem=zsend.at[kind, unit],
            recv_sem=zrecv.at[kind, unit], device_id=(partner,), device_id_type=MESH)

    def zwait(unit, kind):
        dev = peers[kind] if kind < 4 else other(peers[kind - 3])
        pltpu.make_async_remote_copy(
            src_ref=zsrc(unit), dst_ref=zdst(unit, dev), send_sem=zsend.at[kind, unit],
            recv_sem=zrecv.at[kind, unit], device_id=(partner,), device_id_type=MESH).wait_recv()

    def zstart(unit):
        for kind in (1, 2, 3, 0):
            zcopy(unit, kind).start()

    def zforward(units):
        for kind in (1, 2, 3):
            for unit in units:
                zwait(unit, kind)
                zcopy(unit, kind + 3).start()

    def zfinish(units):
        for unit in units:
            zwait(unit, 0)
        for kind in (4, 5, 6):
            for unit in units:
                zwait(unit, kind)

    def bcast(ref_of, send_sem, recv_sem, wait):
        for off in range(1, DEVS):
            dev = (me + off) % DEVS
            slot = dev if wait else me
            copy = pltpu.make_async_remote_copy(
                src_ref=ref_of(slot), dst_ref=ref_of(slot), send_sem=send_sem(off),
                recv_sem=recv_sem(slot), device_id=(dev,), device_id_type=MESH)
            if wait:
                copy.wait_recv()
            else:
                copy.start()

    def bcast_drain(ref_of, send_sem, recv_sem):
        for off in range(1, DEVS):
            pltpu.make_async_remote_copy(
                src_ref=ref_of(me), dst_ref=ref_of(me), send_sem=send_sem(off),
                recv_sem=recv_sem(me), device_id=((me + off) % DEVS,), device_id_type=MESH).wait_send()

    m_args = (lambda d: mx.at[d], lambda o: psend.at[1, o], lambda d: precv.at[1, d])
    p_args = (lambda d: px.at[d], lambda o: psend.at[0, o], lambda d: precv.at[0, d])
    v_args = (lambda d: vx.at[d], lambda o: vsend.at[o], lambda d: vrecv.at[d])

    def r_args(step):
        return (lambda d: rx.at[step, d], lambda o: rsend.at[step, o], lambda d: rrecv.at[step, d])

    def l_args(part):
        lo, cnt = ((0, 6), (6, 6))[part]
        return (lambda d: lx.at[d, pl.ds(lo, cnt)], lambda o: lsend.at[part, o], lambda d: lrecv.at[part, d])

    my_rows = pl.ds(pl.multiple_of(me * ROWS, ROWS), ROWS)
    zall[0, my_rows] = z1_ref[...]
    zall[1, my_rows] = z2_ref[...]
    zown[0] = z1_ref[...]
    zown[1] = z2_ref[...]
    for view in range(VIEWS - 2):
        zall[2 + view, my_rows] = zs_ref[view]
        zown[2 + view] = zs_ref[view]

    pl.semaphore_wait(barrier, DEVS - 1)
    zstart(0)
    zstart(1)
    bcast(*m_args, wait=False)
    zstart(2)

    c_copies = []
    for off in range(1, DEVS):
        lo = pl.multiple_of(((me + off) % DEVS) * OWN, OWN)
        c_copies.append(pltpu.make_async_copy(c_hbm.at[pl.ds(lo, OWN)], cv.at[pl.ds(lo, OWN)], csem.at[off]))
        c_copies[-1].start()
    c_own_copy.wait()

    def exp_block(view, ch):
        rows = pl.ds(pl.multiple_of(ch * KC, KC), KC)
        scores = nt_dot(cv[pl.ds(pl.multiple_of(own0 + ch * KC, KC), KC)], zall[view])
        e = jnp.exp(scores * (1.0 / TAU))
        et[view, rows] = e
        return rows, e

    def fold(x):
        return jnp.sum(x.reshape(x.shape[0] // 8, 8, x.shape[1]), axis=0)

    def exp_view(view):
        def step(ch, acc):
            _, e = exp_block(view, ch)
            return acc + fold(e)
        acc = lax.fori_loop(0, NCH, step, jnp.zeros((8, NROW), F32))
        lx[me, view] = jnp.sum(acc, axis=0, keepdims=True)

    def exp_views(lo, hi):
        def step(view, carry):
            exp_view(view)
            return carry
        lax.fori_loop(lo, hi, step, 0)

    zforward((0, 1))
    bcast(*m_args, wait=True)
    zfinish((0, 1))
    for q in range(NROW // 128):
        mvec[:, q * 128:(q + 1) * 128] = mx[2 * q] + mx[2 * q + 1]
    live_total = jnp.sum(mvec[...], axis=1, keepdims=True)

    SB = 64

    for view in range(2):
        def step(ch, acc):
            rows, e = exp_block(view, ch)
            a0[view, rows] = e * e
            return acc + fold(e)
        acc = lax.fori_loop(0, NCH, step, jnp.zeros((8, NROW), F32))
        lx[me, view] = jnp.sum(acc, axis=0, keepdims=True)

    def sink_pass(it):
        for view in range(2):
            scale = (1.0 if it == 0 else live_total) * (1.0 / PROTOS)

            def step(blk, acc):
                rows = pl.ds(pl.multiple_of(blk * SB, SB), SB)
                a = a0[view, rows]
                w = mvec[...] if it == 0 else wvec[view]
                colsum = jnp.sum(a * w, axis=1, keepdims=True)
                v = scale / colsum
                if it == ITERS - 1:
                    vb[view, rows] = jnp.broadcast_to(v, (SB, 128))
                return acc + fold(a * v)
            acc = lax.fori_loop(0, OWN // SB, step, jnp.zeros((8, NROW), F32))
            rx[it, me, :, view * NROW:(view + 1) * NROW] = jnp.sum(acc, axis=0, keepdims=True)
        bcast(*r_args(it), wait=False)

    def sink_close(it):
        bcast(*r_args(it), wait=True)
        tot = rx[it, 0]
        for d in range(1, DEVS):
            tot = tot + rx[it, d]
        for view in range(2):
            wvec[view] = mvec[...] / tot[:, view * NROW:(view + 1) * NROW]

    sink_pass(0)
    zstart(3)
    zforward((2,))
    zfinish((2,))
    exp_views(2, 6)
    bcast(*l_args(0), wait=False)
    sink_close(0)
    sink_pass(1)
    zstart(4)
    zforward((3,))
    zfinish((3,))
    exp_views(6, 9)
    sink_close(1)
    sink_pass(2)
    zforward((4,))
    zfinish((4,))
    exp_views(9, 12)
    bcast(*l_args(1), wait=False)

    for view in range(2):
        for blk in range(OWN // 128):
            vt = vb[view, blk * 128:(blk + 1) * 128].T
            vx[me, view, :, blk * 128:(blk + 1) * 128] = vt[0:1, :]
    bcast(*v_args, wait=False)

    sink_close(2)
    bcast(*l_args(0), wait=True)
    bcast(*l_args(1), wait=True)
    grad_scale = 1.0 / (TAU * live_total * (2 + 2 * (VIEWS - 2)))
    log_sum = jnp.zeros((1, NROW), F32)
    for view in range(VIEWS):
        tot = lx[0, view]
        for d in range(1, DEVS):
            tot = tot + lx[d, view]
        mult = 1.0 if view < 2 else 2.0
        acf[view] = (mult * grad_scale) * mvec[...] / tot
        log_sum = log_sum + mult * jnp.log(tot)
    log_sum = jnp.sum(log_sum * mvec[...], axis=1, keepdims=True)

    def acopy(src_dev, ch, half, to, kind):
        lo = src_dev * OWN + ch * KC
        if half is None:
            rows = pl.ds(pl.multiple_of(lo, KC), KC)
        else:
            rows = pl.ds(pl.multiple_of(lo + half * (KC // 2), KC // 2), KC // 2)
        return pltpu.make_async_remote_copy(
            src_ref=dcv.at[rows], dst_ref=dcv.at[rows], send_sem=asend.at[kind, ch],
            recv_sem=arecv.at[kind, ch], device_id=(to,), device_id_type=MESH)

    def dc_chunk(ch, carry):
        rows = pl.ds(pl.multiple_of(ch * KC, KC), KC)
        for view in range(2):
            v = vb[view, rows]
            v = jnp.concatenate([v] * (NROW // 128), axis=1)
            gq[view] = (wvec[view] * grad_scale) * (v * a0[view, rows])
        gq[2] = gq[0] + gq[1]
        g0 = (acf[0] * et[0, rows] - gq[1]).astype(BF16)
        acc = jnp.dot(g0, zall[0], preferred_element_type=F32)
        g1 = (acf[1] * et[1, rows] - gq[0]).astype(BF16)
        acc = acc + jnp.dot(g1, zall[1], preferred_element_type=F32)

        def step(view, acc):
            g = (acf[view] * et[view, rows] - gq[2]).astype(BF16)
            return acc + jnp.dot(g, zall[view], preferred_element_type=F32)
        acc = lax.fori_loop(2, VIEWS, step, acc)
        dcv[pl.ds(pl.multiple_of(own0 + ch * KC, KC), KC)] = acc
        for kind, to in ((0, xn), (1, yn), (2, partner)):
            acopy(me, ch, None, to, kind).start()
        return carry
    lax.fori_loop(0, NCH, dc_chunk, 0)

    lanes = pl.ds(pl.multiple_of((me // 2) * 128, 128), 128)
    for view in range(VIEWS):
        cf[view:view + 1, :] = acf[view, :, lanes]
    for view in range(2):
        cf[VIEWS + view:VIEWS + view + 1, :] = wvec[view, :, lanes]
    ct[...] = cf[...].T
    own_cf = ct[pl.ds(pl.multiple_of(core * ROWS, ROWS), ROWS), :]
    for j in range(VIEWS + 2):
        ab[j] = jnp.broadcast_to(own_cf[:, j:j + 1], (ROWS, 128))

    for copy in c_copies:
        copy.wait()
    bcast(*v_args, wait=True)
    dzacc[...] = jnp.zeros_like(dzacc)

    def wide(x):
        return jnp.concatenate([x] * (PC // 128), axis=1)

    def qcopy(view, ch, slot):
        cols = pl.ds(pl.multiple_of(ch * PC, PC), PC)
        return pltpu.make_async_copy(qbuf.at[slot, view], (q1_hbm, q2_hbm)[view].at[:, cols], qsem.at[slot, view])

    def row_chunk(ch, acc):
        slot = ch % 2

        @pl.when(ch >= 2)
        def _():
            for view in range(2):
                qcopy(view, ch - 2, slot).wait()
        cc = cv[pl.ds(pl.multiple_of(ch * PC, PC), PC)]
        scores = nt_dot(zown[...].reshape(VIEWS * ROWS, DIM), cc)
        dev = ch // (OWN // PC)
        half = pl.ds(pl.multiple_of((ch % (OWN // PC)) * PC, PC), PC)
        e_large, q_large = [], []
        for view in range(2):
            e = jnp.exp(scores[view * ROWS:(view + 1) * ROWS] * (1.0 / TAU))
            q = wide(ab[VIEWS + view]) * (vx[dev, view, :, half] * (e * e))
            qbuf[slot, view] = q
            e_large.append(e)
            q_large.append(q)
        q_sum = q_large[0] + q_large[1]
        gq_sum = q_sum * grad_scale
        parts = [(wide(ab[0]) * e_large[0] - q_large[1] * grad_scale).astype(BF16),
                 (wide(ab[1]) * e_large[1] - q_large[0] * grad_scale).astype(BF16)]
        s_sum = None
        for view in range(2, VIEWS):
            s = scores[view * ROWS:(view + 1) * ROWS]
            s_sum = s if s_sum is None else s_sum + s
            parts.append((wide(ab[view]) * jnp.exp(s * (1.0 / TAU)) - gq_sum).astype(BF16))
        dot = q_large[1] * scores[0:ROWS] + q_large[0] * scores[ROWS:2 * ROWS] + q_sum * s_sum
        for view in range(2):
            qcopy(view, ch, slot).start()
        dzacc[...] += jnp.dot(jnp.concatenate(parts, axis=0), cc, preferred_element_type=F32)
        return acc + fold(dot)
    acc = lax.fori_loop(0, PROTOS // PC, row_chunk, jnp.zeros((8, PC), F32))
    cross = jnp.sum(jnp.sum(acc, axis=0, keepdims=True), axis=1, keepdims=True)
    px[me] = jnp.broadcast_to(cross, (1, 128))
    bcast(*p_args, wait=False)
    dz1_ref[...] = dzacc[0:ROWS]
    dz2_ref[...] = dzacc[ROWS:2 * ROWS]
    for view in range(VIEWS - 2):
        dzs_ref[view] = dzacc[(view + 2) * ROWS:(view + 3) * ROWS]

    def out_copy(dev, ch, half, kind):
        lo = dev * OWN + ch * KC
        if half is None:
            rows = pl.ds(pl.multiple_of(lo, KC), KC)
        else:
            rows = pl.ds(pl.multiple_of(lo + half * (KC // 2), KC // 2), KC // 2)
        return pltpu.make_async_copy(dcv.at[rows], dc_hbm.at[rows], osem.at[kind, ch])

    def gather_near(ch, carry):
        acopy(xn, ch, None, xn, 0).wait_recv()
        acopy(xn, ch, 0, yn, 3).start()
        acopy(xn, ch, None, partner, 5).start()
        acopy(yn, ch, None, yn, 1).wait_recv()
        acopy(yn, ch, 1, xn, 4).start()
        acopy(yn, ch, None, partner, 6).start()
        out_copy(me, ch, None, 0).start()
        out_copy(xn, ch, None, 1).start()
        out_copy(yn, ch, None, 2).start()
        acopy(partner, ch, None, partner, 2).wait_recv()
        out_copy(partner, ch, None, 3).start()
        return carry

    def gather_far(ch, carry):
        acopy(dg, ch, 0, yn, 3).wait_recv()
        acopy(dg, ch, 0, partner, 7).start()
        acopy(dg, ch, 1, xn, 4).wait_recv()
        acopy(dg, ch, 1, partner, 8).start()
        out_copy(dg, ch, None, 4).start()
        acopy(other(xn), ch, None, partner, 5).wait_recv()
        out_copy(other(xn), ch, None, 5).start()
        acopy(other(yn), ch, None, partner, 6).wait_recv()
        out_copy(other(yn), ch, None, 6).start()
        acopy(other(dg), ch, 0, partner, 7).wait_recv()
        acopy(other(dg), ch, 1, partner, 8).wait_recv()
        out_copy(other(dg), ch, None, 7).start()
        return carry
    lax.fori_loop(0, NCH, gather_near, 0)
    bcast(*p_args, wait=True)
    tot = px[0]
    for d in range(1, DEVS):
        tot = tot + px[d]
    loss = -(tot[:, 0:1] * (1.0 / TAU) - log_sum) / (live_total * (2 + 2 * (VIEWS - 2)))
    loss_ref[...] = jnp.broadcast_to(loss, (1, 128))
    lax.fori_loop(0, NCH, gather_far, 0)

    def drain(ch, carry):
        for kind in (0, 1, 2):
            acopy(me, ch, None, partner, kind).wait_send()
        acopy(xn, ch, 0, yn, 3).wait_send()
        acopy(yn, ch, 1, xn, 4).wait_send()
        acopy(xn, ch, None, partner, 5).wait_send()
        acopy(yn, ch, None, partner, 6).wait_send()
        acopy(dg, ch, 0, partner, 7).wait_send()
        acopy(dg, ch, 1, partner, 8).wait_send()
        for kind, dev in enumerate((me, xn, yn, partner, dg, other(xn), other(yn), other(dg))):
            out_copy(dev, ch, None, kind).wait()
        return carry
    for unit in range(len(UNITS)):
        for kind in range(7):
            zcopy(unit, kind).wait_send()
    bcast_drain(*m_args)
    bcast_drain(*p_args)
    bcast_drain(*v_args)
    for it in range(ITERS):
        bcast_drain(*r_args(it))
    for part in range(2):
        bcast_drain(*l_args(part))
    for ch in (PROTOS // PC - 2, PROTOS // PC - 1):
        for view in range(2):
            qcopy(view, ch, ch % 2).wait()
    lax.fori_loop(0, NCH, drain, 0)


def local_step(z_one, z_two, z_small, protos, live_mask):
    vmem = pl.BlockSpec(memory_space=pltpu.VMEM)
    hbm = pl.BlockSpec(memory_space=pl.ANY)
    dma = pltpu.SemaphoreType.DMA
    views = VIEWS
    out = pl.pallas_call(
        body,
        out_shape=(
            jax.ShapeDtypeStruct((ROWS, PROTOS), F32),
            jax.ShapeDtypeStruct((ROWS, PROTOS), F32),
            jax.ShapeDtypeStruct((1, 128), F32),
            jax.ShapeDtypeStruct((ROWS, DIM), F32),
            jax.ShapeDtypeStruct((ROWS, DIM), F32),
            jax.ShapeDtypeStruct((views - 2, ROWS, DIM), F32),
            jax.ShapeDtypeStruct((PROTOS, DIM), F32),
        ),
        in_specs=[vmem, vmem, vmem, vmem, hbm],
        out_specs=(hbm, hbm, vmem, vmem, vmem, vmem, hbm),
        scratch_shapes=[
            pltpu.VMEM((views, NROW, DIM), BF16),
            pltpu.VMEM((views, ROWS, DIM), BF16),
            pltpu.VMEM((PROTOS, DIM), BF16),
            pltpu.VMEM((views, OWN, NROW), F32),
            pltpu.VMEM((2, OWN, NROW), F32),
            pltpu.VMEM((3, KC, NROW), F32),
            pltpu.VMEM((8, 128), BF16),
            pltpu.VMEM((PROTOS, DIM), F32),
            pltpu.VMEM((2, 2, ROWS, PC), F32),
            pltpu.VMEM((2, OWN, 128), F32),
            pltpu.VMEM((DEVS, 2, 1, OWN), F32),
            pltpu.VMEM((ITERS, DEVS, 1, 2 * NROW), F32),
            pltpu.VMEM((DEVS, views, 1, NROW), F32),
            pltpu.VMEM((DEVS, 1, 128), F32),
            pltpu.VMEM((DEVS, 1, 128), F32),
            pltpu.VMEM((1, NROW), F32),
            pltpu.VMEM((2, 1, NROW), F32),
            pltpu.VMEM((views, 1, NROW), F32),
            pltpu.VMEM((128, 128), F32),
            pltpu.VMEM((128, 128), F32),
            pltpu.VMEM((views + 2, ROWS, 128), F32),
            pltpu.VMEM((8, 128), F32),
            pltpu.VMEM((views * ROWS, DIM), F32),
            dma((DEVS,)),
            dma((7, 5)), dma((7, 5)),
            dma((ITERS, DEVS)), dma((ITERS, DEVS)),
            dma((2, DEVS)), dma((2, DEVS)),
            dma((DEVS,)), dma((DEVS,)),
            dma((2, DEVS)), dma((2, DEVS)),
            dma((9, NCH)), dma((9, NCH)),
            dma((2, 2)),
            dma((8, NCH)),
        ],
        compiler_params=pltpu.CompilerParams(
            collective_id=0, has_side_effects=True, vmem_limit_bytes=62 * 1024 * 1024),
        name="swav_step",
    )(live_mask.reshape(1, ROWS), z_one, z_two, z_small, protos)
    q_one, q_two, loss, dz_one, dz_two, dz_small, d_protos = out
    return q_one, q_two, loss[0, 0], dz_one, dz_two, dz_small, d_protos


def solution(mesh):
    row_spec = P("data", None)
    crop_spec = P(None, "data", None)
    return jax.shard_map(local_step, mesh=mesh,
                         in_specs=(row_spec, row_spec, crop_spec, P(None, None), P("data")),
                         out_specs=(row_spec, row_spec, P(), row_spec, row_spec, crop_spec, P(None, None)),
                         check_vma=False)
```

```python
import functools
import math

import jax
import jax.numpy as jnp
from jax import lax
from jax.experimental import pallas as pl
from jax.experimental.pallas import tpu as pltpu
from jax.sharding import PartitionSpec as P

EPS = 0.05
TAU = 0.1
ITERS = 3
DEVS = 8
ROWS = 64
NROW = ROWS * DEVS
PROTOS = 8192
DIM = 256
VIEWS = 12
OWN = PROTOS // DEVS
KC = 256
NCH = OWN // KC
PC = 512
MESH = pl.DeviceIdType.MESH
F32 = jnp.float32
BF16 = jnp.bfloat16
UNITS = ((0, 1), (1, 1), (2, 4), (6, 3), (9, 3))


def nt_dot(a, b):
    return lax.dot_general(a, b, (((1,), (1,)), ((), ())), preferred_element_type=F32)


def body(mask_ref, z1_ref, z2_ref, zs_ref, c_hbm,
         q_out, loss_ref, dz_out, dcv,
         zall, zown, cv, et, a0, vb, vx, rx, lx, mx, px,
         mvec, wvec, acf, cf, ct, ab, lacc,
         csem, zsend, zrecv, rsend, rrecv, lsend, lrecv, vsend, vrecv, psend, precv,
         asend, arecv):
    me = lax.axis_index("data")
    core = me % 2
    xpos = (me // 2) % 2
    ypos = me // 4
    partner = me + 1 - 2 * core
    xn = me + 2 - 4 * xpos
    yn = me + 4 - 8 * ypos
    dg = xn + 4 - 8 * ypos

    def other(d):
        return d + 1 - 2 * core

    own0 = pl.multiple_of(me * OWN, OWN)
    c_copy = pltpu.make_async_copy(c_hbm, cv, csem)
    c_copy.start()

    barrier = pltpu.get_barrier_semaphore()
    for off in range(1, DEVS):
        pl.semaphore_signal(barrier, inc=1, device_id=((me + off) % DEVS,), device_id_type=MESH)

    mrow = mask_ref[...].astype(F32)
    sel = (lax.broadcasted_iota(jnp.int32, (ROWS, 128), 1)
           == lax.broadcasted_iota(jnp.int32, (ROWS, 128), 0) + ROWS * core)
    mplaced = jnp.dot(jnp.broadcast_to(mrow, (8, ROWS)).astype(BF16), sel.astype(BF16),
                      preferred_element_type=F32)
    mx[me] = mplaced[0:1, :]

    def zdst(unit, dev):
        lo, cnt = UNITS[unit]
        rows = pl.ds(pl.multiple_of(dev * ROWS, ROWS), ROWS)
        if cnt == 1:
            return zall.at[lo, rows]
        return zall.at[pl.ds(lo, cnt), rows]

    def zsrc(unit):
        lo, cnt = UNITS[unit]
        if unit == 0:
            return z1_ref
        if unit == 1:
            return z2_ref
        return zs_ref.at[pl.ds(lo - 2, cnt)]

    peers = (partner, xn, yn, dg)

    def zcopy(unit, kind):
        if kind < 4:
            return pltpu.make_async_remote_copy(
                src_ref=zsrc(unit), dst_ref=zdst(unit, me), send_sem=zsend.at[kind, unit],
                recv_sem=zrecv.at[kind, unit], device_id=(peers[kind],), device_id_type=MESH)
        dev = peers[kind - 3]
        return pltpu.make_async_remote_copy(
            src_ref=zdst(unit, dev), dst_ref=zdst(unit, dev), send_sem=zsend.at[kind, unit],
            recv_sem=zrecv.at[kind, unit], device_id=(partner,), device_id_type=MESH)

    def zwait(unit, kind):
        dev = peers[kind] if kind < 4 else other(peers[kind - 3])
        pltpu.make_async_remote_copy(
            src_ref=zsrc(unit), dst_ref=zdst(unit, dev), send_sem=zsend.at[kind, unit],
            recv_sem=zrecv.at[kind, unit], device_id=(partner,), device_id_type=MESH).wait_recv()

    def zstart(unit):
        for kind in (1, 2, 3, 0):
            zcopy(unit, kind).start()

    def zforward(units):
        for kind in (1, 2, 3):
            for unit in units:
                zwait(unit, kind)
                zcopy(unit, kind + 3).start()

    def zfinish(units):
        for unit in units:
            zwait(unit, 0)
        for kind in (4, 5, 6):
            for unit in units:
                zwait(unit, kind)

    def bcast(ref_of, send_sem, recv_sem, wait):
        for off in range(1, DEVS):
            dev = (me + off) % DEVS
            slot = dev if wait else me
            copy = pltpu.make_async_remote_copy(
                src_ref=ref_of(slot), dst_ref=ref_of(slot), send_sem=send_sem(off),
                recv_sem=recv_sem(slot), device_id=(dev,), device_id_type=MESH)
            if wait:
                copy.wait_recv()
            else:
                copy.start()

    def bcast_drain(ref_of, send_sem, recv_sem):
        for off in range(1, DEVS):
            pltpu.make_async_remote_copy(
                src_ref=ref_of(me), dst_ref=ref_of(me), send_sem=send_sem(off),
                recv_sem=recv_sem(me), device_id=((me + off) % DEVS,), device_id_type=MESH).wait_send()

    m_args = (lambda d: mx.at[d], lambda o: psend.at[1, o], lambda d: precv.at[1, d])
    p_args = (lambda d: px.at[d], lambda o: psend.at[0, o], lambda d: precv.at[0, d])
    v_args = (lambda d: vx.at[d], lambda o: vsend.at[o], lambda d: vrecv.at[d])

    def r_args(step):
        return (lambda d: rx.at[step, d], lambda o: rsend.at[step, o], lambda d: rrecv.at[step, d])

    l_args = (lambda d: lx.at[d], lambda o: lsend.at[o], lambda d: lrecv.at[d])

    my_rows = pl.ds(pl.multiple_of(me * ROWS, ROWS), ROWS)
    zall[0, my_rows] = z1_ref[...]
    zall[1, my_rows] = z2_ref[...]
    zown[0] = z1_ref[...]
    zown[1] = z2_ref[...]
    for view in range(VIEWS - 2):
        zall[2 + view, my_rows] = zs_ref[view]
        zown[2 + view] = zs_ref[view]

    pl.semaphore_wait(barrier, DEVS - 1)
    zstart(0)
    zstart(1)
    bcast(*m_args, wait=False)
    zstart(2)

    def fold(x):
        return jnp.sum(x.reshape(x.shape[0] // 8, 8, x.shape[1]), axis=0)

    def lane_fold(x):
        out = x[:, 0:128]
        for i in range(1, x.shape[1] // 128):
            out = out + x[:, i * 128:(i + 1) * 128]
        return out

    lacc[...] = jnp.zeros_like(lacc)
    c_copy.wait()

    def sum_chunk(ch, carry):
        cc = cv[pl.ds(pl.multiple_of(ch * PC, PC), PC)]
        scores = nt_dot(zown[...].reshape(VIEWS * ROWS, DIM), cc)
        lacc[...] += lane_fold(jnp.exp(scores * (1.0 / TAU)))
        return carry
    lax.fori_loop(0, PROTOS // PC, sum_chunk, 0)
    for view in range(VIEWS):
        la = lacc[view * ROWS:(view + 1) * ROWS]
        lx[me, view] = jnp.sum(jnp.concatenate([la, la], axis=0).T, axis=0, keepdims=True)
    bcast(*l_args, wait=False)

    def exp_block(view, ch):
        rows = pl.ds(pl.multiple_of(ch * KC, KC), KC)
        scores = nt_dot(cv[pl.ds(pl.multiple_of(own0 + ch * KC, KC), KC)], zall[view])
        e = jnp.exp(scores * (1.0 / TAU))
        et[view, rows] = e
        return rows, e

    def exp_views(lo, hi):
        def step(i, carry):
            exp_block(lo + i // NCH, i % NCH)
            return carry
        lax.fori_loop(0, (hi - lo) * NCH, step, 0)

    zforward((0, 1))
    bcast(*m_args, wait=True)
    zfinish((0, 1))
    for q in range(NROW // 128):
        mvec[:, q * 128:(q + 1) * 128] = mx[2 * q] + mx[2 * q + 1]
    live_total = jnp.sum(mvec[...], axis=1, keepdims=True)

    SB = 128

    def sq_step(ch, carry):
        for view in range(2):
            rows, e = exp_block(view, ch)
            a0[view, rows] = e * e
        return carry
    lax.fori_loop(0, NCH, sq_step, 0)

    def sink_pass(it):
        scale = (1.0 if it == 0 else live_total) * (1.0 / PROTOS)

        def step(blk, accs):
            rows = pl.ds(pl.multiple_of(blk * SB, SB), SB)
            out = []
            for view in range(2):
                a = a0[view, rows]
                w = mvec[...] if it == 0 else wvec[view]
                colsum = jnp.sum(a * w, axis=1, keepdims=True)
                v = scale / colsum
                if it == ITERS - 1:
                    vb[view, rows] = jnp.broadcast_to(v, (SB, 128))
                out.append(accs[view] + fold(a * v))
            return tuple(out)
        zero = jnp.zeros((8, NROW), F32)
        accs = lax.fori_loop(0, OWN // SB, step, (zero, zero))
        for view in range(2):
            rx[it, me, :, view * NROW:(view + 1) * NROW] = jnp.sum(accs[view], axis=0, keepdims=True)
        bcast(*r_args(it), wait=False)

    def sink_close(it):
        bcast(*r_args(it), wait=True)
        tot = rx[it, 0]
        for d in range(1, DEVS):
            tot = tot + rx[it, d]
        for view in range(2):
            wvec[view] = mvec[...] / tot[:, view * NROW:(view + 1) * NROW]

    sink_pass(0)
    zstart(3)
    bcast(*l_args, wait=True)
    grad_scale = 1.0 / (TAU * live_total * (2 + 2 * (VIEWS - 2)))
    log_sum = jnp.zeros((1, NROW), F32)
    low = lax.broadcasted_iota(jnp.int32, (1, 128), 1) < ROWS
    for view in range(VIEWS):
        tot = jnp.concatenate([jnp.where(low, lx[2 * q, view], lx[2 * q + 1, view])
                               for q in range(NROW // 128)], axis=1)
        mult = 1.0 if view < 2 else 2.0
        acf[view] = (mult * grad_scale) * mvec[...] / tot
        log_sum = log_sum + mult * jnp.log(tot)
    log_sum = jnp.sum(log_sum * mvec[...], axis=1, keepdims=True)
    zforward((2,))
    sink_close(0)
    sink_pass(1)
    zstart(4)
    zfinish((2,))
    exp_views(2, 6)
    zforward((3,))
    sink_close(1)
    sink_pass(2)
    zfinish((3,))
    exp_views(6, 9)
    for view in range(2):
        for blk in range(OWN // 128):
            vt = vb[view, blk * 128:(blk + 1) * 128].T
            vx[me, view, :, blk * 128:(blk + 1) * 128] = vt[0:1, :]
    bcast(*v_args, wait=False)
    zforward((4,))
    zfinish((4,))
    exp_views(9, 12)
    sink_close(2)

    def acopy(src_dev, ch, half, to, kind):
        lo = src_dev * OWN + ch * KC
        if half is None:
            rows = pl.ds(pl.multiple_of(lo, KC), KC)
        else:
            rows = pl.ds(pl.multiple_of(lo + half * (KC // 2), KC // 2), KC // 2)
        return pltpu.make_async_remote_copy(
            src_ref=dcv.at[rows], dst_ref=dcv.at[rows], send_sem=asend.at[kind, ch],
            recv_sem=arecv.at[kind, ch], device_id=(to,), device_id_type=MESH)

    def dc_chunk(ch, carry):
        rows = pl.ds(pl.multiple_of(ch * KC, KC), KC)
        gq = []
        for view in range(2):
            v = jnp.concatenate([vb[view, rows]] * (NROW // 128), axis=1)
            gq.append((wvec[view] * grad_scale) * (v * a0[view, rows]))
        sub = [gq[1], gq[0]] + [gq[0] + gq[1]] * (VIEWS - 2)
        acc = None
        for view in range(VIEWS):
            g = (acf[view] * et[view, rows] - sub[view]).astype(BF16)
            part = jnp.dot(g, zall[view], preferred_element_type=F32)
            acc = part if acc is None else acc + part
        dcv[pl.ds(pl.multiple_of(own0 + ch * KC, KC), KC)] = acc
        for kind, to in ((0, xn), (1, yn), (2, partner)):
            acopy(me, ch, None, to, kind).start()
        return carry
    lax.fori_loop(0, NCH, dc_chunk, 0)

    lanes = pl.ds(pl.multiple_of((me // 2) * 128, 128), 128)
    for view in range(VIEWS):
        cf[view:view + 1, :] = acf[view, :, lanes]
    for view in range(2):
        cf[VIEWS + view:VIEWS + view + 1, :] = wvec[view, :, lanes]
    ct[...] = cf[...].T
    own_cf = ct[pl.ds(pl.multiple_of(core * ROWS, ROWS), ROWS), :]
    for j in range(VIEWS + 2):
        ab[j] = jnp.broadcast_to(own_cf[:, j:j + 1], (ROWS, 128))

    bcast(*v_args, wait=True)
    dz_out[...] = jnp.zeros_like(dz_out)

    def wide(x):
        return jnp.concatenate([x] * (PC // 128), axis=1)

    def row_chunk(ch, acc):
        cols = pl.ds(pl.multiple_of(ch * PC, PC), PC)
        cc = cv[pl.ds(pl.multiple_of(ch * PC, PC), PC)]
        scores = nt_dot(zown[...].reshape(VIEWS * ROWS, DIM), cc)
        dev = ch // (OWN // PC)
        half = pl.ds(pl.multiple_of((ch % (OWN // PC)) * PC, PC), PC)
        e_large, q_large = [], []
        for view in range(2):
            e = jnp.exp(scores[view * ROWS:(view + 1) * ROWS] * (1.0 / TAU))
            q = wide(ab[VIEWS + view]) * (vx[dev, view, :, half] * (e * e))
            q_out[view, :, cols] = q
            e_large.append(e)
            q_large.append(q)
        q_sum = q_large[0] + q_large[1]
        gq_sum = q_sum * grad_scale
        parts = [(wide(ab[0]) * e_large[0] - q_large[1] * grad_scale).astype(BF16),
                 (wide(ab[1]) * e_large[1] - q_large[0] * grad_scale).astype(BF16)]
        s_sum = None
        for view in range(2, VIEWS):
            s = scores[view * ROWS:(view + 1) * ROWS]
            s_sum = s if s_sum is None else s_sum + s
            parts.append((wide(ab[view]) * jnp.exp(s * (1.0 / TAU)) - gq_sum).astype(BF16))
        dot = q_large[1] * scores[0:ROWS] + q_large[0] * scores[ROWS:2 * ROWS] + q_sum * s_sum
        dz = jnp.dot(jnp.concatenate(parts, axis=0), cc, preferred_element_type=F32)
        dz_out[...] += dz.reshape(VIEWS, ROWS, DIM)
        return acc + fold(dot)
    acc = lax.fori_loop(0, PROTOS // PC, row_chunk, jnp.zeros((8, PC), F32))
    cross = jnp.sum(jnp.sum(acc, axis=0, keepdims=True), axis=1, keepdims=True)
    px[me] = jnp.broadcast_to(cross, (1, 128))
    bcast(*p_args, wait=False)

    def gather_near(ch, carry):
        acopy(xn, ch, None, xn, 0).wait_recv()
        acopy(xn, ch, 0, yn, 3).start()
        acopy(xn, ch, None, partner, 5).start()
        acopy(yn, ch, None, yn, 1).wait_recv()
        acopy(yn, ch, 1, xn, 4).start()
        acopy(yn, ch, None, partner, 6).start()
        acopy(partner, ch, None, partner, 2).wait_recv()
        return carry

    def gather_far(ch, carry):
        acopy(dg, ch, 0, yn, 3).wait_recv()
        acopy(dg, ch, 0, partner, 7).start()
        acopy(dg, ch, 1, xn, 4).wait_recv()
        acopy(dg, ch, 1, partner, 8).start()
        acopy(other(xn), ch, None, partner, 5).wait_recv()
        acopy(other(yn), ch, None, partner, 6).wait_recv()
        acopy(other(dg), ch, 0, partner, 7).wait_recv()
        acopy(other(dg), ch, 1, partner, 8).wait_recv()
        return carry
    lax.fori_loop(0, NCH, gather_near, 0)
    bcast(*p_args, wait=True)
    tot = px[0]
    for d in range(1, DEVS):
        tot = tot + px[d]
    loss = -(tot[:, 0:1] * (1.0 / TAU) - log_sum) / (live_total * (2 + 2 * (VIEWS - 2)))
    loss_ref[...] = jnp.broadcast_to(loss, (1, 128))
    lax.fori_loop(0, NCH, gather_far, 0)

    def drain(ch, carry):
        for kind in (0, 1, 2):
            acopy(me, ch, None, partner, kind).wait_send()
        acopy(xn, ch, 0, yn, 3).wait_send()
        acopy(yn, ch, 1, xn, 4).wait_send()
        acopy(xn, ch, None, partner, 5).wait_send()
        acopy(yn, ch, None, partner, 6).wait_send()
        acopy(dg, ch, 0, partner, 7).wait_send()
        acopy(dg, ch, 1, partner, 8).wait_send()
        return carry
    for unit in range(len(UNITS)):
        for kind in range(7):
            zcopy(unit, kind).wait_send()
    bcast_drain(*m_args)
    bcast_drain(*p_args)
    bcast_drain(*v_args)
    for it in range(ITERS):
        bcast_drain(*r_args(it))
    bcast_drain(*l_args)
    lax.fori_loop(0, NCH, drain, 0)


def write_out(q_ref, loss_in, dz_ref, dc_ref, q1_hbm, q2_hbm, loss_ref, dz1_hbm, dz2_hbm, dzs_hbm, dc_hbm, sem):
    copies = []
    for src, dst in ((dc_ref, dc_hbm), (q_ref.at[0], q1_hbm), (q_ref.at[1], q2_hbm),
                     (dz_ref.at[pl.ds(2, VIEWS - 2)], dzs_hbm), (dz_ref.at[0], dz1_hbm), (dz_ref.at[1], dz2_hbm)):
        copies.append(pltpu.make_async_copy(src, dst, sem.at[len(copies)]))
        copies[-1].start()
    loss_ref[0, 0] = jnp.max(loss_in[:, 0:1])
    for copy in copies:
        copy.wait()


def local_step(z_one, z_two, z_small, protos, live_mask):
    vmem = pl.BlockSpec(memory_space=pltpu.VMEM)
    hbm = pl.BlockSpec(memory_space=pl.ANY)
    dma = pltpu.SemaphoreType.DMA
    views = VIEWS
    staged = pl.pallas_call(
        body,
        out_shape=(
            pltpu.VMEM((2, ROWS, PROTOS), F32),
            pltpu.VMEM((1, 128), F32),
            pltpu.VMEM((views, ROWS, DIM), F32),
            pltpu.VMEM((PROTOS, DIM), F32),
        ),
        in_specs=[vmem, vmem, vmem, vmem, hbm],
        out_specs=(vmem, vmem, vmem, vmem),
        scratch_shapes=[
            pltpu.VMEM((views, NROW, DIM), BF16),
            pltpu.VMEM((views, ROWS, DIM), BF16),
            pltpu.VMEM((PROTOS, DIM), BF16),
            pltpu.VMEM((views, OWN, NROW), F32),
            pltpu.VMEM((2, OWN, NROW), F32),
            pltpu.VMEM((2, OWN, 128), F32),
            pltpu.VMEM((DEVS, 2, 1, OWN), F32),
            pltpu.VMEM((ITERS, DEVS, 1, 2 * NROW), F32),
            pltpu.VMEM((DEVS, views, 1, 128), F32),
            pltpu.VMEM((DEVS, 1, 128), F32),
            pltpu.VMEM((DEVS, 1, 128), F32),
            pltpu.VMEM((1, NROW), F32),
            pltpu.VMEM((2, 1, NROW), F32),
            pltpu.VMEM((views, 1, NROW), F32),
            pltpu.VMEM((128, 128), F32),
            pltpu.VMEM((128, 128), F32),
            pltpu.VMEM((views + 2, ROWS, 128), F32),
            pltpu.VMEM((views * ROWS, 128), F32),
            dma(()),
            dma((7, 5)), dma((7, 5)),
            dma((ITERS, DEVS)), dma((ITERS, DEVS)),
            dma((DEVS,)), dma((DEVS,)),
            dma((DEVS,)), dma((DEVS,)),
            dma((2, DEVS)), dma((2, DEVS)),
            dma((9, NCH)), dma((9, NCH)),
        ],
        compiler_params=pltpu.CompilerParams(
            collective_id=0, has_side_effects=True, vmem_limit_bytes=48 * 1024 * 1024),
        name="swav_step",
    )(live_mask.reshape(1, ROWS), z_one, z_two, z_small, protos)
    q_one, q_two, loss, dz_one, dz_two, dz_small, d_protos = pl.pallas_call(
        write_out,
        out_shape=(
            jax.ShapeDtypeStruct((ROWS, PROTOS), F32),
            jax.ShapeDtypeStruct((ROWS, PROTOS), F32),
            jax.ShapeDtypeStruct((1, 1), F32),
            jax.ShapeDtypeStruct((ROWS, DIM), F32),
            jax.ShapeDtypeStruct((ROWS, DIM), F32),
            jax.ShapeDtypeStruct((views - 2, ROWS, DIM), F32),
            jax.ShapeDtypeStruct((PROTOS, DIM), F32),
        ),
        in_specs=[vmem] * 4,
        out_specs=(hbm, hbm, pl.BlockSpec(memory_space=pltpu.SMEM), hbm, hbm, hbm, hbm),
        scratch_shapes=[dma((6,))],
        compiler_params=pltpu.CompilerParams(vmem_limit_bytes=1024 * 1024),
        name="write_out",
    )(*staged)
    return q_one, q_two, loss[0, 0], dz_one, dz_two, dz_small, d_protos


def solution(mesh):
    row_spec = P("data", None)
    crop_spec = P(None, "data", None)
    return jax.shard_map(local_step, mesh=mesh,
                         in_specs=(row_spec, row_spec, crop_spec, P(None, None), P("data")),
                         out_specs=(row_spec, row_spec, P(), row_spec, row_spec, crop_spec, P(None, None)),
                         check_vma=False)
```

```python
import functools
import math

import jax
import jax.numpy as jnp
from jax import lax
from jax.experimental import pallas as pl
from jax.experimental.pallas import tpu as pltpu
from jax.sharding import PartitionSpec as P

EPS = 0.05
TAU = 0.1
ITERS = 3
DEVS = 8
ROWS = 64
NROW = ROWS * DEVS
PROTOS = 8192
DIM = 256
VIEWS = 12
OWN = PROTOS // DEVS
KC = 256
NCH = OWN // KC
PC = 512
MESH = pl.DeviceIdType.MESH
F32 = jnp.float32
BF16 = jnp.bfloat16
UNITS = ((0, 1), (1, 1), (2, 4), (6, 4), (10, 2))
SENT = 2
EC = 512


def nt_dot(a, b):
    return lax.dot_general(a, b, (((1,), (1,)), ((), ())), preferred_element_type=F32)


def body(mask_ref, z1_ref, z2_ref, zs_ref, c_hbm,
         q_out, loss_ref, dz_out, dcv,
         zall, zown, cv, et, a0, vb, vx, rx, lx, mx, px,
         mvec, wvec, acf, cf, ct, ab, lacc,
         csem, zsend, zrecv, rsend, rrecv, lsend, lrecv, vsend, vrecv, psend, precv,
         asend, arecv):
    me = lax.axis_index("data")
    core = me % 2
    xpos = (me // 2) % 2
    ypos = me // 4
    partner = me + 1 - 2 * core
    xn = me + 2 - 4 * xpos
    yn = me + 4 - 8 * ypos
    dg = xn + 4 - 8 * ypos

    def other(d):
        return d + 1 - 2 * core

    own0 = pl.multiple_of(me * OWN, OWN)
    c_copy = pltpu.make_async_copy(c_hbm, cv, csem)
    c_copy.start()

    barrier = pltpu.get_barrier_semaphore()
    for off in range(1, DEVS):
        pl.semaphore_signal(barrier, inc=1, device_id=((me + off) % DEVS,), device_id_type=MESH)

    mrow = mask_ref[...].astype(F32)
    sel = (lax.broadcasted_iota(jnp.int32, (ROWS, 128), 1)
           == lax.broadcasted_iota(jnp.int32, (ROWS, 128), 0) + ROWS * core)
    mplaced = jnp.dot(jnp.broadcast_to(mrow, (8, ROWS)).astype(BF16), sel.astype(BF16),
                      preferred_element_type=F32)
    mx[me] = mplaced[0:1, :]

    def zdst(unit, dev):
        lo, cnt = UNITS[unit]
        rows = pl.ds(pl.multiple_of(dev * ROWS, ROWS), ROWS)
        if cnt == 1:
            return zall.at[lo, rows]
        return zall.at[pl.ds(lo, cnt), rows]

    def zsrc(unit):
        lo, cnt = UNITS[unit]
        if unit == 0:
            return z1_ref
        if unit == 1:
            return z2_ref
        return zs_ref.at[pl.ds(lo - 2, cnt)]

    peers = (partner, xn, yn, dg)

    def zcopy(unit, kind):
        if kind < 4:
            return pltpu.make_async_remote_copy(
                src_ref=zsrc(unit), dst_ref=zdst(unit, me), send_sem=zsend.at[kind, unit],
                recv_sem=zrecv.at[kind, unit], device_id=(peers[kind],), device_id_type=MESH)
        dev = peers[kind - 3]
        return pltpu.make_async_remote_copy(
            src_ref=zdst(unit, dev), dst_ref=zdst(unit, dev), send_sem=zsend.at[kind, unit],
            recv_sem=zrecv.at[kind, unit], device_id=(partner,), device_id_type=MESH)

    def zwait(unit, kind):
        dev = peers[kind] if kind < 4 else other(peers[kind - 3])
        pltpu.make_async_remote_copy(
            src_ref=zsrc(unit), dst_ref=zdst(unit, dev), send_sem=zsend.at[kind, unit],
            recv_sem=zrecv.at[kind, unit], device_id=(partner,), device_id_type=MESH).wait_recv()

    def zstart(unit):
        for kind in (1, 2, 3, 0):
            zcopy(unit, kind).start()

    def zforward(units):
        for kind in (1, 2, 3):
            for unit in units:
                zwait(unit, kind)
                zcopy(unit, kind + 3).start()

    def zfinish(units):
        for unit in units:
            zwait(unit, 0)
        for kind in (4, 5, 6):
            for unit in units:
                zwait(unit, kind)

    def bcast(ref_of, send_sem, recv_sem, wait):
        for off in range(1, DEVS):
            dev = (me + off) % DEVS
            slot = dev if wait else me
            copy = pltpu.make_async_remote_copy(
                src_ref=ref_of(slot), dst_ref=ref_of(slot), send_sem=send_sem(off),
                recv_sem=recv_sem(slot), device_id=(dev,), device_id_type=MESH)
            if wait:
                copy.wait_recv()
            else:
                copy.start()

    def bcast_drain(ref_of, send_sem, recv_sem):
        for off in range(1, DEVS):
            pltpu.make_async_remote_copy(
                src_ref=ref_of(me), dst_ref=ref_of(me), send_sem=send_sem(off),
                recv_sem=recv_sem(me), device_id=((me + off) % DEVS,), device_id_type=MESH).wait_send()

    m_args = (lambda d: mx.at[d], lambda o: psend.at[1, o], lambda d: precv.at[1, d])
    p_args = (lambda d: px.at[d], lambda o: psend.at[0, o], lambda d: precv.at[0, d])
    v_args = (lambda d: vx.at[d], lambda o: vsend.at[o], lambda d: vrecv.at[d])

    def r_args(step):
        return (lambda d: rx.at[step, d], lambda o: rsend.at[step, o], lambda d: rrecv.at[step, d])

    l_args = (lambda d: lx.at[d], lambda o: lsend.at[o], lambda d: lrecv.at[d])

    my_rows = pl.ds(pl.multiple_of(me * ROWS, ROWS), ROWS)
    zall[0, my_rows] = z1_ref[...]
    zall[1, my_rows] = z2_ref[...]
    zown[0] = z1_ref[...]
    zown[1] = z2_ref[...]
    for view in range(VIEWS - 2):
        zall[2 + view, my_rows] = zs_ref[view]
        zown[2 + view] = zs_ref[view]

    pl.semaphore_wait(barrier, DEVS - 1)
    zstart(0)
    zstart(1)
    bcast(*m_args, wait=False)
    zstart(2)

    def fold(x):
        return jnp.sum(x.reshape(x.shape[0] // 8, 8, x.shape[1]), axis=0)

    def lane_fold(x):
        out = x[:, 0:128]
        for i in range(1, x.shape[1] // 128):
            out = out + x[:, i * 128:(i + 1) * 128]
        return out

    lacc[...] = jnp.zeros_like(lacc)
    c_copy.wait()

    def sum_chunk(ch, carry):
        cc = cv[pl.ds(pl.multiple_of(ch * PC, PC), PC)]
        scores = nt_dot(zown[...].reshape(VIEWS * ROWS, DIM), cc)
        lacc[...] += lane_fold(jnp.exp(scores * (1.0 / TAU)))
        return carry
    def row_sums_out():
        for view in range(VIEWS):
            la = lacc[view * ROWS:(view + 1) * ROWS]
            lx[me, view] = jnp.sum(jnp.concatenate([la, la], axis=0).T, axis=0, keepdims=True)
        bcast(*l_args, wait=False)

    def exp_block(view, ch):
        rows = pl.ds(pl.multiple_of(ch * EC, EC), EC)
        scores = nt_dot(cv[pl.ds(pl.multiple_of(own0 + ch * EC, EC), EC)], zall[view])
        e = jnp.exp(scores * (1.0 / TAU))
        et[view, rows] = e
        return rows, e

    def exp_views(lo, hi):
        def step(view, carry):
            for ch in range(OWN // EC):
                exp_block(view, ch)
            return carry
        lax.fori_loop(lo, hi, step, 0)

    lax.fori_loop(0, 6, sum_chunk, 0)
    zforward((0, 1))
    lax.fori_loop(6, 8, sum_chunk, 0)
    bcast(*m_args, wait=True)
    zfinish((0, 1))
    for q in range(NROW // 128):
        mvec[:, q * 128:(q + 1) * 128] = mx[2 * q] + mx[2 * q + 1]
    live_total = jnp.sum(mvec[...], axis=1, keepdims=True)

    SB = 128

    def sq_step(i, carry):
        rows, e = exp_block(i // 2, i % 2)
        a0[i // 2, rows] = e * e
        return carry
    lax.fori_loop(0, 2 * (OWN // EC), sq_step, 0)

    def sink_pass(it):
        scale = (1.0 if it == 0 else live_total) * (1.0 / PROTOS)

        def step(blk, accs):
            rows = pl.ds(pl.multiple_of(blk * SB, SB), SB)
            out = []
            for view in range(2):
                a = a0[view, rows]
                w = mvec[...] if it == 0 else wvec[view]
                colsum = jnp.sum(a * w, axis=1, keepdims=True)
                v = scale / colsum
                if it == ITERS - 1:
                    vb[view, rows] = jnp.broadcast_to(v, (SB, 128))
                out.append(accs[view] + fold(a * v))
            return tuple(out)
        zero = jnp.zeros((8, NROW), F32)
        accs = lax.fori_loop(0, OWN // SB, step, (zero, zero))
        for view in range(2):
            rx[it, me, :, view * NROW:(view + 1) * NROW] = jnp.sum(accs[view], axis=0, keepdims=True)
        bcast(*r_args(it), wait=False)

    def sink_close(it):
        bcast(*r_args(it), wait=True)
        tot = rx[it, 0]
        for d in range(1, DEVS):
            tot = tot + rx[it, d]
        for view in range(2):
            wvec[view] = mvec[...] / tot[:, view * NROW:(view + 1) * NROW]

    sink_pass(0)
    zstart(3)
    lax.fori_loop(8, PROTOS // PC, sum_chunk, 0)
    row_sums_out()
    zforward((2,))
    sink_close(0)
    sink_pass(1)
    zstart(4)
    zfinish((2,))
    exp_views(2, 6)
    zforward((3,))
    sink_close(1)
    sink_pass(2)
    bcast(*l_args, wait=True)
    grad_scale = 1.0 / (TAU * live_total * (2 + 2 * (VIEWS - 2)))
    log_sum = jnp.zeros((1, NROW), F32)
    low = lax.broadcasted_iota(jnp.int32, (1, 128), 1) < ROWS
    for view in range(VIEWS):
        tot = jnp.concatenate([jnp.where(low, lx[2 * q, view], lx[2 * q + 1, view])
                               for q in range(NROW // 128)], axis=1)
        mult = 1.0 if view < 2 else 2.0
        acf[view] = (mult * grad_scale) * mvec[...] / tot
        log_sum = log_sum + mult * jnp.log(tot)
    log_sum = jnp.sum(log_sum * mvec[...], axis=1, keepdims=True)
    for view in range(2):
        for blk in range(OWN // 128):
            vt = vb[view, blk * 128:(blk + 1) * 128].T
            vx[me, view, :, blk * 128:(blk + 1) * 128] = vt[0:1, :]
    bcast(*v_args, wait=False)
    zfinish((3,))
    exp_views(6, 10)
    zforward((4,))
    zfinish((4,))
    exp_views(10, 12)
    sink_close(2)

    def acopy(src_dev, ch, half, to, kind):
        lo = src_dev * OWN + ch * KC
        if half is None:
            rows = pl.ds(pl.multiple_of(lo, KC), KC)
        else:
            rows = pl.ds(pl.multiple_of(lo + half * (KC // 2), KC // 2), KC // 2)
        return pltpu.make_async_remote_copy(
            src_ref=dcv.at[rows], dst_ref=dcv.at[rows], send_sem=asend.at[kind, ch],
            recv_sem=arecv.at[kind, ch], device_id=(to,), device_id_type=MESH)

    def dc_chunk(ch, carry):
        rows = pl.ds(pl.multiple_of(ch * KC, KC), KC)
        gq = []
        for view in range(2):
            v = jnp.concatenate([vb[view, rows]] * (NROW // 128), axis=1)
            gq.append((wvec[view] * grad_scale) * (v * a0[view, rows]))
        sub = [gq[1], gq[0]] + [gq[0] + gq[1]] * (VIEWS - 2)
        acc = None
        for view in range(VIEWS):
            g = (acf[view] * et[view, rows] - sub[view]).astype(BF16)
            part = jnp.dot(g, zall[view], preferred_element_type=F32)
            acc = part if acc is None else acc + part
        dcv[pl.ds(pl.multiple_of(own0 + ch * KC, KC), KC)] = acc
        acopy(me, ch, None, partner, 2).start()
        return carry

    def dc_sent(ch, carry):
        dc_chunk(ch, carry)
        acopy(me, ch, None, xn, 0).start()
        acopy(me, ch, None, yn, 1).start()
        return carry
    lax.fori_loop(0, SENT, dc_sent, 0)
    lax.fori_loop(SENT, NCH, dc_chunk, 0)

    def dc_again(i, carry):
        which = i % 3
        ch = SENT + i // 3
        dev = me + (1 - which % 2) * (2 - 4 * xpos) + ((which + 1) // 2) * (4 - 8 * ypos)
        lo = pl.multiple_of(dev * OWN + ch * KC, KC)
        cc = cv[pl.ds(lo, KC)]

        def expo(view):
            return jnp.exp(nt_dot(cc, zall[view]) * (1.0 / TAU))
        gq, es = [], []
        for view in range(2):
            vrow = vx[dev, view, :, pl.ds(pl.multiple_of(ch * KC, KC), KC)]
            v = jnp.concatenate([jnp.broadcast_to(vrow[:, j * 128:(j + 1) * 128], (128, 128)).T
                                 for j in range(KC // 128)], axis=0)
            v = jnp.concatenate([v] * (NROW // 128), axis=1)
            e = expo(view)
            es.append(e)
            gq.append((wvec[view] * grad_scale) * (v * (e * e)))
        sub = [gq[1], gq[0]] + [gq[0] + gq[1]] * (VIEWS - 2)
        acc = None
        for view in range(VIEWS):
            e = es[view] if view < 2 else expo(view)
            g = (acf[view] * e - sub[view]).astype(BF16)
            part = jnp.dot(g, zall[view], preferred_element_type=F32)
            acc = part if acc is None else acc + part
        dcv[pl.ds(lo, KC)] = acc
        acopy(dev, ch, None, partner, 5 + which).start()
        return carry

    def relay(ch):
        acopy(xn, ch, None, xn, 0).wait_recv()
        acopy(xn, ch, 0, yn, 3).start()
        acopy(xn, ch, None, partner, 5).start()
        acopy(yn, ch, None, yn, 1).wait_recv()
        acopy(yn, ch, 1, xn, 4).start()
        acopy(yn, ch, None, partner, 6).start()

    bcast(*v_args, wait=True)
    lax.fori_loop(0, 3, dc_again, 0)
    relay(0)
    lax.fori_loop(3, 3 * (NCH - SENT), dc_again, 0)
    relay(1)

    lanes = pl.ds(pl.multiple_of((me // 2) * 128, 128), 128)
    for view in range(VIEWS):
        cf[view:view + 1, :] = acf[view, :, lanes]
    for view in range(2):
        cf[VIEWS + view:VIEWS + view + 1, :] = wvec[view, :, lanes]
    ct[...] = cf[...].T
    own_cf = ct[pl.ds(pl.multiple_of(core * ROWS, ROWS), ROWS), :]
    for j in range(VIEWS + 2):
        ab[j] = jnp.broadcast_to(own_cf[:, j:j + 1], (ROWS, 128))

    dz_out[...] = jnp.zeros_like(dz_out)

    def wide(x):
        return jnp.concatenate([x] * (PC // 128), axis=1)

    def row_chunk(ch, acc):
        cols = pl.ds(pl.multiple_of(ch * PC, PC), PC)
        cc = cv[pl.ds(pl.multiple_of(ch * PC, PC), PC)]
        scores = nt_dot(zown[...].reshape(VIEWS * ROWS, DIM), cc)
        dev = ch // (OWN // PC)
        half = pl.ds(pl.multiple_of((ch % (OWN // PC)) * PC, PC), PC)
        e_large, q_large = [], []
        for view in range(2):
            e = jnp.exp(scores[view * ROWS:(view + 1) * ROWS] * (1.0 / TAU))
            q = wide(ab[VIEWS + view]) * (vx[dev, view, :, half] * (e * e))
            q_out[view, :, cols] = q
            e_large.append(e)
            q_large.append(q)
        q_sum = q_large[0] + q_large[1]
        gq_sum = q_sum * grad_scale
        parts = [(wide(ab[0]) * e_large[0] - q_large[1] * grad_scale).astype(BF16),
                 (wide(ab[1]) * e_large[1] - q_large[0] * grad_scale).astype(BF16)]
        s_sum = None
        for view in range(2, VIEWS):
            s = scores[view * ROWS:(view + 1) * ROWS]
            s_sum = s if s_sum is None else s_sum + s
            parts.append((wide(ab[view]) * jnp.exp(s * (1.0 / TAU)) - gq_sum).astype(BF16))
        dot = q_large[1] * scores[0:ROWS] + q_large[0] * scores[ROWS:2 * ROWS] + q_sum * s_sum
        dz = jnp.dot(jnp.concatenate(parts, axis=0), cc, preferred_element_type=F32)
        dz_out[...] += dz.reshape(VIEWS, ROWS, DIM)
        return acc + fold(dot)
    acc = lax.fori_loop(0, PROTOS // PC, row_chunk, jnp.zeros((8, PC), F32))
    cross = jnp.sum(jnp.sum(acc, axis=0, keepdims=True), axis=1, keepdims=True)
    px[me] = jnp.broadcast_to(cross, (1, 128))
    bcast(*p_args, wait=False)

    def gather_far(ch, carry):
        acopy(dg, ch, 0, yn, 3).wait_recv()
        acopy(dg, ch, 0, partner, 7).start()
        acopy(dg, ch, 1, xn, 4).wait_recv()
        acopy(dg, ch, 1, partner, 8).start()
        return carry

    bcast(*p_args, wait=True)
    tot = px[0]
    for d in range(1, DEVS):
        tot = tot + px[d]
    loss = -(tot[:, 0:1] * (1.0 / TAU) - log_sum) / (live_total * (2 + 2 * (VIEWS - 2)))
    loss_ref[...] = jnp.broadcast_to(loss, (1, 128))
    lax.fori_loop(0, SENT, gather_far, 0)

    def drain_sent(ch, carry):
        acopy(other(dg), ch, 0, partner, 7).wait_recv()
        acopy(other(dg), ch, 1, partner, 8).wait_recv()
        for kind in (0, 1):
            acopy(me, ch, None, partner, kind).wait_send()
        acopy(xn, ch, 0, yn, 3).wait_send()
        acopy(yn, ch, 1, xn, 4).wait_send()
        acopy(dg, ch, 0, partner, 7).wait_send()
        acopy(dg, ch, 1, partner, 8).wait_send()
        return carry

    def drain_again(ch, carry):
        acopy(other(dg), ch, None, partner, 7).wait_recv()
        acopy(dg, ch, None, partner, 7).wait_send()
        return carry

    def drain(ch, carry):
        acopy(partner, ch, None, partner, 2).wait_recv()
        acopy(other(xn), ch, None, partner, 5).wait_recv()
        acopy(other(yn), ch, None, partner, 6).wait_recv()
        acopy(me, ch, None, partner, 2).wait_send()
        acopy(xn, ch, None, partner, 5).wait_send()
        acopy(yn, ch, None, partner, 6).wait_send()
        return carry
    for unit in range(len(UNITS)):
        for kind in range(7):
            zcopy(unit, kind).wait_send()
    bcast_drain(*m_args)
    bcast_drain(*p_args)
    bcast_drain(*v_args)
    for it in range(ITERS):
        bcast_drain(*r_args(it))
    bcast_drain(*l_args)
    lax.fori_loop(0, NCH, drain, 0)
    lax.fori_loop(SENT, NCH, drain_again, 0)
    lax.fori_loop(0, SENT, drain_sent, 0)


def write_out(q_ref, loss_in, dz_ref, dc_ref, q1_hbm, q2_hbm, loss_ref, dz1_hbm, dz2_hbm, dzs_hbm, dc_hbm, sem):
    copies = []
    for src, dst in ((dc_ref, dc_hbm), (q_ref.at[0], q1_hbm), (q_ref.at[1], q2_hbm),
                     (dz_ref.at[pl.ds(2, VIEWS - 2)], dzs_hbm), (dz_ref.at[0], dz1_hbm), (dz_ref.at[1], dz2_hbm)):
        copies.append(pltpu.make_async_copy(src, dst, sem.at[len(copies)]))
        copies[-1].start()
    loss_ref[0, 0] = jnp.max(loss_in[:, 0:1])
    for copy in copies:
        copy.wait()


def local_step(z_one, z_two, z_small, protos, live_mask):
    vmem = pl.BlockSpec(memory_space=pltpu.VMEM)
    hbm = pl.BlockSpec(memory_space=pl.ANY)
    dma = pltpu.SemaphoreType.DMA
    views = VIEWS
    staged = pl.pallas_call(
        body,
        out_shape=(
            pltpu.VMEM((2, ROWS, PROTOS), F32),
            pltpu.VMEM((1, 128), F32),
            pltpu.VMEM((views, ROWS, DIM), F32),
            pltpu.VMEM((PROTOS, DIM), F32),
        ),
        in_specs=[vmem, vmem, vmem, vmem, hbm],
        out_specs=(vmem, vmem, vmem, vmem),
        scratch_shapes=[
            pltpu.VMEM((views, NROW, DIM), BF16),
            pltpu.VMEM((views, ROWS, DIM), BF16),
            pltpu.VMEM((PROTOS, DIM), BF16),
            pltpu.VMEM((views, OWN, NROW), F32),
            pltpu.VMEM((2, OWN, NROW), F32),
            pltpu.VMEM((2, OWN, 128), F32),
            pltpu.VMEM((DEVS, 2, 1, OWN), F32),
            pltpu.VMEM((ITERS, DEVS, 1, 2 * NROW), F32),
            pltpu.VMEM((DEVS, views, 1, 128), F32),
            pltpu.VMEM((DEVS, 1, 128), F32),
            pltpu.VMEM((DEVS, 1, 128), F32),
            pltpu.VMEM((1, NROW), F32),
            pltpu.VMEM((2, 1, NROW), F32),
            pltpu.VMEM((views, 1, NROW), F32),
            pltpu.VMEM((128, 128), F32),
            pltpu.VMEM((128, 128), F32),
            pltpu.VMEM((views + 2, ROWS, 128), F32),
            pltpu.VMEM((views * ROWS, 128), F32),
            dma(()),
            dma((7, 5)), dma((7, 5)),
            dma((ITERS, DEVS)), dma((ITERS, DEVS)),
            dma((DEVS,)), dma((DEVS,)),
            dma((DEVS,)), dma((DEVS,)),
            dma((2, DEVS)), dma((2, DEVS)),
            dma((9, NCH)), dma((9, NCH)),
        ],
        compiler_params=pltpu.CompilerParams(
            collective_id=0, has_side_effects=True, vmem_limit_bytes=48 * 1024 * 1024),
        name="swav_step",
    )(live_mask.reshape(1, ROWS), z_one, z_two, z_small, protos)
    q_one, q_two, loss, dz_one, dz_two, dz_small, d_protos = pl.pallas_call(
        write_out,
        out_shape=(
            jax.ShapeDtypeStruct((ROWS, PROTOS), F32),
            jax.ShapeDtypeStruct((ROWS, PROTOS), F32),
            jax.ShapeDtypeStruct((1, 1), F32),
            jax.ShapeDtypeStruct((ROWS, DIM), F32),
            jax.ShapeDtypeStruct((ROWS, DIM), F32),
            jax.ShapeDtypeStruct((views - 2, ROWS, DIM), F32),
            jax.ShapeDtypeStruct((PROTOS, DIM), F32),
        ),
        in_specs=[vmem] * 4,
        out_specs=(hbm, hbm, pl.BlockSpec(memory_space=pltpu.SMEM), hbm, hbm, hbm, hbm),
        scratch_shapes=[dma((6,))],
        compiler_params=pltpu.CompilerParams(vmem_limit_bytes=1024 * 1024),
        name="write_out",
    )(*staged)
    return q_one, q_two, loss[0, 0], dz_one, dz_two, dz_small, d_protos


def solution(mesh):
    row_spec = P("data", None)
    crop_spec = P(None, "data", None)
    return jax.shard_map(local_step, mesh=mesh,
                         in_specs=(row_spec, row_spec, crop_spec, P(None, None), P("data")),
                         out_specs=(row_spec, row_spec, P(), row_spec, row_spec, crop_spec, P(None, None)),
                         check_vma=False)
```

```python
import functools
import math

import jax
import jax.numpy as jnp
from jax import lax
from jax.experimental import pallas as pl
from jax.experimental.pallas import tpu as pltpu
from jax.sharding import PartitionSpec as P

EPS = 0.05
TAU = 0.1
ITERS = 3
DEVS = 8
ROWS = 64
NROW = ROWS * DEVS
PROTOS = 8192
DIM = 256
VIEWS = 12
OWN = PROTOS // DEVS
KC = 256
NCH = OWN // KC
PC = 512
MESH = pl.DeviceIdType.MESH
F32 = jnp.float32
BF16 = jnp.bfloat16
UNITS = ((0, 1), (1, 1), (2, 4), (6, 4), (10, 2))
SENT = 2
EC = 512


def nt_dot(a, b):
    return lax.dot_general(a, b, (((1,), (1,)), ((), ())), preferred_element_type=F32)


def body(mask_ref, z1_ref, z2_ref, zs_ref, c_hbm,
         q_out, loss_ref, dz_out, dcv,
         zall, zown, cv, et, a0, vb, vx, rx, lx, mx, px,
         mvec, wvec, acf, cf, ct, ab, lacc,
         csem, zsend, zrecv, rsend, rrecv, lsend, lrecv, vsend, vrecv, psend, precv,
         asend, arecv):
    me = lax.axis_index("data")
    core = me % 2
    xpos = (me // 2) % 2
    ypos = me // 4
    partner = me + 1 - 2 * core
    xn = me + 2 - 4 * xpos
    yn = me + 4 - 8 * ypos
    dg = xn + 4 - 8 * ypos

    def other(d):
        return d + 1 - 2 * core

    own0 = pl.multiple_of(me * OWN, OWN)
    c_copy = pltpu.make_async_copy(c_hbm, cv, csem)
    c_copy.start()

    barrier = pltpu.get_barrier_semaphore()
    for off in range(1, DEVS):
        pl.semaphore_signal(barrier, inc=1, device_id=((me + off) % DEVS,), device_id_type=MESH)

    mrow = mask_ref[...].astype(F32)
    sel = (lax.broadcasted_iota(jnp.int32, (ROWS, 128), 1)
           == lax.broadcasted_iota(jnp.int32, (ROWS, 128), 0) + ROWS * core)
    mplaced = jnp.dot(jnp.broadcast_to(mrow, (8, ROWS)).astype(BF16), sel.astype(BF16),
                      preferred_element_type=F32)
    mx[me] = mplaced[0:1, :]

    def zdst(unit, dev):
        lo, cnt = UNITS[unit]
        rows = pl.ds(pl.multiple_of(dev * ROWS, ROWS), ROWS)
        if cnt == 1:
            return zall.at[lo, rows]
        return zall.at[pl.ds(lo, cnt), rows]

    def zsrc(unit):
        lo, cnt = UNITS[unit]
        if unit == 0:
            return z1_ref
        if unit == 1:
            return z2_ref
        return zs_ref.at[pl.ds(lo - 2, cnt)]

    peers = (partner, xn, yn, dg)

    def zcopy(unit, kind):
        if kind < 4:
            return pltpu.make_async_remote_copy(
                src_ref=zsrc(unit), dst_ref=zdst(unit, me), send_sem=zsend.at[kind, unit],
                recv_sem=zrecv.at[kind, unit], device_id=(peers[kind],), device_id_type=MESH)
        dev = peers[kind - 3]
        return pltpu.make_async_remote_copy(
            src_ref=zdst(unit, dev), dst_ref=zdst(unit, dev), send_sem=zsend.at[kind, unit],
            recv_sem=zrecv.at[kind, unit], device_id=(partner,), device_id_type=MESH)

    def zwait(unit, kind):
        dev = peers[kind] if kind < 4 else other(peers[kind - 3])
        pltpu.make_async_remote_copy(
            src_ref=zsrc(unit), dst_ref=zdst(unit, dev), send_sem=zsend.at[kind, unit],
            recv_sem=zrecv.at[kind, unit], device_id=(partner,), device_id_type=MESH).wait_recv()

    def zstart(unit):
        for kind in (1, 2, 3, 0):
            zcopy(unit, kind).start()

    def zforward(units):
        for kind in (1, 2, 3):
            for unit in units:
                zwait(unit, kind)
                zcopy(unit, kind + 3).start()

    def zfinish(units):
        for unit in units:
            zwait(unit, 0)
        for kind in (4, 5, 6):
            for unit in units:
                zwait(unit, kind)

    def bcast(ref_of, send_sem, recv_sem, wait):
        for off in range(1, DEVS):
            dev = (me + off) % DEVS
            slot = dev if wait else me
            copy = pltpu.make_async_remote_copy(
                src_ref=ref_of(slot), dst_ref=ref_of(slot), send_sem=send_sem(off),
                recv_sem=recv_sem(slot), device_id=(dev,), device_id_type=MESH)
            if wait:
                copy.wait_recv()
            else:
                copy.start()

    def bcast_drain(ref_of, send_sem, recv_sem):
        for off in range(1, DEVS):
            pltpu.make_async_remote_copy(
                src_ref=ref_of(me), dst_ref=ref_of(me), send_sem=send_sem(off),
                recv_sem=recv_sem(me), device_id=((me + off) % DEVS,), device_id_type=MESH).wait_send()

    m_args = (lambda d: mx.at[d], lambda o: psend.at[1, o], lambda d: precv.at[1, d])
    p_args = (lambda d: px.at[d], lambda o: psend.at[0, o], lambda d: precv.at[0, d])
    v_args = (lambda d: vx.at[d], lambda o: vsend.at[o], lambda d: vrecv.at[d])

    def r_args(step):
        return (lambda d: rx.at[step, d], lambda o: rsend.at[step, o], lambda d: rrecv.at[step, d])

    l_args = (lambda d: lx.at[d], lambda o: lsend.at[o], lambda d: lrecv.at[d])

    my_rows = pl.ds(pl.multiple_of(me * ROWS, ROWS), ROWS)
    zall[0, my_rows] = z1_ref[...]
    zall[1, my_rows] = z2_ref[...]
    zown[0] = z1_ref[...]
    zown[1] = z2_ref[...]
    for view in range(VIEWS - 2):
        zall[2 + view, my_rows] = zs_ref[view]
        zown[2 + view] = zs_ref[view]

    pl.semaphore_wait(barrier, DEVS - 1)
    zstart(0)
    zstart(1)
    bcast(*m_args, wait=False)
    zstart(2)
    zstart(3)
    zstart(4)

    def fold(x):
        return jnp.sum(x.reshape(x.shape[0] // 8, 8, x.shape[1]), axis=0)

    def lane_fold(x):
        out = x[:, 0:128]
        for i in range(1, x.shape[1] // 128):
            out = out + x[:, i * 128:(i + 1) * 128]
        return out

    lacc[...] = jnp.zeros_like(lacc)
    c_copy.wait()

    def sum_chunk(ch, carry):
        cc = cv[pl.ds(pl.multiple_of(ch * PC, PC), PC)]
        scores = nt_dot(zown[...].reshape(VIEWS * ROWS, DIM), cc)
        lacc[...] += lane_fold(jnp.exp(scores * (1.0 / TAU)))
        return carry
    def row_sums_out():
        for view in range(VIEWS):
            la = lacc[view * ROWS:(view + 1) * ROWS]
            lx[me, view] = jnp.sum(jnp.concatenate([la, la], axis=0).T, axis=0, keepdims=True)
        bcast(*l_args, wait=False)

    def exp_block(view, ch):
        rows = pl.ds(pl.multiple_of(ch * EC, EC), EC)
        scores = nt_dot(cv[pl.ds(pl.multiple_of(own0 + ch * EC, EC), EC)], zall[view])
        e = jnp.exp(scores * (1.0 / TAU))
        et[view, rows] = e
        return rows, e

    def exp_views(lo, hi):
        def step(view, carry):
            for ch in range(OWN // EC):
                exp_block(view, ch)
            return carry
        lax.fori_loop(lo, hi, step, 0)

    lax.fori_loop(0, 6, sum_chunk, 0)
    zforward((0, 1))
    lax.fori_loop(6, 8, sum_chunk, 0)
    bcast(*m_args, wait=True)
    zfinish((0, 1))
    for q in range(NROW // 128):
        mvec[:, q * 128:(q + 1) * 128] = mx[2 * q] + mx[2 * q + 1]
    live_total = jnp.sum(mvec[...], axis=1, keepdims=True)

    SB = 128

    def sq_step(i, carry):
        rows, e = exp_block(i // 2, i % 2)
        a0[i // 2, rows] = e * e
        return carry
    lax.fori_loop(0, 2 * (OWN // EC), sq_step, 0)

    def sink_pass(it):
        scale = (1.0 if it == 0 else live_total) * (1.0 / PROTOS)

        def step(blk, accs):
            rows = pl.ds(pl.multiple_of(blk * SB, SB), SB)
            out = []
            for view in range(2):
                a = a0[view, rows]
                w = mvec[...] if it == 0 else wvec[view]
                colsum = jnp.sum(a * w, axis=1, keepdims=True)
                v = scale / colsum
                if it == ITERS - 1:
                    vb[view, rows] = jnp.broadcast_to(v, (SB, 128))
                out.append(accs[view] + fold(a * v))
            return tuple(out)
        zero = jnp.zeros((8, NROW), F32)
        accs = lax.fori_loop(0, OWN // SB, step, (zero, zero))
        for view in range(2):
            rx[it, me, :, view * NROW:(view + 1) * NROW] = jnp.sum(accs[view], axis=0, keepdims=True)
        bcast(*r_args(it), wait=False)

    def sink_close(it):
        bcast(*r_args(it), wait=True)
        tot = rx[it, 0]
        for d in range(1, DEVS):
            tot = tot + rx[it, d]
        for view in range(2):
            wvec[view] = mvec[...] / tot[:, view * NROW:(view + 1) * NROW]

    sink_pass(0)
    lax.fori_loop(8, PROTOS // PC, sum_chunk, 0)
    row_sums_out()
    zforward((2,))
    sink_close(0)
    sink_pass(1)
    zfinish((2,))
    exp_views(2, 6)
    zforward((3,))
    sink_close(1)
    sink_pass(2)
    bcast(*l_args, wait=True)
    grad_scale = 1.0 / (TAU * live_total * (2 + 2 * (VIEWS - 2)))
    log_sum = jnp.zeros((1, NROW), F32)
    low = lax.broadcasted_iota(jnp.int32, (1, 128), 1) < ROWS
    for view in range(VIEWS):
        tot = jnp.concatenate([jnp.where(low, lx[2 * q, view], lx[2 * q + 1, view])
                               for q in range(NROW // 128)], axis=1)
        mult = 1.0 if view < 2 else 2.0
        acf[view] = (mult * grad_scale) * mvec[...] / tot
        log_sum = log_sum + mult * jnp.log(tot)
    log_sum = jnp.sum(log_sum * mvec[...], axis=1, keepdims=True)
    for view in range(2):
        for blk in range(OWN // 128):
            vt = vb[view, blk * 128:(blk + 1) * 128].T
            vx[me, view, :, blk * 128:(blk + 1) * 128] = vt[0:1, :]
    bcast(*v_args, wait=False)
    zfinish((3,))
    exp_views(6, 10)
    zforward((4,))
    zfinish((4,))
    exp_views(10, 12)
    sink_close(2)

    def acopy(src_dev, ch, half, to, kind):
        lo = src_dev * OWN + ch * KC
        if half is None:
            rows = pl.ds(pl.multiple_of(lo, KC), KC)
        else:
            rows = pl.ds(pl.multiple_of(lo + half * (KC // 2), KC // 2), KC // 2)
        return pltpu.make_async_remote_copy(
            src_ref=dcv.at[rows], dst_ref=dcv.at[rows], send_sem=asend.at[kind, ch],
            recv_sem=arecv.at[kind, ch], device_id=(to,), device_id_type=MESH)

    def dc_chunk(ch, carry):
        rows = pl.ds(pl.multiple_of(ch * KC, KC), KC)
        gq = []
        for view in range(2):
            v = jnp.concatenate([vb[view, rows]] * (NROW // 128), axis=1)
            gq.append((wvec[view] * grad_scale) * (v * a0[view, rows]))
        sub = [gq[1], gq[0]] + [gq[0] + gq[1]] * (VIEWS - 2)
        acc = None
        for view in range(VIEWS):
            g = (acf[view] * et[view, rows] - sub[view]).astype(BF16)
            part = jnp.dot(g, zall[view], preferred_element_type=F32)
            acc = part if acc is None else acc + part
        dcv[pl.ds(pl.multiple_of(own0 + ch * KC, KC), KC)] = acc
        acopy(me, ch, None, partner, 2).start()
        return carry

    def dc_sent(ch, carry):
        dc_chunk(ch, carry)
        acopy(me, ch, None, xn, 0).start()
        acopy(me, ch, None, yn, 1).start()
        return carry
    lax.fori_loop(0, SENT, dc_sent, 0)
    lax.fori_loop(SENT, NCH, dc_chunk, 0)

    def dc_again(i, carry):
        which = i % 3
        ch = SENT + i // 3
        dev = me + (1 - which % 2) * (2 - 4 * xpos) + ((which + 1) // 2) * (4 - 8 * ypos)
        lo = pl.multiple_of(dev * OWN + ch * KC, KC)
        cc = cv[pl.ds(lo, KC)]

        def expo(view):
            return jnp.exp(nt_dot(cc, zall[view]) * (1.0 / TAU))
        gq, es = [], []
        for view in range(2):
            vrow = vx[dev, view, :, pl.ds(pl.multiple_of(ch * KC, KC), KC)]
            v = jnp.concatenate([jnp.broadcast_to(vrow[:, j * 128:(j + 1) * 128], (128, 128)).T
                                 for j in range(KC // 128)], axis=0)
            v = jnp.concatenate([v] * (NROW // 128), axis=1)
            e = expo(view)
            es.append(e)
            gq.append((wvec[view] * grad_scale) * (v * (e * e)))
        sub = [gq[1], gq[0]] + [gq[0] + gq[1]] * (VIEWS - 2)
        acc = None
        for view in range(VIEWS):
            e = es[view] if view < 2 else expo(view)
            g = (acf[view] * e - sub[view]).astype(BF16)
            part = jnp.dot(g, zall[view], preferred_element_type=F32)
            acc = part if acc is None else acc + part
        dcv[pl.ds(lo, KC)] = acc
        acopy(dev, ch, None, partner, 5 + which).start()
        return carry

    def relay(ch):
        acopy(xn, ch, None, xn, 0).wait_recv()
        acopy(xn, ch, 0, yn, 3).start()
        acopy(xn, ch, None, partner, 5).start()
        acopy(yn, ch, None, yn, 1).wait_recv()
        acopy(yn, ch, 1, xn, 4).start()
        acopy(yn, ch, None, partner, 6).start()

    bcast(*v_args, wait=True)
    lax.fori_loop(0, 3, dc_again, 0)
    relay(0)
    lax.fori_loop(3, 3 * (NCH - SENT), dc_again, 0)
    relay(1)

    lanes = pl.ds(pl.multiple_of((me // 2) * 128, 128), 128)
    for view in range(VIEWS):
        cf[view:view + 1, :] = acf[view, :, lanes]
    for view in range(2):
        cf[VIEWS + view:VIEWS + view + 1, :] = wvec[view, :, lanes]
    ct[...] = cf[...].T
    own_cf = ct[pl.ds(pl.multiple_of(core * ROWS, ROWS), ROWS), :]
    for j in range(VIEWS + 2):
        ab[j] = jnp.broadcast_to(own_cf[:, j:j + 1], (ROWS, 128))

    dz_out[...] = jnp.zeros_like(dz_out)

    def wide(x):
        return jnp.concatenate([x] * (PC // 128), axis=1)

    def row_chunk(ch, acc):
        cols = pl.ds(pl.multiple_of(ch * PC, PC), PC)
        cc = cv[pl.ds(pl.multiple_of(ch * PC, PC), PC)]
        scores = nt_dot(zown[...].reshape(VIEWS * ROWS, DIM), cc)
        dev = ch // (OWN // PC)
        half = pl.ds(pl.multiple_of((ch % (OWN // PC)) * PC, PC), PC)
        e_large, q_large = [], []
        for view in range(2):
            e = jnp.exp(scores[view * ROWS:(view + 1) * ROWS] * (1.0 / TAU))
            q = wide(ab[VIEWS + view]) * (vx[dev, view, :, half] * (e * e))
            q_out[view, :, cols] = q
            e_large.append(e)
            q_large.append(q)
        q_sum = q_large[0] + q_large[1]
        gq_sum = q_sum * grad_scale
        parts = [(wide(ab[0]) * e_large[0] - q_large[1] * grad_scale).astype(BF16),
                 (wide(ab[1]) * e_large[1] - q_large[0] * grad_scale).astype(BF16)]
        s_sum = None
        for view in range(2, VIEWS):
            s = scores[view * ROWS:(view + 1) * ROWS]
            s_sum = s if s_sum is None else s_sum + s
            parts.append((wide(ab[view]) * jnp.exp(s * (1.0 / TAU)) - gq_sum).astype(BF16))
        dot = q_large[1] * scores[0:ROWS] + q_large[0] * scores[ROWS:2 * ROWS] + q_sum * s_sum
        dz = jnp.dot(jnp.concatenate(parts, axis=0), cc, preferred_element_type=F32)
        dz_out[...] += dz.reshape(VIEWS, ROWS, DIM)
        return acc + fold(dot)
    acc = lax.fori_loop(0, PROTOS // PC, row_chunk, jnp.zeros((8, PC), F32))
    cross = jnp.sum(jnp.sum(acc, axis=0, keepdims=True), axis=1, keepdims=True)
    px[me] = jnp.broadcast_to(cross, (1, 128))
    bcast(*p_args, wait=False)

    def gather_far(ch, carry):
        acopy(dg, ch, 0, yn, 3).wait_recv()
        acopy(dg, ch, 0, partner, 7).start()
        acopy(dg, ch, 1, xn, 4).wait_recv()
        acopy(dg, ch, 1, partner, 8).start()
        return carry

    bcast(*p_args, wait=True)
    tot = px[0]
    for d in range(1, DEVS):
        tot = tot + px[d]
    loss = -(tot[:, 0:1] * (1.0 / TAU) - log_sum) / (live_total * (2 + 2 * (VIEWS - 2)))
    loss_ref[...] = jnp.broadcast_to(loss, (1, 128))
    lax.fori_loop(0, SENT, gather_far, 0)

    def drain_sent(ch, carry):
        acopy(other(dg), ch, 0, partner, 7).wait_recv()
        acopy(other(dg), ch, 1, partner, 8).wait_recv()
        for kind in (0, 1):
            acopy(me, ch, None, partner, kind).wait_send()
        acopy(xn, ch, 0, yn, 3).wait_send()
        acopy(yn, ch, 1, xn, 4).wait_send()
        acopy(dg, ch, 0, partner, 7).wait_send()
        acopy(dg, ch, 1, partner, 8).wait_send()
        return carry

    def drain_again(ch, carry):
        acopy(other(dg), ch, None, partner, 7).wait_recv()
        acopy(dg, ch, None, partner, 7).wait_send()
        return carry

    def drain(ch, carry):
        acopy(partner, ch, None, partner, 2).wait_recv()
        acopy(other(xn), ch, None, partner, 5).wait_recv()
        acopy(other(yn), ch, None, partner, 6).wait_recv()
        acopy(me, ch, None, partner, 2).wait_send()
        acopy(xn, ch, None, partner, 5).wait_send()
        acopy(yn, ch, None, partner, 6).wait_send()
        return carry
    for unit in range(len(UNITS)):
        for kind in range(7):
            zcopy(unit, kind).wait_send()
    bcast_drain(*m_args)
    bcast_drain(*p_args)
    bcast_drain(*v_args)
    for it in range(ITERS):
        bcast_drain(*r_args(it))
    bcast_drain(*l_args)
    lax.fori_loop(0, NCH, drain, 0)
    lax.fori_loop(SENT, NCH, drain_again, 0)
    lax.fori_loop(0, SENT, drain_sent, 0)


def write_out(q_ref, loss_in, dz_ref, dc_ref, q1_hbm, q2_hbm, loss_ref, dz1_hbm, dz2_hbm, dzs_hbm, dc_hbm, sem):
    copies = []
    for src, dst in ((dc_ref, dc_hbm), (q_ref.at[0], q1_hbm), (q_ref.at[1], q2_hbm),
                     (dz_ref.at[pl.ds(2, VIEWS - 2)], dzs_hbm), (dz_ref.at[0], dz1_hbm), (dz_ref.at[1], dz2_hbm)):
        copies.append(pltpu.make_async_copy(src, dst, sem.at[len(copies)]))
        copies[-1].start()
    loss_ref[0, 0] = jnp.max(loss_in[:, 0:1])
    for copy in copies:
        copy.wait()


def local_step(z_one, z_two, z_small, protos, live_mask):
    vmem = pl.BlockSpec(memory_space=pltpu.VMEM)
    hbm = pl.BlockSpec(memory_space=pl.ANY)
    dma = pltpu.SemaphoreType.DMA
    views = VIEWS
    staged = pl.pallas_call(
        body,
        out_shape=(
            pltpu.VMEM((2, ROWS, PROTOS), F32),
            pltpu.VMEM((1, 128), F32),
            pltpu.VMEM((views, ROWS, DIM), F32),
            pltpu.VMEM((PROTOS, DIM), F32),
        ),
        in_specs=[vmem, vmem, vmem, vmem, hbm],
        out_specs=(vmem, vmem, vmem, vmem),
        scratch_shapes=[
            pltpu.VMEM((views, NROW, DIM), BF16),
            pltpu.VMEM((views, ROWS, DIM), BF16),
            pltpu.VMEM((PROTOS, DIM), BF16),
            pltpu.VMEM((views, OWN, NROW), F32),
            pltpu.VMEM((2, OWN, NROW), F32),
            pltpu.VMEM((2, OWN, 128), F32),
            pltpu.VMEM((DEVS, 2, 1, OWN), F32),
            pltpu.VMEM((ITERS, DEVS, 1, 2 * NROW), F32),
            pltpu.VMEM((DEVS, views, 1, 128), F32),
            pltpu.VMEM((DEVS, 1, 128), F32),
            pltpu.VMEM((DEVS, 1, 128), F32),
            pltpu.VMEM((1, NROW), F32),
            pltpu.VMEM((2, 1, NROW), F32),
            pltpu.VMEM((views, 1, NROW), F32),
            pltpu.VMEM((128, 128), F32),
            pltpu.VMEM((128, 128), F32),
            pltpu.VMEM((views + 2, ROWS, 128), F32),
            pltpu.VMEM((views * ROWS, 128), F32),
            dma(()),
            dma((7, 5)), dma((7, 5)),
            dma((ITERS, DEVS)), dma((ITERS, DEVS)),
            dma((DEVS,)), dma((DEVS,)),
            dma((DEVS,)), dma((DEVS,)),
            dma((2, DEVS)), dma((2, DEVS)),
            dma((9, NCH)), dma((9, NCH)),
        ],
        compiler_params=pltpu.CompilerParams(
            collective_id=0, has_side_effects=True, vmem_limit_bytes=48 * 1024 * 1024),
        name="swav_step",
    )(live_mask.reshape(1, ROWS), z_one, z_two, z_small, protos)
    q_one, q_two, loss, dz_one, dz_two, dz_small, d_protos = pl.pallas_call(
        write_out,
        out_shape=(
            jax.ShapeDtypeStruct((ROWS, PROTOS), F32),
            jax.ShapeDtypeStruct((ROWS, PROTOS), F32),
            jax.ShapeDtypeStruct((1, 1), F32),
            jax.ShapeDtypeStruct((ROWS, DIM), F32),
            jax.ShapeDtypeStruct((ROWS, DIM), F32),
            jax.ShapeDtypeStruct((views - 2, ROWS, DIM), F32),
            jax.ShapeDtypeStruct((PROTOS, DIM), F32),
        ),
        in_specs=[vmem] * 4,
        out_specs=(hbm, hbm, pl.BlockSpec(memory_space=pltpu.SMEM), hbm, hbm, hbm, hbm),
        scratch_shapes=[dma((6,))],
        compiler_params=pltpu.CompilerParams(vmem_limit_bytes=1024 * 1024),
        name="write_out",
    )(*staged)
    return q_one, q_two, loss[0, 0], dz_one, dz_two, dz_small, d_protos


def solution(mesh):
    row_spec = P("data", None)
    crop_spec = P(None, "data", None)
    return jax.shard_map(local_step, mesh=mesh,
                         in_specs=(row_spec, row_spec, crop_spec, P(None, None), P("data")),
                         out_specs=(row_spec, row_spec, P(), row_spec, row_spec, crop_spec, P(None, None)),
                         check_vma=False)
```

```python
import functools
import math

import jax
import jax.numpy as jnp
from jax import lax
from jax.experimental import pallas as pl
from jax.experimental.pallas import tpu as pltpu
from jax.sharding import PartitionSpec as P

EPS = 0.05
TAU = 0.1
ITERS = 3
DEVS = 8
ROWS = 64
NROW = ROWS * DEVS
PROTOS = 8192
DIM = 256
VIEWS = 12
OWN = PROTOS // DEVS
KC = 256
NCH = OWN // KC
PC = 512
MESH = pl.DeviceIdType.MESH
F32 = jnp.float32
BF16 = jnp.bfloat16
UNITS = ((0, 1), (1, 1), (2, 4), (6, 4), (10, 2))
SENT = 3
EC = 512


def nt_dot(a, b):
    return lax.dot_general(a, b, (((1,), (1,)), ((), ())), preferred_element_type=F32)


def body(mask_ref, z1_ref, z2_ref, zs_ref, c_hbm,
         q_out, loss_ref, dz_out, dcv,
         zall, zown, cv, et, a0, vb, vx, rx, lx, mx, px,
         mvec, wvec, acf, cf, ct, ab, lacc,
         csem, zsend, zrecv, rsend, rrecv, lsend, lrecv, vsend, vrecv, psend, precv,
         asend, arecv):
    me = lax.axis_index("data")
    core = me % 2
    xpos = (me // 2) % 2
    ypos = me // 4
    partner = me + 1 - 2 * core
    xn = me + 2 - 4 * xpos
    yn = me + 4 - 8 * ypos
    dg = xn + 4 - 8 * ypos

    def other(d):
        return d + 1 - 2 * core

    own0 = pl.multiple_of(me * OWN, OWN)
    c_copy = pltpu.make_async_copy(c_hbm, cv, csem)
    c_copy.start()

    barrier = pltpu.get_barrier_semaphore()
    for off in range(1, DEVS):
        pl.semaphore_signal(barrier, inc=1, device_id=((me + off) % DEVS,), device_id_type=MESH)

    mrow = mask_ref[...].astype(F32)
    sel = (lax.broadcasted_iota(jnp.int32, (ROWS, 128), 1)
           == lax.broadcasted_iota(jnp.int32, (ROWS, 128), 0) + ROWS * core)
    mplaced = jnp.dot(jnp.broadcast_to(mrow, (8, ROWS)).astype(BF16), sel.astype(BF16),
                      preferred_element_type=F32)
    mx[me] = mplaced[0:1, :]

    def zdst(unit, dev):
        lo, cnt = UNITS[unit]
        rows = pl.ds(pl.multiple_of(dev * ROWS, ROWS), ROWS)
        if cnt == 1:
            return zall.at[lo, rows]
        return zall.at[pl.ds(lo, cnt), rows]

    def zsrc(unit):
        lo, cnt = UNITS[unit]
        if unit == 0:
            return z1_ref
        if unit == 1:
            return z2_ref
        return zs_ref.at[pl.ds(lo - 2, cnt)]

    peers = (partner, xn, yn, dg)

    def zcopy(unit, kind):
        if kind < 4:
            return pltpu.make_async_remote_copy(
                src_ref=zsrc(unit), dst_ref=zdst(unit, me), send_sem=zsend.at[kind, unit],
                recv_sem=zrecv.at[kind, unit], device_id=(peers[kind],), device_id_type=MESH)
        dev = peers[kind - 3]
        return pltpu.make_async_remote_copy(
            src_ref=zdst(unit, dev), dst_ref=zdst(unit, dev), send_sem=zsend.at[kind, unit],
            recv_sem=zrecv.at[kind, unit], device_id=(partner,), device_id_type=MESH)

    def zwait(unit, kind):
        dev = peers[kind] if kind < 4 else other(peers[kind - 3])
        pltpu.make_async_remote_copy(
            src_ref=zsrc(unit), dst_ref=zdst(unit, dev), send_sem=zsend.at[kind, unit],
            recv_sem=zrecv.at[kind, unit], device_id=(partner,), device_id_type=MESH).wait_recv()

    def zstart(unit):
        for kind in (1, 2, 3, 0):
            zcopy(unit, kind).start()

    def zforward(units):
        for kind in (1, 2, 3):
            for unit in units:
                zwait(unit, kind)
                zcopy(unit, kind + 3).start()

    def zfinish(units):
        for unit in units:
            zwait(unit, 0)
        for kind in (4, 5, 6):
            for unit in units:
                zwait(unit, kind)

    def bcast(ref_of, send_sem, recv_sem, wait):
        for off in range(1, DEVS):
            dev = (me + off) % DEVS
            slot = dev if wait else me
            copy = pltpu.make_async_remote_copy(
                src_ref=ref_of(slot), dst_ref=ref_of(slot), send_sem=send_sem(off),
                recv_sem=recv_sem(slot), device_id=(dev,), device_id_type=MESH)
            if wait:
                copy.wait_recv()
            else:
                copy.start()

    def bcast_drain(ref_of, send_sem, recv_sem):
        for off in range(1, DEVS):
            pltpu.make_async_remote_copy(
                src_ref=ref_of(me), dst_ref=ref_of(me), send_sem=send_sem(off),
                recv_sem=recv_sem(me), device_id=((me + off) % DEVS,), device_id_type=MESH).wait_send()

    m_args = (lambda d: mx.at[d], lambda o: psend.at[1, o], lambda d: precv.at[1, d])
    p_args = (lambda d: px.at[d], lambda o: psend.at[0, o], lambda d: precv.at[0, d])
    v_args = (lambda d: vx.at[d], lambda o: vsend.at[o], lambda d: vrecv.at[d])

    def r_args(step):
        return (lambda d: rx.at[step, d], lambda o: rsend.at[step, o], lambda d: rrecv.at[step, d])

    l_args = (lambda d: lx.at[d], lambda o: lsend.at[o], lambda d: lrecv.at[d])

    my_rows = pl.ds(pl.multiple_of(me * ROWS, ROWS), ROWS)
    zall[0, my_rows] = z1_ref[...]
    zall[1, my_rows] = z2_ref[...]
    zown[0] = z1_ref[...]
    zown[1] = z2_ref[...]
    for view in range(VIEWS - 2):
        zall[2 + view, my_rows] = zs_ref[view]
        zown[2 + view] = zs_ref[view]

    pl.semaphore_wait(barrier, DEVS - 1)
    zstart(0)
    zstart(1)
    bcast(*m_args, wait=False)
    zstart(2)

    def fold(x):
        return jnp.sum(x.reshape(x.shape[0] // 8, 8, x.shape[1]), axis=0)

    def lane_fold(x):
        out = x[:, 0:128]
        for i in range(1, x.shape[1] // 128):
            out = out + x[:, i * 128:(i + 1) * 128]
        return out

    lacc[...] = jnp.zeros_like(lacc)
    c_copy.wait()

    def sum_chunk(ch, carry):
        cc = cv[pl.ds(pl.multiple_of(ch * PC, PC), PC)]
        scores = nt_dot(zown[...].reshape(VIEWS * ROWS, DIM), cc)
        lacc[...] += lane_fold(jnp.exp(scores * (1.0 / TAU)))
        return carry
    def row_sums_out():
        for view in range(VIEWS):
            la = lacc[view * ROWS:(view + 1) * ROWS]
            lx[me, view] = jnp.sum(jnp.concatenate([la, la], axis=0).T, axis=0, keepdims=True)
        bcast(*l_args, wait=False)

    def exp_block(view, ch):
        rows = pl.ds(pl.multiple_of(ch * EC, EC), EC)
        scores = nt_dot(cv[pl.ds(pl.multiple_of(own0 + ch * EC, EC), EC)], zall[view])
        e = jnp.exp(scores * (1.0 / TAU))
        et[view, rows] = e
        return rows, e

    def exp_views(lo, hi):
        def step(view, carry):
            for ch in range(OWN // EC):
                exp_block(view, ch)
            return carry
        lax.fori_loop(lo, hi, step, 0)

    lax.fori_loop(0, 6, sum_chunk, 0)
    zforward((0, 1))
    lax.fori_loop(6, 8, sum_chunk, 0)
    bcast(*m_args, wait=True)
    zfinish((0, 1))
    for q in range(NROW // 128):
        mvec[:, q * 128:(q + 1) * 128] = mx[2 * q] + mx[2 * q + 1]
    live_total = jnp.sum(mvec[...], axis=1, keepdims=True)

    SB = 128

    def sq_step(i, carry):
        rows, e = exp_block(i // 2, i % 2)
        a0[i // 2, rows] = e * e
        return carry
    lax.fori_loop(0, 2 * (OWN // EC), sq_step, 0)

    def sink_pass(it):
        scale = (1.0 if it == 0 else live_total) * (1.0 / PROTOS)

        def step(blk, accs):
            rows = pl.ds(pl.multiple_of(blk * SB, SB), SB)
            out = []
            for view in range(2):
                a = a0[view, rows]
                w = mvec[...] if it == 0 else wvec[view]
                colsum = jnp.sum(a * w, axis=1, keepdims=True)
                v = scale / colsum
                if it == ITERS - 1:
                    vb[view, rows] = jnp.broadcast_to(v, (SB, 128))
                out.append(accs[view] + fold(a * v))
            return tuple(out)
        zero = jnp.zeros((8, NROW), F32)
        accs = lax.fori_loop(0, OWN // SB, step, (zero, zero))
        for view in range(2):
            rx[it, me, :, view * NROW:(view + 1) * NROW] = jnp.sum(accs[view], axis=0, keepdims=True)
        bcast(*r_args(it), wait=False)

    def sink_close(it):
        bcast(*r_args(it), wait=True)
        tot = rx[it, 0]
        for d in range(1, DEVS):
            tot = tot + rx[it, d]
        for view in range(2):
            wvec[view] = mvec[...] / tot[:, view * NROW:(view + 1) * NROW]

    sink_pass(0)
    zstart(3)
    lax.fori_loop(8, PROTOS // PC, sum_chunk, 0)
    row_sums_out()
    zforward((2,))
    sink_close(0)
    sink_pass(1)
    zstart(4)
    zfinish((2,))
    exp_views(2, 6)
    zforward((3,))
    sink_close(1)
    sink_pass(2)
    bcast(*l_args, wait=True)
    grad_scale = 1.0 / (TAU * live_total * (2 + 2 * (VIEWS - 2)))
    log_sum = jnp.zeros((1, NROW), F32)
    low = lax.broadcasted_iota(jnp.int32, (1, 128), 1) < ROWS
    for view in range(VIEWS):
        tot = jnp.concatenate([jnp.where(low, lx[2 * q, view], lx[2 * q + 1, view])
                               for q in range(NROW // 128)], axis=1)
        mult = 1.0 if view < 2 else 2.0
        acf[view] = (mult * grad_scale) * mvec[...] / tot
        log_sum = log_sum + mult * jnp.log(tot)
    log_sum = jnp.sum(log_sum * mvec[...], axis=1, keepdims=True)
    for view in range(2):
        for blk in range(OWN // 128):
            vt = vb[view, blk * 128:(blk + 1) * 128].T
            vx[me, view, :, blk * 128:(blk + 1) * 128] = vt[0:1, :]
    bcast(*v_args, wait=False)
    zfinish((3,))
    exp_views(6, 10)
    zforward((4,))
    zfinish((4,))
    exp_views(10, 12)
    sink_close(2)

    def acopy(src_dev, ch, half, to, kind):
        lo = src_dev * OWN + ch * KC
        if half is None:
            rows = pl.ds(pl.multiple_of(lo, KC), KC)
        else:
            rows = pl.ds(pl.multiple_of(lo + half * (KC // 2), KC // 2), KC // 2)
        return pltpu.make_async_remote_copy(
            src_ref=dcv.at[rows], dst_ref=dcv.at[rows], send_sem=asend.at[kind, ch],
            recv_sem=arecv.at[kind, ch], device_id=(to,), device_id_type=MESH)

    def dc_chunk(ch, carry):
        rows = pl.ds(pl.multiple_of(ch * KC, KC), KC)
        gq = []
        for view in range(2):
            v = jnp.concatenate([vb[view, rows]] * (NROW // 128), axis=1)
            gq.append((wvec[view] * grad_scale) * (v * a0[view, rows]))
        sub = [gq[1], gq[0]] + [gq[0] + gq[1]] * (VIEWS - 2)
        acc = None
        for view in range(VIEWS):
            g = (acf[view] * et[view, rows] - sub[view]).astype(BF16)
            part = jnp.dot(g, zall[view], preferred_element_type=F32)
            acc = part if acc is None else acc + part
        dcv[pl.ds(pl.multiple_of(own0 + ch * KC, KC), KC)] = acc
        acopy(me, ch, None, partner, 2).start()
        return carry

    def dc_sent(ch, carry):
        dc_chunk(ch, carry)
        acopy(me, ch, None, xn, 0).start()
        acopy(me, ch, None, yn, 1).start()
        return carry
    lax.fori_loop(0, SENT, dc_sent, 0)
    lax.fori_loop(SENT, NCH, dc_chunk, 0)

    def dc_again(i, carry):
        which = i % 3
        ch = SENT + i // 3
        dev = me + (1 - which % 2) * (2 - 4 * xpos) + ((which + 1) // 2) * (4 - 8 * ypos)
        lo = pl.multiple_of(dev * OWN + ch * KC, KC)
        cc = cv[pl.ds(lo, KC)]

        def expo(view):
            return jnp.exp(nt_dot(cc, zall[view]) * (1.0 / TAU))
        gq, es = [], []
        for view in range(2):
            vrow = vx[dev, view, :, pl.ds(pl.multiple_of(ch * KC, KC), KC)]
            v = jnp.concatenate([jnp.broadcast_to(vrow[:, j * 128:(j + 1) * 128], (128, 128)).T
                                 for j in range(KC // 128)], axis=0)
            v = jnp.concatenate([v] * (NROW // 128), axis=1)
            e = expo(view)
            es.append(e)
            gq.append((wvec[view] * grad_scale) * (v * (e * e)))
        sub = [gq[1], gq[0]] + [gq[0] + gq[1]] * (VIEWS - 2)
        acc = None
        for view in range(VIEWS):
            e = es[view] if view < 2 else expo(view)
            g = (acf[view] * e - sub[view]).astype(BF16)
            part = jnp.dot(g, zall[view], preferred_element_type=F32)
            acc = part if acc is None else acc + part
        dcv[pl.ds(lo, KC)] = acc
        acopy(dev, ch, None, partner, 5 + which).start()
        return carry

    def relay(ch):
        acopy(xn, ch, None, xn, 0).wait_recv()
        acopy(xn, ch, 0, yn, 3).start()
        acopy(xn, ch, None, partner, 5).start()
        acopy(yn, ch, None, yn, 1).wait_recv()
        acopy(yn, ch, 1, xn, 4).start()
        acopy(yn, ch, None, partner, 6).start()

    bcast(*v_args, wait=True)
    lax.fori_loop(0, 3 * (NCH - SENT), dc_again, 0)
    relay(0)

    lanes = pl.ds(pl.multiple_of((me // 2) * 128, 128), 128)
    for view in range(VIEWS):
        cf[view:view + 1, :] = acf[view, :, lanes]
    for view in range(2):
        cf[VIEWS + view:VIEWS + view + 1, :] = wvec[view, :, lanes]
    ct[...] = cf[...].T
    own_cf = ct[pl.ds(pl.multiple_of(core * ROWS, ROWS), ROWS), :]
    for j in range(VIEWS + 2):
        ab[j] = jnp.broadcast_to(own_cf[:, j:j + 1], (ROWS, 128))

    dz_out[...] = jnp.zeros_like(dz_out)

    def wide(x):
        return jnp.concatenate([x] * (PC // 128), axis=1)

    def row_chunk(ch, acc):
        cols = pl.ds(pl.multiple_of(ch * PC, PC), PC)
        cc = cv[pl.ds(pl.multiple_of(ch * PC, PC), PC)]
        scores = nt_dot(zown[...].reshape(VIEWS * ROWS, DIM), cc)
        dev = ch // (OWN // PC)
        half = pl.ds(pl.multiple_of((ch % (OWN // PC)) * PC, PC), PC)
        e_large, q_large = [], []
        for view in range(2):
            e = jnp.exp(scores[view * ROWS:(view + 1) * ROWS] * (1.0 / TAU))
            q = wide(ab[VIEWS + view]) * (vx[dev, view, :, half] * (e * e))
            q_out[view, :, cols] = q
            e_large.append(e)
            q_large.append(q)
        q_sum = q_large[0] + q_large[1]
        gq_sum = q_sum * grad_scale
        parts = [(wide(ab[0]) * e_large[0] - q_large[1] * grad_scale).astype(BF16),
                 (wide(ab[1]) * e_large[1] - q_large[0] * grad_scale).astype(BF16)]
        s_sum = None
        for view in range(2, VIEWS):
            s = scores[view * ROWS:(view + 1) * ROWS]
            s_sum = s if s_sum is None else s_sum + s
            parts.append((wide(ab[view]) * jnp.exp(s * (1.0 / TAU)) - gq_sum).astype(BF16))
        dot = q_large[1] * scores[0:ROWS] + q_large[0] * scores[ROWS:2 * ROWS] + q_sum * s_sum
        dz = jnp.dot(jnp.concatenate(parts, axis=0), cc, preferred_element_type=F32)
        dz_out[...] += dz.reshape(VIEWS, ROWS, DIM)
        return acc + fold(dot)
    acc = lax.fori_loop(0, PROTOS // PC // 2, row_chunk, jnp.zeros((8, PC), F32))
    relay(1)
    acc = lax.fori_loop(PROTOS // PC // 2, PROTOS // PC, row_chunk, acc)
    relay(2)
    cross = jnp.sum(jnp.sum(acc, axis=0, keepdims=True), axis=1, keepdims=True)
    px[me] = jnp.broadcast_to(cross, (1, 128))
    bcast(*p_args, wait=False)

    def gather_far(ch, carry):
        acopy(dg, ch, 0, yn, 3).wait_recv()
        acopy(dg, ch, 0, partner, 7).start()
        acopy(dg, ch, 1, xn, 4).wait_recv()
        acopy(dg, ch, 1, partner, 8).start()
        return carry

    bcast(*p_args, wait=True)
    tot = px[0]
    for d in range(1, DEVS):
        tot = tot + px[d]
    loss = -(tot[:, 0:1] * (1.0 / TAU) - log_sum) / (live_total * (2 + 2 * (VIEWS - 2)))
    loss_ref[...] = jnp.broadcast_to(loss, (1, 128))
    lax.fori_loop(0, SENT, gather_far, 0)

    def drain_sent(ch, carry):
        acopy(other(dg), ch, 0, partner, 7).wait_recv()
        acopy(other(dg), ch, 1, partner, 8).wait_recv()
        for kind in (0, 1):
            acopy(me, ch, None, partner, kind).wait_send()
        acopy(xn, ch, 0, yn, 3).wait_send()
        acopy(yn, ch, 1, xn, 4).wait_send()
        acopy(dg, ch, 0, partner, 7).wait_send()
        acopy(dg, ch, 1, partner, 8).wait_send()
        return carry

    def drain_again(ch, carry):
        acopy(other(dg), ch, None, partner, 7).wait_recv()
        acopy(dg, ch, None, partner, 7).wait_send()
        return carry

    def drain(ch, carry):
        acopy(partner, ch, None, partner, 2).wait_recv()
        acopy(other(xn), ch, None, partner, 5).wait_recv()
        acopy(other(yn), ch, None, partner, 6).wait_recv()
        acopy(me, ch, None, partner, 2).wait_send()
        acopy(xn, ch, None, partner, 5).wait_send()
        acopy(yn, ch, None, partner, 6).wait_send()
        return carry
    for unit in range(len(UNITS)):
        for kind in range(7):
            zcopy(unit, kind).wait_send()
    bcast_drain(*m_args)
    bcast_drain(*p_args)
    bcast_drain(*v_args)
    for it in range(ITERS):
        bcast_drain(*r_args(it))
    bcast_drain(*l_args)
    lax.fori_loop(0, NCH, drain, 0)
    lax.fori_loop(SENT, NCH, drain_again, 0)
    lax.fori_loop(0, SENT, drain_sent, 0)


def write_out(q_ref, loss_in, dz_ref, dc_ref, q1_hbm, q2_hbm, loss_ref, dz1_hbm, dz2_hbm, dzs_hbm, dc_hbm, sem):
    copies = []
    for src, dst in ((dc_ref, dc_hbm), (q_ref.at[0], q1_hbm), (q_ref.at[1], q2_hbm),
                     (dz_ref.at[pl.ds(2, VIEWS - 2)], dzs_hbm), (dz_ref.at[0], dz1_hbm), (dz_ref.at[1], dz2_hbm)):
        copies.append(pltpu.make_async_copy(src, dst, sem.at[len(copies)]))
        copies[-1].start()
    loss_ref[0, 0] = jnp.max(loss_in[:, 0:1])
    for copy in copies:
        copy.wait()


def local_step(z_one, z_two, z_small, protos, live_mask):
    vmem = pl.BlockSpec(memory_space=pltpu.VMEM)
    hbm = pl.BlockSpec(memory_space=pl.ANY)
    dma = pltpu.SemaphoreType.DMA
    views = VIEWS
    staged = pl.pallas_call(
        body,
        out_shape=(
            pltpu.VMEM((2, ROWS, PROTOS), F32),
            pltpu.VMEM((1, 128), F32),
            pltpu.VMEM((views, ROWS, DIM), F32),
            pltpu.VMEM((PROTOS, DIM), F32),
        ),
        in_specs=[vmem, vmem, vmem, vmem, hbm],
        out_specs=(vmem, vmem, vmem, vmem),
        scratch_shapes=[
            pltpu.VMEM((views, NROW, DIM), BF16),
            pltpu.VMEM((views, ROWS, DIM), BF16),
            pltpu.VMEM((PROTOS, DIM), BF16),
            pltpu.VMEM((views, OWN, NROW), F32),
            pltpu.VMEM((2, OWN, NROW), F32),
            pltpu.VMEM((2, OWN, 128), F32),
            pltpu.VMEM((DEVS, 2, 1, OWN), F32),
            pltpu.VMEM((ITERS, DEVS, 1, 2 * NROW), F32),
            pltpu.VMEM((DEVS, views, 1, 128), F32),
            pltpu.VMEM((DEVS, 1, 128), F32),
            pltpu.VMEM((DEVS, 1, 128), F32),
            pltpu.VMEM((1, NROW), F32),
            pltpu.VMEM((2, 1, NROW), F32),
            pltpu.VMEM((views, 1, NROW), F32),
            pltpu.VMEM((128, 128), F32),
            pltpu.VMEM((128, 128), F32),
            pltpu.VMEM((views + 2, ROWS, 128), F32),
            pltpu.VMEM((views * ROWS, 128), F32),
            dma(()),
            dma((7, 5)), dma((7, 5)),
            dma((ITERS, DEVS)), dma((ITERS, DEVS)),
            dma((DEVS,)), dma((DEVS,)),
            dma((DEVS,)), dma((DEVS,)),
            dma((2, DEVS)), dma((2, DEVS)),
            dma((9, NCH)), dma((9, NCH)),
        ],
        compiler_params=pltpu.CompilerParams(
            collective_id=0, has_side_effects=True, vmem_limit_bytes=48 * 1024 * 1024),
        name="swav_step",
    )(live_mask.reshape(1, ROWS), z_one, z_two, z_small, protos)
    q_one, q_two, loss, dz_one, dz_two, dz_small, d_protos = pl.pallas_call(
        write_out,
        out_shape=(
            jax.ShapeDtypeStruct((ROWS, PROTOS), F32),
            jax.ShapeDtypeStruct((ROWS, PROTOS), F32),
            jax.ShapeDtypeStruct((1, 1), F32),
            jax.ShapeDtypeStruct((ROWS, DIM), F32),
            jax.ShapeDtypeStruct((ROWS, DIM), F32),
            jax.ShapeDtypeStruct((views - 2, ROWS, DIM), F32),
            jax.ShapeDtypeStruct((PROTOS, DIM), F32),
        ),
        in_specs=[vmem] * 4,
        out_specs=(hbm, hbm, pl.BlockSpec(memory_space=pltpu.SMEM), hbm, hbm, hbm, hbm),
        scratch_shapes=[dma((6,))],
        compiler_params=pltpu.CompilerParams(vmem_limit_bytes=1024 * 1024),
        name="write_out",
    )(*staged)
    return q_one, q_two, loss[0, 0], dz_one, dz_two, dz_small, d_protos


def solution(mesh):
    row_spec = P("data", None)
    crop_spec = P(None, "data", None)
    return jax.shard_map(local_step, mesh=mesh,
                         in_specs=(row_spec, row_spec, crop_spec, P(None, None), P("data")),
                         out_specs=(row_spec, row_spec, P(), row_spec, row_spec, crop_spec, P(None, None)),
                         check_vma=False)
```

```python
import functools
import math

import jax
import jax.numpy as jnp
from jax import lax
from jax.experimental import pallas as pl
from jax.experimental.pallas import tpu as pltpu
from jax.sharding import PartitionSpec as P

EPS = 0.05
TAU = 0.1
ITERS = 3
DEVS = 8
ROWS = 64
NROW = ROWS * DEVS
PROTOS = 8192
DIM = 256
VIEWS = 12
OWN = PROTOS // DEVS
KC = 256
NCH = OWN // KC
PC = 512
MESH = pl.DeviceIdType.MESH
F32 = jnp.float32
BF16 = jnp.bfloat16
UNITS = ((0, 1), (1, 1), (2, 4), (6, 4), (10, 2))
SENT = 3
EC = 512


def nt_dot(a, b):
    return lax.dot_general(a, b, (((1,), (1,)), ((), ())), preferred_element_type=F32)


def body(mask_ref, z1_hbm, z2_hbm, zs_hbm, c_hbm,
         q_out, loss_ref, dz_out, dcv,
         zall, zown, cv, et, a0, vb, vx, rx, lx, mx, px,
         mvec, wvec, acf, cf, ct, ab, lacc,
         csem, isem, zsend, zrecv, rsend, rrecv, lsend, lrecv, vsend, vrecv, psend, precv,
         asend, arecv):
    me = lax.axis_index("data")
    core = me % 2
    xpos = (me // 2) % 2
    ypos = me // 4
    partner = me + 1 - 2 * core
    xn = me + 2 - 4 * xpos
    yn = me + 4 - 8 * ypos
    dg = xn + 4 - 8 * ypos

    def other(d):
        return d + 1 - 2 * core

    my_rows = pl.ds(pl.multiple_of(me * ROWS, ROWS), ROWS)
    small = pl.ds(2, VIEWS - 2)
    own_copies = []
    for src, dst in ((z1_hbm, zown.at[0]), (z2_hbm, zown.at[1]), (zs_hbm, zown.at[small]),
                     (z1_hbm, zall.at[0, my_rows]), (z2_hbm, zall.at[1, my_rows]), (zs_hbm, zall.at[small, my_rows])):
        own_copies.append(pltpu.make_async_copy(src, dst, isem.at[len(own_copies)]))
        own_copies[-1].start()
    own0 = pl.multiple_of(me * OWN, OWN)
    c_copy = pltpu.make_async_copy(c_hbm, cv, csem)
    c_copy.start()

    barrier = pltpu.get_barrier_semaphore()
    for off in range(1, DEVS):
        pl.semaphore_signal(barrier, inc=1, device_id=((me + off) % DEVS,), device_id_type=MESH)

    mrow = mask_ref[...].astype(F32)
    sel = (lax.broadcasted_iota(jnp.int32, (ROWS, 128), 1)
           == lax.broadcasted_iota(jnp.int32, (ROWS, 128), 0) + ROWS * core)
    mplaced = jnp.dot(jnp.broadcast_to(mrow, (8, ROWS)).astype(BF16), sel.astype(BF16),
                      preferred_element_type=F32)
    mx[me] = mplaced[0:1, :]

    def zdst(unit, dev):
        lo, cnt = UNITS[unit]
        rows = pl.ds(pl.multiple_of(dev * ROWS, ROWS), ROWS)
        if cnt == 1:
            return zall.at[lo, rows]
        return zall.at[pl.ds(lo, cnt), rows]

    def zsrc(unit):
        lo, cnt = UNITS[unit]
        return zown.at[lo] if cnt == 1 else zown.at[pl.ds(lo, cnt)]

    peers = (partner, xn, yn, dg)

    def zcopy(unit, kind):
        if kind < 4:
            return pltpu.make_async_remote_copy(
                src_ref=zsrc(unit), dst_ref=zdst(unit, me), send_sem=zsend.at[kind, unit],
                recv_sem=zrecv.at[kind, unit], device_id=(peers[kind],), device_id_type=MESH)
        dev = peers[kind - 3]
        return pltpu.make_async_remote_copy(
            src_ref=zdst(unit, dev), dst_ref=zdst(unit, dev), send_sem=zsend.at[kind, unit],
            recv_sem=zrecv.at[kind, unit], device_id=(partner,), device_id_type=MESH)

    def zwait(unit, kind):
        dev = peers[kind] if kind < 4 else other(peers[kind - 3])
        pltpu.make_async_remote_copy(
            src_ref=zsrc(unit), dst_ref=zdst(unit, dev), send_sem=zsend.at[kind, unit],
            recv_sem=zrecv.at[kind, unit], device_id=(partner,), device_id_type=MESH).wait_recv()

    def zstart(unit):
        for kind in (1, 2, 3, 0):
            zcopy(unit, kind).start()

    def zforward(units):
        for kind in (1, 2, 3):
            for unit in units:
                zwait(unit, kind)
                zcopy(unit, kind + 3).start()

    def zfinish(units):
        for unit in units:
            zwait(unit, 0)
        for kind in (4, 5, 6):
            for unit in units:
                zwait(unit, kind)

    def bcast(ref_of, send_sem, recv_sem, wait):
        for off in range(1, DEVS):
            dev = (me + off) % DEVS
            slot = dev if wait else me
            copy = pltpu.make_async_remote_copy(
                src_ref=ref_of(slot), dst_ref=ref_of(slot), send_sem=send_sem(off),
                recv_sem=recv_sem(slot), device_id=(dev,), device_id_type=MESH)
            if wait:
                copy.wait_recv()
            else:
                copy.start()

    def bcast_drain(ref_of, send_sem, recv_sem):
        for off in range(1, DEVS):
            pltpu.make_async_remote_copy(
                src_ref=ref_of(me), dst_ref=ref_of(me), send_sem=send_sem(off),
                recv_sem=recv_sem(me), device_id=((me + off) % DEVS,), device_id_type=MESH).wait_send()

    m_args = (lambda d: mx.at[d], lambda o: psend.at[1, o], lambda d: precv.at[1, d])
    p_args = (lambda d: px.at[d], lambda o: psend.at[0, o], lambda d: precv.at[0, d])
    v_args = (lambda d: vx.at[d], lambda o: vsend.at[o], lambda d: vrecv.at[d])

    def r_args(step):
        return (lambda d: rx.at[step, d], lambda o: rsend.at[step, o], lambda d: rrecv.at[step, d])

    l_args = (lambda d: lx.at[d], lambda o: lsend.at[o], lambda d: lrecv.at[d])

    for copy in own_copies:
        copy.wait()
    pl.semaphore_wait(barrier, DEVS - 1)
    zstart(0)
    zstart(1)
    bcast(*m_args, wait=False)
    zstart(2)

    def fold(x):
        return jnp.sum(x.reshape(x.shape[0] // 8, 8, x.shape[1]), axis=0)

    def lane_fold(x):
        out = x[:, 0:128]
        for i in range(1, x.shape[1] // 128):
            out = out + x[:, i * 128:(i + 1) * 128]
        return out

    lacc[...] = jnp.zeros_like(lacc)
    c_copy.wait()

    def sum_chunk(ch, carry):
        cc = cv[pl.ds(pl.multiple_of(ch * PC, PC), PC)]
        scores = nt_dot(zown[...].reshape(VIEWS * ROWS, DIM), cc)
        lacc[...] += lane_fold(jnp.exp(scores * (1.0 / TAU)))
        return carry
    def row_sums_out():
        for view in range(VIEWS):
            la = lacc[view * ROWS:(view + 1) * ROWS]
            lx[me, view] = jnp.sum(jnp.concatenate([la, la], axis=0).T, axis=0, keepdims=True)
        bcast(*l_args, wait=False)

    def exp_block(view, ch):
        rows = pl.ds(pl.multiple_of(ch * EC, EC), EC)
        scores = nt_dot(cv[pl.ds(pl.multiple_of(own0 + ch * EC, EC), EC)], zall[view])
        e = jnp.exp(scores * (1.0 / TAU))
        et[view, rows] = e
        return rows, e

    def exp_views(lo, hi):
        def step(view, carry):
            for ch in range(OWN // EC):
                exp_block(view, ch)
            return carry
        lax.fori_loop(lo, hi, step, 0)

    lax.fori_loop(0, 6, sum_chunk, 0)
    zforward((0, 1))
    lax.fori_loop(6, 8, sum_chunk, 0)
    bcast(*m_args, wait=True)
    zfinish((0, 1))
    for q in range(NROW // 128):
        mvec[:, q * 128:(q + 1) * 128] = mx[2 * q] + mx[2 * q + 1]
    live_total = jnp.sum(mvec[...], axis=1, keepdims=True)

    SB = 128

    def sq_step(i, carry):
        rows, e = exp_block(i // 2, i % 2)
        a0[i // 2, rows] = e * e
        return carry
    lax.fori_loop(0, 2 * (OWN // EC), sq_step, 0)

    def sink_pass(it):
        scale = (1.0 if it == 0 else live_total) * (1.0 / PROTOS)

        def step(blk, accs):
            rows = pl.ds(pl.multiple_of(blk * SB, SB), SB)
            out = []
            for view in range(2):
                a = a0[view, rows]
                w = mvec[...] if it == 0 else wvec[view]
                colsum = jnp.sum(a * w, axis=1, keepdims=True)
                v = scale / colsum
                if it == ITERS - 1:
                    vb[view, rows] = jnp.broadcast_to(v, (SB, 128))
                out.append(accs[view] + fold(a * v))
            return tuple(out)
        zero = jnp.zeros((8, NROW), F32)
        accs = lax.fori_loop(0, OWN // SB, step, (zero, zero))
        for view in range(2):
            rx[it, me, :, view * NROW:(view + 1) * NROW] = jnp.sum(accs[view], axis=0, keepdims=True)
        bcast(*r_args(it), wait=False)

    def sink_close(it):
        bcast(*r_args(it), wait=True)
        tot = rx[it, 0]
        for d in range(1, DEVS):
            tot = tot + rx[it, d]
        for view in range(2):
            wvec[view] = mvec[...] / tot[:, view * NROW:(view + 1) * NROW]

    sink_pass(0)
    zstart(3)
    lax.fori_loop(8, PROTOS // PC, sum_chunk, 0)
    row_sums_out()
    zforward((2,))
    sink_close(0)
    sink_pass(1)
    zstart(4)
    zfinish((2,))
    exp_views(2, 6)
    zforward((3,))
    sink_close(1)
    sink_pass(2)
    bcast(*l_args, wait=True)
    grad_scale = 1.0 / (TAU * live_total * (2 + 2 * (VIEWS - 2)))
    log_sum = jnp.zeros((1, NROW), F32)
    low = lax.broadcasted_iota(jnp.int32, (1, 128), 1) < ROWS
    for view in range(VIEWS):
        tot = jnp.concatenate([jnp.where(low, lx[2 * q, view], lx[2 * q + 1, view])
                               for q in range(NROW // 128)], axis=1)
        mult = 1.0 if view < 2 else 2.0
        acf[view] = (mult * grad_scale) * mvec[...] / tot
        log_sum = log_sum + mult * jnp.log(tot)
    log_sum = jnp.sum(log_sum * mvec[...], axis=1, keepdims=True)
    for view in range(2):
        for blk in range(OWN // 128):
            vt = vb[view, blk * 128:(blk + 1) * 128].T
            vx[me, view, :, blk * 128:(blk + 1) * 128] = vt[0:1, :]
    bcast(*v_args, wait=False)
    zfinish((3,))
    exp_views(6, 10)
    zforward((4,))
    zfinish((4,))
    exp_views(10, 12)
    sink_close(2)

    def acopy(src_dev, ch, half, to, kind):
        lo = src_dev * OWN + ch * KC
        if half is None:
            rows = pl.ds(pl.multiple_of(lo, KC), KC)
        else:
            rows = pl.ds(pl.multiple_of(lo + half * (KC // 2), KC // 2), KC // 2)
        return pltpu.make_async_remote_copy(
            src_ref=dcv.at[rows], dst_ref=dcv.at[rows], send_sem=asend.at[kind, ch],
            recv_sem=arecv.at[kind, ch], device_id=(to,), device_id_type=MESH)

    def dc_chunk(ch, carry):
        rows = pl.ds(pl.multiple_of(ch * KC, KC), KC)
        gq = []
        for view in range(2):
            v = jnp.concatenate([vb[view, rows]] * (NROW // 128), axis=1)
            gq.append((wvec[view] * grad_scale) * (v * a0[view, rows]))
        sub = [gq[1], gq[0]] + [gq[0] + gq[1]] * (VIEWS - 2)
        acc = None
        for view in range(VIEWS):
            g = (acf[view] * et[view, rows] - sub[view]).astype(BF16)
            part = jnp.dot(g, zall[view], preferred_element_type=F32)
            acc = part if acc is None else acc + part
        dcv[pl.ds(pl.multiple_of(own0 + ch * KC, KC), KC)] = acc
        acopy(me, ch, None, partner, 2).start()
        return carry

    def dc_sent(ch, carry):
        dc_chunk(ch, carry)
        acopy(me, ch, None, xn, 0).start()
        acopy(me, ch, None, yn, 1).start()
        return carry
    lax.fori_loop(0, SENT, dc_sent, 0)
    lax.fori_loop(SENT, NCH, dc_chunk, 0)

    def dc_again(i, carry):
        which = i % 3
        ch = SENT + i // 3
        dev = me + (1 - which % 2) * (2 - 4 * xpos) + ((which + 1) // 2) * (4 - 8 * ypos)
        lo = pl.multiple_of(dev * OWN + ch * KC, KC)
        cc = cv[pl.ds(lo, KC)]

        def expo(view):
            return jnp.exp(nt_dot(cc, zall[view]) * (1.0 / TAU))
        gq, es = [], []
        for view in range(2):
            vrow = vx[dev, view, :, pl.ds(pl.multiple_of(ch * KC, KC), KC)]
            v = jnp.concatenate([jnp.broadcast_to(vrow[:, j * 128:(j + 1) * 128], (128, 128)).T
                                 for j in range(KC // 128)], axis=0)
            v = jnp.concatenate([v] * (NROW // 128), axis=1)
            e = expo(view)
            es.append(e)
            gq.append((wvec[view] * grad_scale) * (v * (e * e)))
        sub = [gq[1], gq[0]] + [gq[0] + gq[1]] * (VIEWS - 2)
        acc = None
        for view in range(VIEWS):
            e = es[view] if view < 2 else expo(view)
            g = (acf[view] * e - sub[view]).astype(BF16)
            part = jnp.dot(g, zall[view], preferred_element_type=F32)
            acc = part if acc is None else acc + part
        dcv[pl.ds(lo, KC)] = acc
        acopy(dev, ch, None, partner, 5 + which).start()
        return carry

    def relay(ch):
        acopy(xn, ch, None, xn, 0).wait_recv()
        acopy(xn, ch, 0, yn, 3).start()
        acopy(xn, ch, None, partner, 5).start()
        acopy(yn, ch, None, yn, 1).wait_recv()
        acopy(yn, ch, 1, xn, 4).start()
        acopy(yn, ch, None, partner, 6).start()

    bcast(*v_args, wait=True)
    lax.fori_loop(0, 2, dc_again, 0)
    relay(0)
    lax.fori_loop(2, 3, dc_again, 0)
    relay(1)

    lanes = pl.ds(pl.multiple_of((me // 2) * 128, 128), 128)
    for view in range(VIEWS):
        cf[view:view + 1, :] = acf[view, :, lanes]
    for view in range(2):
        cf[VIEWS + view:VIEWS + view + 1, :] = wvec[view, :, lanes]
    ct[...] = cf[...].T
    own_cf = ct[pl.ds(pl.multiple_of(core * ROWS, ROWS), ROWS), :]
    for j in range(VIEWS + 2):
        ab[j] = jnp.broadcast_to(own_cf[:, j:j + 1], (ROWS, 128))

    dz_out[...] = jnp.zeros_like(dz_out)

    def wide(x):
        return jnp.concatenate([x] * (PC // 128), axis=1)

    def row_chunk(ch, acc):
        cols = pl.ds(pl.multiple_of(ch * PC, PC), PC)
        cc = cv[pl.ds(pl.multiple_of(ch * PC, PC), PC)]
        scores = nt_dot(zown[...].reshape(VIEWS * ROWS, DIM), cc)
        dev = ch // (OWN // PC)
        half = pl.ds(pl.multiple_of((ch % (OWN // PC)) * PC, PC), PC)
        e_large, q_large = [], []
        for view in range(2):
            e = jnp.exp(scores[view * ROWS:(view + 1) * ROWS] * (1.0 / TAU))
            q = wide(ab[VIEWS + view]) * (vx[dev, view, :, half] * (e * e))
            q_out[view, :, cols] = q
            e_large.append(e)
            q_large.append(q)
        q_sum = q_large[0] + q_large[1]
        gq_sum = q_sum * grad_scale
        parts = [(wide(ab[0]) * e_large[0] - q_large[1] * grad_scale).astype(BF16),
                 (wide(ab[1]) * e_large[1] - q_large[0] * grad_scale).astype(BF16)]
        s_sum = None
        for view in range(2, VIEWS):
            s = scores[view * ROWS:(view + 1) * ROWS]
            s_sum = s if s_sum is None else s_sum + s
            parts.append((wide(ab[view]) * jnp.exp(s * (1.0 / TAU)) - gq_sum).astype(BF16))
        dot = q_large[1] * scores[0:ROWS] + q_large[0] * scores[ROWS:2 * ROWS] + q_sum * s_sum
        dz = jnp.dot(jnp.concatenate(parts, axis=0), cc, preferred_element_type=F32)
        dz_out[...] += dz.reshape(VIEWS, ROWS, DIM)
        return acc + fold(dot)
    def far(ch):
        acopy(dg, ch, 0, yn, 3).wait_recv()
        acopy(dg, ch, 0, partner, 7).start()
        acopy(dg, ch, 1, xn, 4).wait_recv()
        acopy(dg, ch, 1, partner, 8).start()

    acc = lax.fori_loop(0, 6, row_chunk, jnp.zeros((8, PC), F32))
    relay(2)
    acc = lax.fori_loop(6, 12, row_chunk, acc)
    far(0)
    far(1)
    acc = lax.fori_loop(12, PROTOS // PC, row_chunk, acc)
    cross = jnp.sum(jnp.sum(acc, axis=0, keepdims=True), axis=1, keepdims=True)
    px[me] = jnp.broadcast_to(cross, (1, 128))
    bcast(*p_args, wait=False)

    bcast(*p_args, wait=True)
    tot = px[0]
    for d in range(1, DEVS):
        tot = tot + px[d]
    loss = -(tot[:, 0:1] * (1.0 / TAU) - log_sum) / (live_total * (2 + 2 * (VIEWS - 2)))
    loss_ref[...] = jnp.broadcast_to(loss, (1, 128))
    far(2)

    def drain_sent(ch, carry):
        acopy(other(dg), ch, 0, partner, 7).wait_recv()
        acopy(other(dg), ch, 1, partner, 8).wait_recv()
        for kind in (0, 1):
            acopy(me, ch, None, partner, kind).wait_send()
        acopy(xn, ch, 0, yn, 3).wait_send()
        acopy(yn, ch, 1, xn, 4).wait_send()
        acopy(dg, ch, 0, partner, 7).wait_send()
        acopy(dg, ch, 1, partner, 8).wait_send()
        return carry

    def drain_again(ch, carry):
        acopy(other(dg), ch, None, partner, 7).wait_recv()
        acopy(dg, ch, None, partner, 7).wait_send()
        return carry

    def drain(ch, carry):
        acopy(partner, ch, None, partner, 2).wait_recv()
        acopy(other(xn), ch, None, partner, 5).wait_recv()
        acopy(other(yn), ch, None, partner, 6).wait_recv()
        acopy(me, ch, None, partner, 2).wait_send()
        acopy(xn, ch, None, partner, 5).wait_send()
        acopy(yn, ch, None, partner, 6).wait_send()
        return carry
    for unit in range(len(UNITS)):
        for kind in range(7):
            zcopy(unit, kind).wait_send()
    bcast_drain(*m_args)
    bcast_drain(*p_args)
    bcast_drain(*v_args)
    for it in range(ITERS):
        bcast_drain(*r_args(it))
    bcast_drain(*l_args)
    lax.fori_loop(0, NCH, drain, 0)
    lax.fori_loop(SENT, NCH, drain_again, 0)
    lax.fori_loop(0, SENT, drain_sent, 0)


def write_out(q_ref, loss_in, dz_ref, dc_ref, q1_hbm, q2_hbm, loss_ref, dz1_hbm, dz2_hbm, dzs_hbm, dc_hbm, sem):
    copies = []
    pairs = []
    for i in range(8):
        rows = pl.ds(i * (PROTOS // 8), PROTOS // 8)
        pairs.append((dc_ref.at[rows], dc_hbm.at[rows]))
    for i in range(4):
        rows = pl.ds(i * (ROWS // 4), ROWS // 4)
        pairs.append((q_ref.at[0, rows], q1_hbm.at[rows]))
        pairs.append((q_ref.at[1, rows], q2_hbm.at[rows]))
    pairs += [(dz_ref.at[pl.ds(2, VIEWS - 2)], dzs_hbm), (dz_ref.at[0], dz1_hbm), (dz_ref.at[1], dz2_hbm)]
    for src, dst in pairs:
        copies.append(pltpu.make_async_copy(src, dst, sem.at[len(copies)]))
        copies[-1].start()
    loss_ref[0, 0] = jnp.max(loss_in[:, 0:1])
    for copy in copies:
        copy.wait()


def local_step(z_one, z_two, z_small, protos, live_mask):
    vmem = pl.BlockSpec(memory_space=pltpu.VMEM)
    hbm = pl.BlockSpec(memory_space=pl.ANY)
    dma = pltpu.SemaphoreType.DMA
    views = VIEWS
    staged = pl.pallas_call(
        body,
        out_shape=(
            pltpu.VMEM((2, ROWS, PROTOS), F32),
            pltpu.VMEM((1, 128), F32),
            pltpu.VMEM((views, ROWS, DIM), F32),
            pltpu.VMEM((PROTOS, DIM), F32),
        ),
        in_specs=[vmem, hbm, hbm, hbm, hbm],
        out_specs=(vmem, vmem, vmem, vmem),
        scratch_shapes=[
            pltpu.VMEM((views, NROW, DIM), BF16),
            pltpu.VMEM((views, ROWS, DIM), BF16),
            pltpu.VMEM((PROTOS, DIM), BF16),
            pltpu.VMEM((views, OWN, NROW), F32),
            pltpu.VMEM((2, OWN, NROW), F32),
            pltpu.VMEM((2, OWN, 128), F32),
            pltpu.VMEM((DEVS, 2, 1, OWN), F32),
            pltpu.VMEM((ITERS, DEVS, 1, 2 * NROW), F32),
            pltpu.VMEM((DEVS, views, 1, 128), F32),
            pltpu.VMEM((DEVS, 1, 128), F32),
            pltpu.VMEM((DEVS, 1, 128), F32),
            pltpu.VMEM((1, NROW), F32),
            pltpu.VMEM((2, 1, NROW), F32),
            pltpu.VMEM((views, 1, NROW), F32),
            pltpu.VMEM((128, 128), F32),
            pltpu.VMEM((128, 128), F32),
            pltpu.VMEM((views + 2, ROWS, 128), F32),
            pltpu.VMEM((views * ROWS, 128), F32),
            dma(()), dma((6,)),
            dma((7, 5)), dma((7, 5)),
            dma((ITERS, DEVS)), dma((ITERS, DEVS)),
            dma((DEVS,)), dma((DEVS,)),
            dma((DEVS,)), dma((DEVS,)),
            dma((2, DEVS)), dma((2, DEVS)),
            dma((9, NCH)), dma((9, NCH)),
        ],
        compiler_params=pltpu.CompilerParams(
            collective_id=0, has_side_effects=True, vmem_limit_bytes=48 * 1024 * 1024),
        name="swav_step",
    )(live_mask.reshape(1, ROWS), z_one, z_two, z_small, protos)
    q_one, q_two, loss, dz_one, dz_two, dz_small, d_protos = pl.pallas_call(
        write_out,
        out_shape=(
            jax.ShapeDtypeStruct((ROWS, PROTOS), F32),
            jax.ShapeDtypeStruct((ROWS, PROTOS), F32),
            jax.ShapeDtypeStruct((1, 1), F32),
            jax.ShapeDtypeStruct((ROWS, DIM), F32),
            jax.ShapeDtypeStruct((ROWS, DIM), F32),
            jax.ShapeDtypeStruct((views - 2, ROWS, DIM), F32),
            jax.ShapeDtypeStruct((PROTOS, DIM), F32),
        ),
        in_specs=[vmem] * 4,
        out_specs=(hbm, hbm, pl.BlockSpec(memory_space=pltpu.SMEM), hbm, hbm, hbm, hbm),
        scratch_shapes=[dma((19,))],
        compiler_params=pltpu.CompilerParams(vmem_limit_bytes=1024 * 1024),
        name="write_out",
    )(*staged)
    return q_one, q_two, loss[0, 0], dz_one, dz_two, dz_small, d_protos


def solution(mesh):
    row_spec = P("data", None)
    crop_spec = P(None, "data", None)
    return jax.shard_map(local_step, mesh=mesh,
                         in_specs=(row_spec, row_spec, crop_spec, P(None, None), P("data")),
                         out_specs=(row_spec, row_spec, P(), row_spec, row_spec, crop_spec, P(None, None)),
                         check_vma=False)
```

```python
import functools
import math

import jax
import jax.numpy as jnp
from jax import lax
from jax.experimental import pallas as pl
from jax.experimental.pallas import tpu as pltpu
from jax.sharding import PartitionSpec as P

EPS = 0.05
TAU = 0.1
ITERS = 3
DEVS = 8
ROWS = 64
NROW = ROWS * DEVS
PROTOS = 8192
DIM = 256
VIEWS = 12
OWN = PROTOS // DEVS
KC = 256
NCH = OWN // KC
PC = 512
MESH = pl.DeviceIdType.MESH
F32 = jnp.float32
BF16 = jnp.bfloat16
UNITS = ((0, 1), (1, 1), (2, 4), (6, 4), (10, 2))
EC = 512


def nt_dot(a, b):
    return lax.dot_general(a, b, (((1,), (1,)), ((), ())), preferred_element_type=F32)


def body(mask_ref, z1_hbm, z2_hbm, zs_hbm, c_hbm,
         q_out, loss_ref, dz_out, dcv,
         zall, zown, cv, et, a0, vb, vx, rx, lx, mx, px,
         mvec, wvec, acf, cf, ct, ab, lacc,
         csem, isem, zsend, zrecv, rsend, rrecv, lsend, lrecv, vsend, vrecv, psend, precv,
         asend, arecv):
    me = lax.axis_index("data")
    core = me % 2
    xpos = (me // 2) % 2
    ypos = me // 4
    partner = me + 1 - 2 * core
    xn = me + 2 - 4 * xpos
    yn = me + 4 - 8 * ypos
    dg = xn + 4 - 8 * ypos

    def other(d):
        return d + 1 - 2 * core

    my_rows = pl.ds(pl.multiple_of(me * ROWS, ROWS), ROWS)
    small = pl.ds(2, VIEWS - 2)
    own_copies = []
    for src, dst in ((z1_hbm, zown.at[0]), (z2_hbm, zown.at[1]), (zs_hbm, zown.at[small]),
                     (z1_hbm, zall.at[0, my_rows]), (z2_hbm, zall.at[1, my_rows]), (zs_hbm, zall.at[small, my_rows])):
        own_copies.append(pltpu.make_async_copy(src, dst, isem.at[len(own_copies)]))
        own_copies[-1].start()
    own0 = pl.multiple_of(me * OWN, OWN)
    c_copy = pltpu.make_async_copy(c_hbm, cv, csem)
    c_copy.start()

    barrier = pltpu.get_barrier_semaphore()
    for off in range(1, DEVS):
        pl.semaphore_signal(barrier, inc=1, device_id=((me + off) % DEVS,), device_id_type=MESH)

    mrow = mask_ref[...].astype(F32)
    sel = (lax.broadcasted_iota(jnp.int32, (ROWS, 128), 1)
           == lax.broadcasted_iota(jnp.int32, (ROWS, 128), 0) + ROWS * core)
    mplaced = jnp.dot(jnp.broadcast_to(mrow, (8, ROWS)).astype(BF16), sel.astype(BF16),
                      preferred_element_type=F32)
    mx[me] = mplaced[0:1, :]

    def zdst(unit, dev):
        lo, cnt = UNITS[unit]
        rows = pl.ds(pl.multiple_of(dev * ROWS, ROWS), ROWS)
        if cnt == 1:
            return zall.at[lo, rows]
        return zall.at[pl.ds(lo, cnt), rows]

    def zsrc(unit):
        lo, cnt = UNITS[unit]
        return zown.at[lo] if cnt == 1 else zown.at[pl.ds(lo, cnt)]

    peers = (partner, xn, yn, dg)

    def zcopy(unit, kind):
        if kind < 4:
            return pltpu.make_async_remote_copy(
                src_ref=zsrc(unit), dst_ref=zdst(unit, me), send_sem=zsend.at[kind, unit],
                recv_sem=zrecv.at[kind, unit], device_id=(peers[kind],), device_id_type=MESH)
        dev = peers[kind - 3]
        return pltpu.make_async_remote_copy(
            src_ref=zdst(unit, dev), dst_ref=zdst(unit, dev), send_sem=zsend.at[kind, unit],
            recv_sem=zrecv.at[kind, unit], device_id=(partner,), device_id_type=MESH)

    def zwait(unit, kind):
        dev = peers[kind] if kind < 4 else other(peers[kind - 3])
        pltpu.make_async_remote_copy(
            src_ref=zsrc(unit), dst_ref=zdst(unit, dev), send_sem=zsend.at[kind, unit],
            recv_sem=zrecv.at[kind, unit], device_id=(partner,), device_id_type=MESH).wait_recv()

    def zstart(unit):
        for kind in (1, 2, 3, 0):
            zcopy(unit, kind).start()

    def zforward(units):
        for kind in (1, 2, 3):
            for unit in units:
                zwait(unit, kind)
                zcopy(unit, kind + 3).start()

    def zfinish(units):
        for unit in units:
            zwait(unit, 0)
        for kind in (4, 5, 6):
            for unit in units:
                zwait(unit, kind)

    def bcast(ref_of, send_sem, recv_sem, wait):
        for off in range(1, DEVS):
            dev = (me + off) % DEVS
            slot = dev if wait else me
            copy = pltpu.make_async_remote_copy(
                src_ref=ref_of(slot), dst_ref=ref_of(slot), send_sem=send_sem(off),
                recv_sem=recv_sem(slot), device_id=(dev,), device_id_type=MESH)
            if wait:
                copy.wait_recv()
            else:
                copy.start()

    def bcast_drain(ref_of, send_sem, recv_sem):
        for off in range(1, DEVS):
            pltpu.make_async_remote_copy(
                src_ref=ref_of(me), dst_ref=ref_of(me), send_sem=send_sem(off),
                recv_sem=recv_sem(me), device_id=((me + off) % DEVS,), device_id_type=MESH).wait_send()

    m_args = (lambda d: mx.at[d], lambda o: psend.at[1, o], lambda d: precv.at[1, d])
    p_args = (lambda d: px.at[d], lambda o: psend.at[0, o], lambda d: precv.at[0, d])
    v_args = (lambda d: vx.at[d], lambda o: vsend.at[o], lambda d: vrecv.at[d])

    def r_args(step):
        return (lambda d: rx.at[step, d], lambda o: rsend.at[step, o], lambda d: rrecv.at[step, d])

    l_args = (lambda d: lx.at[d], lambda o: lsend.at[o], lambda d: lrecv.at[d])

    for copy in own_copies:
        copy.wait()
    pl.semaphore_wait(barrier, DEVS - 1)
    zstart(0)
    zstart(1)
    bcast(*m_args, wait=False)
    zstart(2)

    def fold(x):
        return jnp.sum(x.reshape(x.shape[0] // 8, 8, x.shape[1]), axis=0)

    def lane_fold(x):
        out = x[:, 0:128]
        for i in range(1, x.shape[1] // 128):
            out = out + x[:, i * 128:(i + 1) * 128]
        return out

    lacc[...] = jnp.zeros_like(lacc)
    c_copy.wait()

    def sum_chunk(ch, carry):
        cc = cv[pl.ds(pl.multiple_of(ch * PC, PC), PC)]
        scores = nt_dot(zown[...].reshape(VIEWS * ROWS, DIM), cc)
        lacc[...] += lane_fold(jnp.exp(scores * (1.0 / TAU)))
        return carry
    def row_sums_out():
        for view in range(VIEWS):
            la = lacc[view * ROWS:(view + 1) * ROWS]
            lx[me, view] = jnp.sum(jnp.concatenate([la, la], axis=0).T, axis=0, keepdims=True)
        bcast(*l_args, wait=False)

    def exp_block(view, ch):
        rows = pl.ds(pl.multiple_of(ch * EC, EC), EC)
        scores = nt_dot(cv[pl.ds(pl.multiple_of(own0 + ch * EC, EC), EC)], zall[view])
        e = jnp.exp(scores * (1.0 / TAU))
        et[view, rows] = e
        return rows, e

    def exp_views(lo, hi):
        def step(view, carry):
            for ch in range(OWN // EC):
                exp_block(view, ch)
            return carry
        lax.fori_loop(lo, hi, step, 0)

    lax.fori_loop(0, 6, sum_chunk, 0)
    zforward((0, 1))
    lax.fori_loop(6, 8, sum_chunk, 0)
    bcast(*m_args, wait=True)
    zfinish((0, 1))
    for q in range(NROW // 128):
        mvec[:, q * 128:(q + 1) * 128] = mx[2 * q] + mx[2 * q + 1]
    live_total = jnp.sum(mvec[...], axis=1, keepdims=True)

    SB = 128

    def sq_step(i, carry):
        rows, e = exp_block(i // 2, i % 2)
        a0[i // 2, rows] = e * e
        return carry
    lax.fori_loop(0, 2 * (OWN // EC), sq_step, 0)

    def sink_pass(it):
        scale = (1.0 if it == 0 else live_total) * (1.0 / PROTOS)

        def step(blk, accs):
            rows = pl.ds(pl.multiple_of(blk * SB, SB), SB)
            out = []
            for view in range(2):
                a = a0[view, rows]
                w = mvec[...] if it == 0 else wvec[view]
                colsum = jnp.sum(a * w, axis=1, keepdims=True)
                v = scale / colsum
                if it == ITERS - 1:
                    vb[view, rows] = jnp.broadcast_to(v, (SB, 128))
                out.append(accs[view] + fold(a * v))
            return tuple(out)
        zero = jnp.zeros((8, NROW), F32)
        accs = lax.fori_loop(0, OWN // SB, step, (zero, zero))
        for view in range(2):
            rx[it, me, :, view * NROW:(view + 1) * NROW] = jnp.sum(accs[view], axis=0, keepdims=True)
        bcast(*r_args(it), wait=False)

    def sink_close(it):
        bcast(*r_args(it), wait=True)
        tot = rx[it, 0]
        for d in range(1, DEVS):
            tot = tot + rx[it, d]
        for view in range(2):
            wvec[view] = mvec[...] / tot[:, view * NROW:(view + 1) * NROW]

    sink_pass(0)
    zstart(3)
    lax.fori_loop(8, PROTOS // PC, sum_chunk, 0)
    row_sums_out()
    zforward((2,))
    sink_close(0)
    sink_pass(1)
    zstart(4)
    zfinish((2,))
    exp_views(2, 6)
    zforward((3,))
    sink_close(1)
    sink_pass(2)
    bcast(*l_args, wait=True)
    grad_scale = 1.0 / (TAU * live_total * (2 + 2 * (VIEWS - 2)))
    log_sum = jnp.zeros((1, NROW), F32)
    low = lax.broadcasted_iota(jnp.int32, (1, 128), 1) < ROWS
    for view in range(VIEWS):
        tot = jnp.concatenate([jnp.where(low, lx[2 * q, view], lx[2 * q + 1, view])
                               for q in range(NROW // 128)], axis=1)
        mult = 1.0 if view < 2 else 2.0
        acf[view] = (mult * grad_scale) * mvec[...] / tot
        log_sum = log_sum + mult * jnp.log(tot)
    log_sum = jnp.sum(log_sum * mvec[...], axis=1, keepdims=True)
    for view in range(2):
        for blk in range(OWN // 128):
            vt = vb[view, blk * 128:(blk + 1) * 128].T
            vx[me, view, :, blk * 128:(blk + 1) * 128] = vt[0:1, :]
    bcast(*v_args, wait=False)
    zfinish((3,))
    exp_views(6, 10)
    zforward((4,))
    zfinish((4,))
    exp_views(10, 12)
    sink_close(2)

    def rows_of(dev, ch):
        return pl.ds(pl.multiple_of(dev * OWN + ch * KC, KC), KC)

    def acopy(dev, ch, to, kind):
        rows = rows_of(dev, ch)
        return pltpu.make_async_remote_copy(
            src_ref=dcv.at[rows], dst_ref=dcv.at[rows], send_sem=asend.at[kind, ch],
            recv_sem=arecv.at[kind, ch], device_id=(to,), device_id_type=MESH)

    def dc_chunk(ch, carry):
        rows = pl.ds(pl.multiple_of(ch * KC, KC), KC)
        gq = []
        for view in range(2):
            v = jnp.concatenate([vb[view, rows]] * (NROW // 128), axis=1)
            gq.append((wvec[view] * grad_scale) * (v * a0[view, rows]))
        sub = [gq[1], gq[0]] + [gq[0] + gq[1]] * (VIEWS - 2)
        acc = None
        for view in range(VIEWS):
            g = (acf[view] * et[view, rows] - sub[view]).astype(BF16)
            part = jnp.dot(g, zall[view], preferred_element_type=F32)
            acc = part if acc is None else acc + part
        dcv[pl.ds(pl.multiple_of(own0 + ch * KC, KC), KC)] = acc
        acopy(me, ch, xn, 0).start()
        acopy(me, ch, yn, 1).start()
        acopy(me, ch, partner, 2).start()
        return carry
    lax.fori_loop(0, NCH, dc_chunk, 0)

    def dc_far(ch, carry):
        cc = cv[rows_of(dg, ch)]

        def expo(view):
            return jnp.exp(nt_dot(cc, zall[view]) * (1.0 / TAU))
        gq, es = [], []
        for view in range(2):
            vrow = vx[dg, view, :, pl.ds(pl.multiple_of(ch * KC, KC), KC)]
            v = jnp.concatenate([jnp.broadcast_to(vrow[:, j * 128:(j + 1) * 128], (128, 128)).T
                                 for j in range(KC // 128)], axis=0)
            v = jnp.concatenate([v] * (NROW // 128), axis=1)
            e = expo(view)
            es.append(e)
            gq.append((wvec[view] * grad_scale) * (v * (e * e)))
        sub = [gq[1], gq[0]] + [gq[0] + gq[1]] * (VIEWS - 2)
        acc = None
        for view in range(VIEWS):
            e = es[view] if view < 2 else expo(view)
            g = (acf[view] * e - sub[view]).astype(BF16)
            part = jnp.dot(g, zall[view], preferred_element_type=F32)
            acc = part if acc is None else acc + part
        dcv[rows_of(dg, ch)] = acc
        acopy(dg, ch, partner, 5).start()
        return carry

    def forward(ch):
        for dev, kind in ((xn, 0), (yn, 1)):
            acopy(dev, ch, dev, kind).wait_recv()
            acopy(dev, ch, partner, 3 + kind).start()

    bcast(*v_args, wait=True)
    lax.fori_loop(0, NCH, dc_far, 0)
    forward(0)
    forward(1)

    lanes = pl.ds(pl.multiple_of((me // 2) * 128, 128), 128)
    for view in range(VIEWS):
        cf[view:view + 1, :] = acf[view, :, lanes]
    for view in range(2):
        cf[VIEWS + view:VIEWS + view + 1, :] = wvec[view, :, lanes]
    ct[...] = cf[...].T
    own_cf = ct[pl.ds(pl.multiple_of(core * ROWS, ROWS), ROWS), :]
    for j in range(VIEWS + 2):
        ab[j] = jnp.broadcast_to(own_cf[:, j:j + 1], (ROWS, 128))

    dz_out[...] = jnp.zeros_like(dz_out)

    def wide(x):
        return jnp.concatenate([x] * (PC // 128), axis=1)

    def row_chunk(ch, acc):
        cols = pl.ds(pl.multiple_of(ch * PC, PC), PC)
        cc = cv[pl.ds(pl.multiple_of(ch * PC, PC), PC)]
        scores = nt_dot(zown[...].reshape(VIEWS * ROWS, DIM), cc)
        dev = ch // (OWN // PC)
        half = pl.ds(pl.multiple_of((ch % (OWN // PC)) * PC, PC), PC)
        e_large, q_large = [], []
        for view in range(2):
            e = jnp.exp(scores[view * ROWS:(view + 1) * ROWS] * (1.0 / TAU))
            q = wide(ab[VIEWS + view]) * (vx[dev, view, :, half] * (e * e))
            q_out[view, :, cols] = q
            e_large.append(e)
            q_large.append(q)
        q_sum = q_large[0] + q_large[1]
        gq_sum = q_sum * grad_scale
        parts = [(wide(ab[0]) * e_large[0] - q_large[1] * grad_scale).astype(BF16),
                 (wide(ab[1]) * e_large[1] - q_large[0] * grad_scale).astype(BF16)]
        s_sum = None
        for view in range(2, VIEWS):
            s = scores[view * ROWS:(view + 1) * ROWS]
            s_sum = s if s_sum is None else s_sum + s
            parts.append((wide(ab[view]) * jnp.exp(s * (1.0 / TAU)) - gq_sum).astype(BF16))
        dot = q_large[1] * scores[0:ROWS] + q_large[0] * scores[ROWS:2 * ROWS] + q_sum * s_sum
        dz = jnp.dot(jnp.concatenate(parts, axis=0), cc, preferred_element_type=F32)
        dz_out[...] += dz.reshape(VIEWS, ROWS, DIM)
        return acc + fold(dot)
    acc = lax.fori_loop(0, 6, row_chunk, jnp.zeros((8, PC), F32))
    forward(2)
    acc = lax.fori_loop(6, 12, row_chunk, acc)
    forward(3)
    acc = lax.fori_loop(12, PROTOS // PC, row_chunk, acc)
    cross = jnp.sum(jnp.sum(acc, axis=0, keepdims=True), axis=1, keepdims=True)
    px[me] = jnp.broadcast_to(cross, (1, 128))
    bcast(*p_args, wait=False)

    bcast(*p_args, wait=True)
    tot = px[0]
    for d in range(1, DEVS):
        tot = tot + px[d]
    loss = -(tot[:, 0:1] * (1.0 / TAU) - log_sum) / (live_total * (2 + 2 * (VIEWS - 2)))
    loss_ref[...] = jnp.broadcast_to(loss, (1, 128))

    def drain(ch, carry):
        for kind, dev in ((2, me), (3, xn), (4, yn), (5, dg)):
            acopy(other(dev), ch, partner, kind).wait_recv()
        for kind, dev in ((0, me), (1, me), (2, me), (3, xn), (4, yn), (5, dg)):
            acopy(dev, ch, partner, kind).wait_send()
        return carry
    for unit in range(len(UNITS)):
        for kind in range(7):
            zcopy(unit, kind).wait_send()
    bcast_drain(*m_args)
    bcast_drain(*p_args)
    bcast_drain(*v_args)
    for it in range(ITERS):
        bcast_drain(*r_args(it))
    bcast_drain(*l_args)
    lax.fori_loop(0, NCH, drain, 0)


def write_out(q_ref, loss_in, dz_ref, dc_ref, q1_hbm, q2_hbm, loss_ref, dz1_hbm, dz2_hbm, dzs_hbm, dc_hbm, sem):
    copies = []
    pairs = []
    for i in range(8):
        rows = pl.ds(i * (PROTOS // 8), PROTOS // 8)
        pairs.append((dc_ref.at[rows], dc_hbm.at[rows]))
    for i in range(4):
        rows = pl.ds(i * (ROWS // 4), ROWS // 4)
        pairs.append((q_ref.at[0, rows], q1_hbm.at[rows]))
        pairs.append((q_ref.at[1, rows], q2_hbm.at[rows]))
    pairs += [(dz_ref.at[pl.ds(2, VIEWS - 2)], dzs_hbm), (dz_ref.at[0], dz1_hbm), (dz_ref.at[1], dz2_hbm)]
    for src, dst in pairs:
        copies.append(pltpu.make_async_copy(src, dst, sem.at[len(copies)]))
        copies[-1].start()
    loss_ref[0, 0] = jnp.max(loss_in[:, 0:1])
    for copy in copies:
        copy.wait()


def local_step(z_one, z_two, z_small, protos, live_mask):
    vmem = pl.BlockSpec(memory_space=pltpu.VMEM)
    hbm = pl.BlockSpec(memory_space=pl.ANY)
    dma = pltpu.SemaphoreType.DMA
    views = VIEWS
    staged = pl.pallas_call(
        body,
        out_shape=(
            pltpu.VMEM((2, ROWS, PROTOS), F32),
            pltpu.VMEM((1, 128), F32),
            pltpu.VMEM((views, ROWS, DIM), F32),
            pltpu.VMEM((PROTOS, DIM), F32),
        ),
        in_specs=[vmem, hbm, hbm, hbm, hbm],
        out_specs=(vmem, vmem, vmem, vmem),
        scratch_shapes=[
            pltpu.VMEM((views, NROW, DIM), BF16),
            pltpu.VMEM((views, ROWS, DIM), BF16),
            pltpu.VMEM((PROTOS, DIM), BF16),
            pltpu.VMEM((views, OWN, NROW), F32),
            pltpu.VMEM((2, OWN, NROW), F32),
            pltpu.VMEM((2, OWN, 128), F32),
            pltpu.VMEM((DEVS, 2, 1, OWN), F32),
            pltpu.VMEM((ITERS, DEVS, 1, 2 * NROW), F32),
            pltpu.VMEM((DEVS, views, 1, 128), F32),
            pltpu.VMEM((DEVS, 1, 128), F32),
            pltpu.VMEM((DEVS, 1, 128), F32),
            pltpu.VMEM((1, NROW), F32),
            pltpu.VMEM((2, 1, NROW), F32),
            pltpu.VMEM((views, 1, NROW), F32),
            pltpu.VMEM((128, 128), F32),
            pltpu.VMEM((128, 128), F32),
            pltpu.VMEM((views + 2, ROWS, 128), F32),
            pltpu.VMEM((views * ROWS, 128), F32),
            dma(()), dma((6,)),
            dma((7, 5)), dma((7, 5)),
            dma((ITERS, DEVS)), dma((ITERS, DEVS)),
            dma((DEVS,)), dma((DEVS,)),
            dma((DEVS,)), dma((DEVS,)),
            dma((2, DEVS)), dma((2, DEVS)),
            dma((6, NCH)), dma((6, NCH)),
        ],
        compiler_params=pltpu.CompilerParams(
            collective_id=0, has_side_effects=True, vmem_limit_bytes=48 * 1024 * 1024),
        name="swav_step",
    )(live_mask.reshape(1, ROWS), z_one, z_two, z_small, protos)
    q_one, q_two, loss, dz_one, dz_two, dz_small, d_protos = pl.pallas_call(
        write_out,
        out_shape=(
            jax.ShapeDtypeStruct((ROWS, PROTOS), F32),
            jax.ShapeDtypeStruct((ROWS, PROTOS), F32),
            jax.ShapeDtypeStruct((1, 1), F32),
            jax.ShapeDtypeStruct((ROWS, DIM), F32),
            jax.ShapeDtypeStruct((ROWS, DIM), F32),
            jax.ShapeDtypeStruct((views - 2, ROWS, DIM), F32),
            jax.ShapeDtypeStruct((PROTOS, DIM), F32),
        ),
        in_specs=[vmem] * 4,
        out_specs=(hbm, hbm, pl.BlockSpec(memory_space=pltpu.SMEM), hbm, hbm, hbm, hbm),
        scratch_shapes=[dma((19,))],
        compiler_params=pltpu.CompilerParams(vmem_limit_bytes=1024 * 1024),
        name="write_out",
    )(*staged)
    return q_one, q_two, loss[0, 0], dz_one, dz_two, dz_small, d_protos


def solution(mesh):
    row_spec = P("data", None)
    crop_spec = P(None, "data", None)
    return jax.shard_map(local_step, mesh=mesh,
                         in_specs=(row_spec, row_spec, crop_spec, P(None, None), P("data")),
                         out_specs=(row_spec, row_spec, P(), row_spec, row_spec, crop_spec, P(None, None)),
                         check_vma=False)
```

```python
import functools
import math

import jax
import jax.numpy as jnp
from jax import lax
from jax.experimental import pallas as pl
from jax.experimental.pallas import tpu as pltpu
from jax.sharding import PartitionSpec as P

EPS = 0.05
TAU = 0.1
ITERS = 3
DEVS = 8
ROWS = 64
NROW = ROWS * DEVS
PROTOS = 8192
DIM = 256
VIEWS = 12
OWN = PROTOS // DEVS
KC = 256
NCH = OWN // KC
PC = 512
MESH = pl.DeviceIdType.MESH
F32 = jnp.float32
BF16 = jnp.bfloat16
UNITS = ((0, 1), (1, 1), (2, 4), (6, 4), (10, 2))
FC = 512
EC = 512


def nt_dot(a, b):
    return lax.dot_general(a, b, (((1,), (1,)), ((), ())), preferred_element_type=F32)


def body(mask_ref, z1_hbm, z2_hbm, zs_hbm, c_hbm,
         q_out, loss_ref, dz_out, dcv,
         zall, zown, cv, et, a0, vb, vx, rx, lx, mx, px,
         mvec, wvec, acf, cf, ct, ab, lacc,
         csem, isem, zsend, zrecv, rsend, rrecv, lsend, lrecv, vsend, vrecv, psend, precv,
         asend, arecv):
    me = lax.axis_index("data")
    core = me % 2
    xpos = (me // 2) % 2
    ypos = me // 4
    partner = me + 1 - 2 * core
    xn = me + 2 - 4 * xpos
    yn = me + 4 - 8 * ypos
    dg = xn + 4 - 8 * ypos

    def other(d):
        return d + 1 - 2 * core

    my_rows = pl.ds(pl.multiple_of(me * ROWS, ROWS), ROWS)
    small = pl.ds(2, VIEWS - 2)
    own_copies = []
    for h in range(2):
        half = pl.ds(h * 128, 128)
        for src, dst in ((z1_hbm.at[:, half], zown.at[h, 0]),
                         (z2_hbm.at[:, half], zown.at[h, 1]),
                         (zs_hbm.at[:, :, half], zown.at[h, small]),
                         (z1_hbm.at[:, half], zall.at[h, 0, my_rows]),
                         (z2_hbm.at[:, half], zall.at[h, 1, my_rows]),
                         (zs_hbm.at[:, :, half], zall.at[h, small, my_rows])):
            own_copies.append(pltpu.make_async_copy(src, dst, isem.at[len(own_copies)]))
            own_copies[-1].start()
    own0 = pl.multiple_of(me * OWN, OWN)
    c_copies = []
    for h in range(2):
        c_copies.append(pltpu.make_async_copy(c_hbm.at[:, pl.ds(h * 128, 128)], cv.at[h], csem.at[h]))
        c_copies[-1].start()

    def halves(x0, x1):
        return jnp.concatenate([x0, x1], axis=1)

    def protos_at(rows):
        return halves(cv[0, rows], cv[1, rows])

    def view_rows(view):
        return halves(zall[0, view], zall[1, view])

    def own_rows():
        return halves(zown[0].reshape(VIEWS * ROWS, 128), zown[1].reshape(VIEWS * ROWS, 128))

    barrier = pltpu.get_barrier_semaphore()
    for off in range(1, DEVS):
        pl.semaphore_signal(barrier, inc=1, device_id=((me + off) % DEVS,), device_id_type=MESH)

    mrow = mask_ref[...].astype(F32)
    sel = (lax.broadcasted_iota(jnp.int32, (ROWS, 128), 1)
           == lax.broadcasted_iota(jnp.int32, (ROWS, 128), 0) + ROWS * core)
    mplaced = jnp.dot(jnp.broadcast_to(mrow, (8, ROWS)).astype(BF16), sel.astype(BF16),
                      preferred_element_type=F32)
    mx[me] = mplaced[0:1, :]

    def zdst(unit, dev):
        lo, cnt = UNITS[unit]
        rows = pl.ds(pl.multiple_of(dev * ROWS, ROWS), ROWS)
        if cnt == 1:
            return zall.at[:, lo, rows]
        return zall.at[:, pl.ds(lo, cnt), rows]

    def zsrc(unit):
        lo, cnt = UNITS[unit]
        return zown.at[:, lo] if cnt == 1 else zown.at[:, pl.ds(lo, cnt)]

    peers = (partner, xn, yn, dg)

    def zcopy(unit, kind):
        if kind < 4:
            return pltpu.make_async_remote_copy(
                src_ref=zsrc(unit), dst_ref=zdst(unit, me), send_sem=zsend.at[kind, unit],
                recv_sem=zrecv.at[kind, unit], device_id=(peers[kind],), device_id_type=MESH)
        dev = peers[kind - 3]
        return pltpu.make_async_remote_copy(
            src_ref=zdst(unit, dev), dst_ref=zdst(unit, dev), send_sem=zsend.at[kind, unit],
            recv_sem=zrecv.at[kind, unit], device_id=(partner,), device_id_type=MESH)

    def zwait(unit, kind):
        dev = peers[kind] if kind < 4 else other(peers[kind - 3])
        pltpu.make_async_remote_copy(
            src_ref=zsrc(unit), dst_ref=zdst(unit, dev), send_sem=zsend.at[kind, unit],
            recv_sem=zrecv.at[kind, unit], device_id=(partner,), device_id_type=MESH).wait_recv()

    def zstart(unit):
        for kind in (1, 2, 3, 0):
            zcopy(unit, kind).start()

    def zforward(units):
        for kind in (1, 2, 3):
            for unit in units:
                zwait(unit, kind)
                zcopy(unit, kind + 3).start()

    def zfinish(units):
        for unit in units:
            zwait(unit, 0)
        for kind in (4, 5, 6):
            for unit in units:
                zwait(unit, kind)

    def bcast(ref_of, send_sem, recv_sem, wait):
        for off in range(1, DEVS):
            dev = (me + off) % DEVS
            slot = dev if wait else me
            copy = pltpu.make_async_remote_copy(
                src_ref=ref_of(slot), dst_ref=ref_of(slot), send_sem=send_sem(off),
                recv_sem=recv_sem(slot), device_id=(dev,), device_id_type=MESH)
            if wait:
                copy.wait_recv()
            else:
                copy.start()

    def bcast_drain(ref_of, send_sem, recv_sem):
        for off in range(1, DEVS):
            pltpu.make_async_remote_copy(
                src_ref=ref_of(me), dst_ref=ref_of(me), send_sem=send_sem(off),
                recv_sem=recv_sem(me), device_id=((me + off) % DEVS,), device_id_type=MESH).wait_send()

    m_args = (lambda d: mx.at[d], lambda o: psend.at[1, o], lambda d: precv.at[1, d])
    p_args = (lambda d: px.at[d], lambda o: psend.at[0, o], lambda d: precv.at[0, d])
    v_args = (lambda d: vx.at[d], lambda o: vsend.at[o], lambda d: vrecv.at[d])

    def r_args(step):
        return (lambda d: rx.at[step, d], lambda o: rsend.at[step, o], lambda d: rrecv.at[step, d])

    l_args = (lambda d: lx.at[d], lambda o: lsend.at[o], lambda d: lrecv.at[d])

    for copy in own_copies:
        copy.wait()
    pl.semaphore_wait(barrier, DEVS - 1)
    zstart(0)
    zstart(1)
    bcast(*m_args, wait=False)
    zstart(2)

    def fold(x):
        return jnp.sum(x.reshape(x.shape[0] // 8, 8, x.shape[1]), axis=0)

    def lane_fold(x):
        out = x[:, 0:128]
        for i in range(1, x.shape[1] // 128):
            out = out + x[:, i * 128:(i + 1) * 128]
        return out

    lacc[...] = jnp.zeros_like(lacc)
    for copy in c_copies:
        copy.wait()

    def sum_chunk(ch, carry):
        cc = protos_at(pl.ds(pl.multiple_of(ch * PC, PC), PC))
        scores = nt_dot(own_rows(), cc)
        lacc[...] += lane_fold(jnp.exp(scores * (1.0 / TAU)))
        return carry
    def row_sums_out():
        for view in range(VIEWS):
            la = lacc[view * ROWS:(view + 1) * ROWS]
            lx[me, view] = jnp.sum(jnp.concatenate([la, la], axis=0).T, axis=0, keepdims=True)
        bcast(*l_args, wait=False)

    def exp_block(view, ch):
        rows = pl.ds(pl.multiple_of(ch * EC, EC), EC)
        scores = nt_dot(protos_at(pl.ds(pl.multiple_of(own0 + ch * EC, EC), EC)), view_rows(view))
        e = jnp.exp(scores * (1.0 / TAU))
        et[view, rows] = e
        return rows, e

    def exp_views(lo, hi):
        def step(view, carry):
            for ch in range(OWN // EC):
                exp_block(view, ch)
            return carry
        lax.fori_loop(lo, hi, step, 0)

    lax.fori_loop(0, 6, sum_chunk, 0)
    zforward((0, 1))
    lax.fori_loop(6, 8, sum_chunk, 0)
    bcast(*m_args, wait=True)
    zfinish((0, 1))
    for q in range(NROW // 128):
        mvec[:, q * 128:(q + 1) * 128] = mx[2 * q] + mx[2 * q + 1]
    live_total = jnp.sum(mvec[...], axis=1, keepdims=True)

    SB = 128

    def sq_step(i, carry):
        rows, e = exp_block(i // 2, i % 2)
        a0[i // 2, rows] = e * e
        return carry
    lax.fori_loop(0, 2 * (OWN // EC), sq_step, 0)

    def sink_pass(it):
        scale = (1.0 if it == 0 else live_total) * (1.0 / PROTOS)

        def step(blk, accs):
            rows = pl.ds(pl.multiple_of(blk * SB, SB), SB)
            out = []
            for view in range(2):
                a = a0[view, rows]
                w = mvec[...] if it == 0 else wvec[view]
                colsum = jnp.sum(a * w, axis=1, keepdims=True)
                v = scale / colsum
                if it == ITERS - 1:
                    vb[view, rows] = jnp.broadcast_to(v, (SB, 128))
                out.append(accs[view] + fold(a * v))
            return tuple(out)
        zero = jnp.zeros((8, NROW), F32)
        accs = lax.fori_loop(0, OWN // SB, step, (zero, zero))
        for view in range(2):
            rx[it, me, :, view * NROW:(view + 1) * NROW] = jnp.sum(accs[view], axis=0, keepdims=True)
        bcast(*r_args(it), wait=False)

    def sink_close(it):
        bcast(*r_args(it), wait=True)
        tot = rx[it, 0]
        for d in range(1, DEVS):
            tot = tot + rx[it, d]
        for view in range(2):
            wvec[view] = mvec[...] / tot[:, view * NROW:(view + 1) * NROW]

    sink_pass(0)
    zstart(3)
    lax.fori_loop(8, PROTOS // PC, sum_chunk, 0)
    row_sums_out()
    zforward((2,))
    sink_close(0)
    sink_pass(1)
    zstart(4)
    zfinish((2,))
    exp_views(2, 6)
    zforward((3,))
    sink_close(1)
    sink_pass(2)
    bcast(*l_args, wait=True)
    grad_scale = 1.0 / (TAU * live_total * (2 + 2 * (VIEWS - 2)))
    log_sum = jnp.zeros((1, NROW), F32)
    low = lax.broadcasted_iota(jnp.int32, (1, 128), 1) < ROWS
    for view in range(VIEWS):
        tot = jnp.concatenate([jnp.where(low, lx[2 * q, view], lx[2 * q + 1, view])
                               for q in range(NROW // 128)], axis=1)
        mult = 1.0 if view < 2 else 2.0
        acf[view] = (mult * grad_scale) * mvec[...] / tot
        log_sum = log_sum + mult * jnp.log(tot)
    log_sum = jnp.sum(log_sum * mvec[...], axis=1, keepdims=True)
    for view in range(2):
        for blk in range(OWN // 128):
            vt = vb[view, blk * 128:(blk + 1) * 128].T
            vx[me, view, :, blk * 128:(blk + 1) * 128] = vt[0:1, :]
    bcast(*v_args, wait=False)
    zfinish((3,))
    exp_views(6, 10)
    zforward((4,))
    zfinish((4,))
    exp_views(10, 12)
    sink_close(2)

    def rows_of(dev, ch):
        return pl.ds(pl.multiple_of(dev * OWN + ch * KC, KC), KC)

    def acopy(dev, ch, to, kind):
        rows = rows_of(dev, ch)
        return pltpu.make_async_remote_copy(
            src_ref=dcv.at[rows], dst_ref=dcv.at[rows], send_sem=asend.at[kind, ch],
            recv_sem=arecv.at[kind, ch], device_id=(to,), device_id_type=MESH)

    def dc_chunk(ch, carry):
        rows = pl.ds(pl.multiple_of(ch * KC, KC), KC)
        gq = []
        for view in range(2):
            v = jnp.concatenate([vb[view, rows]] * (NROW // 128), axis=1)
            gq.append((wvec[view] * grad_scale) * (v * a0[view, rows]))
        sub = [gq[1], gq[0]] + [gq[0] + gq[1]] * (VIEWS - 2)
        acc = None
        for view in range(VIEWS):
            g = (acf[view] * et[view, rows] - sub[view]).astype(BF16)
            part = jnp.dot(g, view_rows(view), preferred_element_type=F32)
            acc = part if acc is None else acc + part
        dcv[pl.ds(pl.multiple_of(own0 + ch * KC, KC), KC)] = acc
        acopy(me, ch, xn, 0).start()
        acopy(me, ch, yn, 1).start()
        acopy(me, ch, partner, 2).start()
        return carry
    lax.fori_loop(0, NCH, dc_chunk, 0)

    def dc_far(ch, carry):
        rows = pl.ds(pl.multiple_of(dg * OWN + ch * FC, FC), FC)
        cc = protos_at(rows)

        def expo(view):
            return jnp.exp(nt_dot(cc, view_rows(view)) * (1.0 / TAU))
        gq, es = [], []
        for view in range(2):
            vrow = vx[dg, view, :, pl.ds(pl.multiple_of(ch * FC, FC), FC)]
            v = jnp.concatenate([jnp.broadcast_to(vrow[:, j * 128:(j + 1) * 128], (128, 128)).T
                                 for j in range(FC // 128)], axis=0)
            v = jnp.concatenate([v] * (NROW // 128), axis=1)
            e = expo(view)
            es.append(e)
            gq.append((wvec[view] * grad_scale) * (v * (e * e)))
        sub = [gq[1], gq[0]] + [gq[0] + gq[1]] * (VIEWS - 2)
        acc = None
        for view in range(VIEWS):
            e = es[view] if view < 2 else expo(view)
            g = (acf[view] * e - sub[view]).astype(BF16)
            part = jnp.dot(g, view_rows(view), preferred_element_type=F32)
            acc = part if acc is None else acc + part
        dcv[rows] = acc
        for part in range(FC // KC):
            acopy(dg, ch * (FC // KC) + part, partner, 5).start()
        return carry

    def forward(ch):
        for dev, kind in ((xn, 0), (yn, 1)):
            acopy(dev, ch, dev, kind).wait_recv()
            acopy(dev, ch, partner, 3 + kind).start()

    bcast(*v_args, wait=True)
    lax.fori_loop(0, OWN // FC, dc_far, 0)
    forward(0)
    forward(1)

    lanes = pl.ds(pl.multiple_of((me // 2) * 128, 128), 128)
    for view in range(VIEWS):
        cf[view:view + 1, :] = acf[view, :, lanes]
    for view in range(2):
        cf[VIEWS + view:VIEWS + view + 1, :] = wvec[view, :, lanes]
    ct[...] = cf[...].T
    own_cf = ct[pl.ds(pl.multiple_of(core * ROWS, ROWS), ROWS), :]
    for j in range(VIEWS + 2):
        ab[j] = jnp.broadcast_to(own_cf[:, j:j + 1], (ROWS, 128))

    dz_out[...] = jnp.zeros_like(dz_out)

    def wide(x):
        return jnp.concatenate([x] * (PC // 128), axis=1)

    def row_chunk(ch, acc):
        cols = pl.ds(pl.multiple_of(ch * PC, PC), PC)
        cc = protos_at(pl.ds(pl.multiple_of(ch * PC, PC), PC))
        scores = nt_dot(own_rows(), cc)
        dev = ch // (OWN // PC)
        half = pl.ds(pl.multiple_of((ch % (OWN // PC)) * PC, PC), PC)
        e_large, q_large = [], []
        for view in range(2):
            e = jnp.exp(scores[view * ROWS:(view + 1) * ROWS] * (1.0 / TAU))
            q = wide(ab[VIEWS + view]) * (vx[dev, view, :, half] * (e * e))
            q_out[view, :, cols] = q
            e_large.append(e)
            q_large.append(q)
        q_sum = q_large[0] + q_large[1]
        gq_sum = q_sum * grad_scale
        parts = [(wide(ab[0]) * e_large[0] - q_large[1] * grad_scale).astype(BF16),
                 (wide(ab[1]) * e_large[1] - q_large[0] * grad_scale).astype(BF16)]
        s_sum = None
        for view in range(2, VIEWS):
            s = scores[view * ROWS:(view + 1) * ROWS]
            s_sum = s if s_sum is None else s_sum + s
            parts.append((wide(ab[view]) * jnp.exp(s * (1.0 / TAU)) - gq_sum).astype(BF16))
        dot = q_large[1] * scores[0:ROWS] + q_large[0] * scores[ROWS:2 * ROWS] + q_sum * s_sum
        dz = jnp.dot(jnp.concatenate(parts, axis=0), cc, preferred_element_type=F32)
        dz_out[...] += dz.reshape(VIEWS, ROWS, DIM)
        return acc + fold(dot)
    acc = lax.fori_loop(0, 6, row_chunk, jnp.zeros((8, PC), F32))
    forward(2)
    acc = lax.fori_loop(6, 12, row_chunk, acc)
    forward(3)
    acc = lax.fori_loop(12, PROTOS // PC, row_chunk, acc)
    cross = jnp.sum(jnp.sum(acc, axis=0, keepdims=True), axis=1, keepdims=True)
    px[me] = jnp.broadcast_to(cross, (1, 128))
    bcast(*p_args, wait=False)

    bcast(*p_args, wait=True)
    tot = px[0]
    for d in range(1, DEVS):
        tot = tot + px[d]
    loss = -(tot[:, 0:1] * (1.0 / TAU) - log_sum) / (live_total * (2 + 2 * (VIEWS - 2)))
    loss_ref[...] = jnp.broadcast_to(loss, (1, 128))

    def drain(ch, carry):
        for kind, dev in ((2, me), (3, xn), (4, yn), (5, dg)):
            acopy(other(dev), ch, partner, kind).wait_recv()
        for kind, dev in ((0, me), (1, me), (2, me), (3, xn), (4, yn), (5, dg)):
            acopy(dev, ch, partner, kind).wait_send()
        return carry
    for unit in range(len(UNITS)):
        for kind in range(7):
            zcopy(unit, kind).wait_send()
    bcast_drain(*m_args)
    bcast_drain(*p_args)
    bcast_drain(*v_args)
    for it in range(ITERS):
        bcast_drain(*r_args(it))
    bcast_drain(*l_args)
    lax.fori_loop(0, NCH, drain, 0)


def write_out(q_ref, loss_in, dz_ref, dc_ref, q1_hbm, q2_hbm, loss_ref, dz1_hbm, dz2_hbm, dzs_hbm, dc_hbm, sem):
    copies = []
    pairs = []
    for i in range(8):
        rows = pl.ds(i * (PROTOS // 8), PROTOS // 8)
        pairs.append((dc_ref.at[rows], dc_hbm.at[rows]))
    for i in range(4):
        rows = pl.ds(i * (ROWS // 4), ROWS // 4)
        pairs.append((q_ref.at[0, rows], q1_hbm.at[rows]))
        pairs.append((q_ref.at[1, rows], q2_hbm.at[rows]))
    pairs += [(dz_ref.at[pl.ds(2, VIEWS - 2)], dzs_hbm), (dz_ref.at[0], dz1_hbm), (dz_ref.at[1], dz2_hbm)]
    for src, dst in pairs:
        copies.append(pltpu.make_async_copy(src, dst, sem.at[len(copies)]))
        copies[-1].start()
    loss_ref[0, 0] = jnp.max(loss_in[:, 0:1])
    for copy in copies:
        copy.wait()


def local_step(z_one, z_two, z_small, protos, live_mask):
    vmem = pl.BlockSpec(memory_space=pltpu.VMEM)
    hbm = pl.BlockSpec(memory_space=pl.ANY)
    dma = pltpu.SemaphoreType.DMA
    views = VIEWS
    staged = pl.pallas_call(
        body,
        out_shape=(
            pltpu.VMEM((2, ROWS, PROTOS), F32),
            pltpu.VMEM((1, 128), F32),
            pltpu.VMEM((views, ROWS, DIM), F32),
            pltpu.VMEM((PROTOS, DIM), F32),
        ),
        in_specs=[vmem, hbm, hbm, hbm, hbm],
        out_specs=(vmem, vmem, vmem, vmem),
        scratch_shapes=[
            pltpu.VMEM((2, views, NROW, 128), BF16),
            pltpu.VMEM((2, views, ROWS, 128), BF16),
            pltpu.VMEM((2, PROTOS, 128), BF16),
            pltpu.VMEM((views, OWN, NROW), F32),
            pltpu.VMEM((2, OWN, NROW), F32),
            pltpu.VMEM((2, OWN, 128), F32),
            pltpu.VMEM((DEVS, 2, 1, OWN), F32),
            pltpu.VMEM((ITERS, DEVS, 1, 2 * NROW), F32),
            pltpu.VMEM((DEVS, views, 1, 128), F32),
            pltpu.VMEM((DEVS, 1, 128), F32),
            pltpu.VMEM((DEVS, 1, 128), F32),
            pltpu.VMEM((1, NROW), F32),
            pltpu.VMEM((2, 1, NROW), F32),
            pltpu.VMEM((views, 1, NROW), F32),
            pltpu.VMEM((128, 128), F32),
            pltpu.VMEM((128, 128), F32),
            pltpu.VMEM((views + 2, ROWS, 128), F32),
            pltpu.VMEM((views * ROWS, 128), F32),
            dma((2,)), dma((12,)),
            dma((7, 5)), dma((7, 5)),
            dma((ITERS, DEVS)), dma((ITERS, DEVS)),
            dma((DEVS,)), dma((DEVS,)),
            dma((DEVS,)), dma((DEVS,)),
            dma((2, DEVS)), dma((2, DEVS)),
            dma((6, NCH)), dma((6, NCH)),
        ],
        compiler_params=pltpu.CompilerParams(
            collective_id=0, has_side_effects=True, vmem_limit_bytes=48 * 1024 * 1024),
        name="swav_step",
    )(live_mask.reshape(1, ROWS), z_one, z_two, z_small, protos)
    q_one, q_two, loss, dz_one, dz_two, dz_small, d_protos = pl.pallas_call(
        write_out,
        out_shape=(
            jax.ShapeDtypeStruct((ROWS, PROTOS), F32),
            jax.ShapeDtypeStruct((ROWS, PROTOS), F32),
            jax.ShapeDtypeStruct((1, 1), F32),
            jax.ShapeDtypeStruct((ROWS, DIM), F32),
            jax.ShapeDtypeStruct((ROWS, DIM), F32),
            jax.ShapeDtypeStruct((views - 2, ROWS, DIM), F32),
            jax.ShapeDtypeStruct((PROTOS, DIM), F32),
        ),
        in_specs=[vmem] * 4,
        out_specs=(hbm, hbm, pl.BlockSpec(memory_space=pltpu.SMEM), hbm, hbm, hbm, hbm),
        scratch_shapes=[dma((19,))],
        compiler_params=pltpu.CompilerParams(vmem_limit_bytes=1024 * 1024),
        name="write_out",
    )(*staged)
    return q_one, q_two, loss[0, 0], dz_one, dz_two, dz_small, d_protos


def solution(mesh):
    row_spec = P("data", None)
    crop_spec = P(None, "data", None)
    return jax.shard_map(local_step, mesh=mesh,
                         in_specs=(row_spec, row_spec, crop_spec, P(None, None), P("data")),
                         out_specs=(row_spec, row_spec, P(), row_spec, row_spec, crop_spec, P(None, None)),
                         check_vma=False)
```

```python
import functools
import math

import jax
import jax.numpy as jnp
from jax import lax
from jax.experimental import pallas as pl
from jax.experimental.pallas import tpu as pltpu
from jax.sharding import PartitionSpec as P

EPS = 0.05
TAU = 0.1
ITERS = 3
DEVS = 8
ROWS = 64
NROW = ROWS * DEVS
PROTOS = 8192
DIM = 256
VIEWS = 12
OWN = PROTOS // DEVS
KC = 256
NCH = OWN // KC
KEPT = 8
PC = 512
MESH = pl.DeviceIdType.MESH
F32 = jnp.float32
BF16 = jnp.bfloat16
UNITS = ((0, 1), (1, 1), (2, 5), (7, 3), (10, 2))
FC = 512
EC = 512


def nt_dot(a, b):
    return lax.dot_general(a, b, (((1,), (1,)), ((), ())), preferred_element_type=F32)


def body(mask_ref, z1_hbm, z2_hbm, zs_hbm, c_hbm,
         q_out, loss_ref, dz_out, dcv,
         zall, zown, cv, et, sst, vb, vx, rx, lx, mx, px,
         mvec, wvec, acf, cf, ct, ab, lacc,
         csem, isem, zsend, zrecv, rsend, rrecv, lsend, lrecv, vsend, vrecv, psend, precv,
         asend, arecv):
    me = lax.axis_index("data")
    core = me % 2
    xpos = (me // 2) % 2
    ypos = me // 4
    partner = me + 1 - 2 * core
    xn = me + 2 - 4 * xpos
    yn = me + 4 - 8 * ypos
    dg = xn + 4 - 8 * ypos

    def other(d):
        return d + 1 - 2 * core

    my_rows = pl.ds(pl.multiple_of(me * ROWS, ROWS), ROWS)
    small = pl.ds(2, VIEWS - 2)
    own_copies = []
    for h in range(2):
        half = pl.ds(h * 128, 128)
        for src, dst in ((z1_hbm.at[:, half], zown.at[h, 0]),
                         (z2_hbm.at[:, half], zown.at[h, 1]),
                         (zs_hbm.at[:, :, half], zown.at[h, small]),
                         (z1_hbm.at[:, half], zall.at[h, 0, my_rows]),
                         (z2_hbm.at[:, half], zall.at[h, 1, my_rows]),
                         (zs_hbm.at[:, :, half], zall.at[h, small, my_rows])):
            own_copies.append(pltpu.make_async_copy(src, dst, isem.at[len(own_copies)]))
            own_copies[-1].start()
    own0 = pl.multiple_of(me * OWN, OWN)
    c_copies = []
    for h in range(2):
        c_copies.append(pltpu.make_async_copy(c_hbm.at[:, pl.ds(h * 128, 128)], cv.at[h], csem.at[h]))
        c_copies[-1].start()

    def halves(x0, x1):
        return jnp.concatenate([x0, x1], axis=1)

    def protos_at(rows):
        return halves(cv[0, rows], cv[1, rows])

    def view_rows(view):
        return halves(zall[0, view], zall[1, view])

    def own_rows():
        return halves(zown[0].reshape(VIEWS * ROWS, 128), zown[1].reshape(VIEWS * ROWS, 128))

    barrier = pltpu.get_barrier_semaphore()
    for off in range(1, DEVS):
        pl.semaphore_signal(barrier, inc=1, device_id=((me + off) % DEVS,), device_id_type=MESH)

    mrow = mask_ref[...].astype(F32)
    sel = (lax.broadcasted_iota(jnp.int32, (ROWS, 128), 1)
           == lax.broadcasted_iota(jnp.int32, (ROWS, 128), 0) + ROWS * core)
    mplaced = jnp.dot(jnp.broadcast_to(mrow, (8, ROWS)).astype(BF16), sel.astype(BF16),
                      preferred_element_type=F32)
    mx[me] = mplaced[0:1, :]

    def zdst(unit, dev):
        lo, cnt = UNITS[unit]
        rows = pl.ds(pl.multiple_of(dev * ROWS, ROWS), ROWS)
        if cnt == 1:
            return zall.at[:, lo, rows]
        return zall.at[:, pl.ds(lo, cnt), rows]

    def zsrc(unit):
        lo, cnt = UNITS[unit]
        return zown.at[:, lo] if cnt == 1 else zown.at[:, pl.ds(lo, cnt)]

    peers = (partner, xn, yn, dg)

    def zcopy(unit, kind):
        if kind < 4:
            return pltpu.make_async_remote_copy(
                src_ref=zsrc(unit), dst_ref=zdst(unit, me), send_sem=zsend.at[kind, unit],
                recv_sem=zrecv.at[kind, unit], device_id=(peers[kind],), device_id_type=MESH)
        dev = peers[kind - 3]
        return pltpu.make_async_remote_copy(
            src_ref=zdst(unit, dev), dst_ref=zdst(unit, dev), send_sem=zsend.at[kind, unit],
            recv_sem=zrecv.at[kind, unit], device_id=(partner,), device_id_type=MESH)

    def zwait(unit, kind):
        dev = peers[kind] if kind < 4 else other(peers[kind - 3])
        pltpu.make_async_remote_copy(
            src_ref=zsrc(unit), dst_ref=zdst(unit, dev), send_sem=zsend.at[kind, unit],
            recv_sem=zrecv.at[kind, unit], device_id=(partner,), device_id_type=MESH).wait_recv()

    def zstart(unit):
        for kind in (1, 2, 3, 0):
            zcopy(unit, kind).start()

    def zforward(units):
        for kind in (1, 2, 3):
            for unit in units:
                zwait(unit, kind)
                zcopy(unit, kind + 3).start()

    def zfinish(units):
        for unit in units:
            zwait(unit, 0)
        for kind in (4, 5, 6):
            for unit in units:
                zwait(unit, kind)

    def bcast(ref_of, send_sem, recv_sem, wait):
        for off in range(1, DEVS):
            dev = (me + off) % DEVS
            slot = dev if wait else me
            copy = pltpu.make_async_remote_copy(
                src_ref=ref_of(slot), dst_ref=ref_of(slot), send_sem=send_sem(off),
                recv_sem=recv_sem(slot), device_id=(dev,), device_id_type=MESH)
            if wait:
                copy.wait_recv()
            else:
                copy.start()

    def bcast_drain(ref_of, send_sem, recv_sem):
        for off in range(1, DEVS):
            pltpu.make_async_remote_copy(
                src_ref=ref_of(me), dst_ref=ref_of(me), send_sem=send_sem(off),
                recv_sem=recv_sem(me), device_id=((me + off) % DEVS,), device_id_type=MESH).wait_send()

    m_args = (lambda d: mx.at[d], lambda o: psend.at[1, o], lambda d: precv.at[1, d])
    p_args = (lambda d: px.at[d], lambda o: psend.at[0, o], lambda d: precv.at[0, d])
    v_args = (lambda d: vx.at[d], lambda o: vsend.at[o], lambda d: vrecv.at[d])

    def r_args(step):
        return (lambda d: rx.at[step, d], lambda o: rsend.at[step, o], lambda d: rrecv.at[step, d])

    l_args = (lambda d: lx.at[d], lambda o: lsend.at[o], lambda d: lrecv.at[d])

    for copy in own_copies:
        copy.wait()
    pl.semaphore_wait(barrier, DEVS - 1)
    zstart(0)
    zstart(1)
    bcast(*m_args, wait=False)
    zstart(2)

    def fold(x):
        return jnp.sum(x.reshape(x.shape[0] // 8, 8, x.shape[1]), axis=0)

    def lane_fold(x):
        out = x[:, 0:128]
        for i in range(1, x.shape[1] // 128):
            out = out + x[:, i * 128:(i + 1) * 128]
        return out

    lacc[...] = jnp.zeros_like(lacc)
    for copy in c_copies:
        copy.wait()

    def sum_chunk(ch, carry, keep=False):
        cc = protos_at(pl.ds(pl.multiple_of(ch * PC, PC), PC))
        scores = nt_dot(own_rows(), cc)
        lacc[...] += lane_fold(jnp.exp(scores * (1.0 / TAU)))
        if keep:
            sst[ch - (PROTOS // PC - KEPT)] = scores
        return carry
    def row_sums_out():
        for view in range(VIEWS):
            la = lacc[view * ROWS:(view + 1) * ROWS]
            lx[me, view] = jnp.sum(jnp.concatenate([la, la], axis=0).T, axis=0, keepdims=True)
        bcast(*l_args, wait=False)

    def exp_block(view, ch):
        rows = pl.ds(pl.multiple_of(ch * EC, EC), EC)
        scores = nt_dot(protos_at(pl.ds(pl.multiple_of(own0 + ch * EC, EC), EC)), view_rows(view))
        e = jnp.exp(scores * (1.0 / TAU))
        et[view, rows] = e
        return rows, e

    def exp_views(lo, hi):
        def step(view, carry):
            for ch in range(OWN // EC):
                exp_block(view, ch)
            return carry
        lax.fori_loop(lo, hi, step, 0)

    lax.fori_loop(0, 6, sum_chunk, 0)
    zforward((0, 1))
    lax.fori_loop(6, 8, sum_chunk, 0)
    bcast(*m_args, wait=True)
    zfinish((0, 1))
    for q in range(NROW // 128):
        mvec[:, q * 128:(q + 1) * 128] = mx[2 * q] + mx[2 * q + 1]
    live_total = jnp.sum(mvec[...], axis=1, keepdims=True)

    SB = 128

    exp_views(0, 2)

    def sink_pass(it):
        scale = (1.0 if it == 0 else live_total) * (1.0 / PROTOS)

        def step(blk, accs):
            rows = pl.ds(pl.multiple_of(blk * SB, SB), SB)
            out = []
            for view in range(2):
                e = et[view, rows]
                a = e * e
                w = mvec[...] if it == 0 else wvec[view]
                colsum = jnp.sum(a * w, axis=1, keepdims=True)
                v = scale / colsum
                if it == ITERS - 1:
                    vb[view, rows] = jnp.broadcast_to(v, (SB, 128))
                out.append(accs[view] + fold(a * v))
            return tuple(out)
        zero = jnp.zeros((8, NROW), F32)
        accs = lax.fori_loop(0, OWN // SB, step, (zero, zero))
        for view in range(2):
            rx[it, me, :, view * NROW:(view + 1) * NROW] = jnp.sum(accs[view], axis=0, keepdims=True)
        bcast(*r_args(it), wait=False)

    def sink_close(it):
        bcast(*r_args(it), wait=True)
        tot = rx[it, 0]
        for d in range(1, DEVS):
            tot = tot + rx[it, d]
        for view in range(2):
            wvec[view] = mvec[...] / tot[:, view * NROW:(view + 1) * NROW]

    sink_pass(0)
    zstart(3)
    lax.fori_loop(PROTOS // PC - KEPT, PROTOS // PC, functools.partial(sum_chunk, keep=True), 0)
    zforward((2,))
    sink_close(0)
    sink_pass(1)
    row_sums_out()
    zstart(4)
    zfinish((2,))
    exp_views(2, 7)
    zforward((3,))
    sink_close(1)
    sink_pass(2)
    bcast(*l_args, wait=True)
    grad_scale = 1.0 / (TAU * live_total * (2 + 2 * (VIEWS - 2)))
    log_sum = jnp.zeros((1, NROW), F32)
    low = lax.broadcasted_iota(jnp.int32, (1, 128), 1) < ROWS
    for view in range(VIEWS):
        tot = jnp.concatenate([jnp.where(low, lx[2 * q, view], lx[2 * q + 1, view])
                               for q in range(NROW // 128)], axis=1)
        mult = 1.0 if view < 2 else 2.0
        acf[view] = (mult * grad_scale) * mvec[...] / tot
        log_sum = log_sum + mult * jnp.log(tot)
    log_sum = jnp.sum(log_sum * mvec[...], axis=1, keepdims=True)
    for view in range(2):
        for blk in range(OWN // 128):
            vt = vb[view, blk * 128:(blk + 1) * 128].T
            vx[me, view, :, blk * 128:(blk + 1) * 128] = vt[0:1, :]
    bcast(*v_args, wait=False)
    zfinish((3,))
    exp_views(7, 10)
    zforward((4,))
    zfinish((4,))
    exp_views(10, 12)
    sink_close(2)

    def rows_of(dev, ch):
        return pl.ds(pl.multiple_of(dev * OWN + ch * KC, KC), KC)

    def acopy(dev, ch, to, kind):
        rows = rows_of(dev, ch)
        return pltpu.make_async_remote_copy(
            src_ref=dcv.at[rows], dst_ref=dcv.at[rows], send_sem=asend.at[kind, ch],
            recv_sem=arecv.at[kind, ch], device_id=(to,), device_id_type=MESH)

    def dc_chunk(ch, carry):
        rows = pl.ds(pl.multiple_of(ch * KC, KC), KC)
        gq = []
        for view in range(2):
            v = jnp.concatenate([vb[view, rows]] * (NROW // 128), axis=1)
            e = et[view, rows]
            gq.append((wvec[view] * grad_scale) * (v * (e * e)))
        sub = [gq[1], gq[0]] + [gq[0] + gq[1]] * (VIEWS - 2)
        acc = None
        for view in range(VIEWS):
            g = (acf[view] * et[view, rows] - sub[view]).astype(BF16)
            part = jnp.dot(g, view_rows(view), preferred_element_type=F32)
            acc = part if acc is None else acc + part
        dcv[pl.ds(pl.multiple_of(own0 + ch * KC, KC), KC)] = acc
        acopy(me, ch, xn, 0).start()
        acopy(me, ch, yn, 1).start()
        acopy(me, ch, partner, 2).start()
        return carry
    lax.fori_loop(0, NCH, dc_chunk, 0)

    def dc_far(ch, carry):
        rows = pl.ds(pl.multiple_of(dg * OWN + ch * FC, FC), FC)
        cc = protos_at(rows)

        def expo(view):
            return jnp.exp(nt_dot(cc, view_rows(view)) * (1.0 / TAU))
        gq, es = [], []
        for view in range(2):
            vrow = vx[dg, view, :, pl.ds(pl.multiple_of(ch * FC, FC), FC)]
            v = jnp.concatenate([jnp.broadcast_to(vrow[:, j * 128:(j + 1) * 128], (128, 128)).T
                                 for j in range(FC // 128)], axis=0)
            v = jnp.concatenate([v] * (NROW // 128), axis=1)
            e = expo(view)
            es.append(e)
            gq.append((wvec[view] * grad_scale) * (v * (e * e)))
        sub = [gq[1], gq[0]] + [gq[0] + gq[1]] * (VIEWS - 2)
        acc = None
        for view in range(VIEWS):
            e = es[view] if view < 2 else expo(view)
            g = (acf[view] * e - sub[view]).astype(BF16)
            part = jnp.dot(g, view_rows(view), preferred_element_type=F32)
            acc = part if acc is None else acc + part
        dcv[rows] = acc
        for part in range(FC // KC):
            acopy(dg, ch * (FC // KC) + part, partner, 5).start()
        return carry

    def forward(ch):
        for dev, kind in ((xn, 0), (yn, 1)):
            acopy(dev, ch, dev, kind).wait_recv()
            acopy(dev, ch, partner, 3 + kind).start()

    bcast(*v_args, wait=True)
    lax.fori_loop(0, OWN // FC, dc_far, 0)
    forward(0)
    forward(1)

    lanes = pl.ds(pl.multiple_of((me // 2) * 128, 128), 128)
    for view in range(VIEWS):
        cf[view:view + 1, :] = acf[view, :, lanes]
    for view in range(2):
        cf[VIEWS + view:VIEWS + view + 1, :] = wvec[view, :, lanes]
    ct[...] = cf[...].T
    own_cf = ct[pl.ds(pl.multiple_of(core * ROWS, ROWS), ROWS), :]
    for j in range(VIEWS + 2):
        ab[j] = jnp.broadcast_to(own_cf[:, j:j + 1], (ROWS, 128))

    dz_out[...] = jnp.zeros_like(dz_out)

    def wide(x):
        return jnp.concatenate([x] * (PC // 128), axis=1)

    def row_chunk(ch, acc, kept=False):
        cols = pl.ds(pl.multiple_of(ch * PC, PC), PC)
        cc = protos_at(pl.ds(pl.multiple_of(ch * PC, PC), PC))
        if kept:
            def score(view):
                return sst[ch - (PROTOS // PC - KEPT), view * ROWS:(view + 1) * ROWS]
        else:
            scores = nt_dot(own_rows(), cc)

            def score(view):
                return scores[view * ROWS:(view + 1) * ROWS]
        dev = ch // (OWN // PC)
        half = pl.ds(pl.multiple_of((ch % (OWN // PC)) * PC, PC), PC)
        e_large, q_large = [], []
        for view in range(2):
            e = jnp.exp(score(view) * (1.0 / TAU))
            q = wide(ab[VIEWS + view]) * (vx[dev, view, :, half] * (e * e))
            q_out[view, :, cols] = q
            e_large.append(e)
            q_large.append(q)
        q_sum = q_large[0] + q_large[1]
        gq_sum = q_sum * grad_scale
        parts = [(wide(ab[0]) * e_large[0] - q_large[1] * grad_scale).astype(BF16),
                 (wide(ab[1]) * e_large[1] - q_large[0] * grad_scale).astype(BF16)]
        s_sum = None
        for view in range(2, VIEWS):
            s = score(view)
            s_sum = s if s_sum is None else s_sum + s
            parts.append((wide(ab[view]) * jnp.exp(s * (1.0 / TAU)) - gq_sum).astype(BF16))
        dot = q_large[1] * score(0) + q_large[0] * score(1) + q_sum * s_sum
        dz = jnp.dot(jnp.concatenate(parts, axis=0), cc, preferred_element_type=F32)
        dz_out[...] += dz.reshape(VIEWS, ROWS, DIM)
        return acc + fold(dot)
    acc = lax.fori_loop(0, PROTOS // PC - KEPT, row_chunk, jnp.zeros((8, PC), F32))
    forward(2)
    row_kept = functools.partial(row_chunk, kept=True)
    acc = lax.fori_loop(PROTOS // PC - KEPT, PROTOS // PC - 2, row_kept, acc)
    forward(3)
    acc = lax.fori_loop(PROTOS // PC - 2, PROTOS // PC, row_kept, acc)
    cross = jnp.sum(jnp.sum(acc, axis=0, keepdims=True), axis=1, keepdims=True)
    px[me] = jnp.broadcast_to(cross, (1, 128))
    bcast(*p_args, wait=False)

    bcast(*p_args, wait=True)
    tot = px[0]
    for d in range(1, DEVS):
        tot = tot + px[d]
    loss = -(tot[:, 0:1] * (1.0 / TAU) - log_sum) / (live_total * (2 + 2 * (VIEWS - 2)))
    loss_ref[...] = jnp.broadcast_to(loss, (1, 128))

    def drain(ch, carry):
        for kind, dev in ((2, me), (3, xn), (4, yn), (5, dg)):
            acopy(other(dev), ch, partner, kind).wait_recv()
        for kind, dev in ((0, me), (1, me), (2, me), (3, xn), (4, yn), (5, dg)):
            acopy(dev, ch, partner, kind).wait_send()
        return carry
    for unit in range(len(UNITS)):
        for kind in range(7):
            zcopy(unit, kind).wait_send()
    bcast_drain(*m_args)
    bcast_drain(*p_args)
    bcast_drain(*v_args)
    for it in range(ITERS):
        bcast_drain(*r_args(it))
    bcast_drain(*l_args)
    lax.fori_loop(0, NCH, drain, 0)


def write_out(q_ref, loss_in, dz_ref, dc_ref, q1_hbm, q2_hbm, loss_ref, dz1_hbm, dz2_hbm, dzs_hbm, dc_hbm, sem):
    copies = []
    pairs = []
    for i in range(8):
        rows = pl.ds(i * (PROTOS // 8), PROTOS // 8)
        pairs.append((dc_ref.at[rows], dc_hbm.at[rows]))
    for i in range(4):
        rows = pl.ds(i * (ROWS // 4), ROWS // 4)
        pairs.append((q_ref.at[0, rows], q1_hbm.at[rows]))
        pairs.append((q_ref.at[1, rows], q2_hbm.at[rows]))
    pairs += [(dz_ref.at[pl.ds(2, VIEWS - 2)], dzs_hbm), (dz_ref.at[0], dz1_hbm), (dz_ref.at[1], dz2_hbm)]
    for src, dst in pairs:
        copies.append(pltpu.make_async_copy(src, dst, sem.at[len(copies)]))
        copies[-1].start()
    loss_ref[0, 0] = jnp.max(loss_in[:, 0:1])
    for copy in copies:
        copy.wait()


def local_step(z_one, z_two, z_small, protos, live_mask):
    vmem = pl.BlockSpec(memory_space=pltpu.VMEM)
    hbm = pl.BlockSpec(memory_space=pl.ANY)
    dma = pltpu.SemaphoreType.DMA
    views = VIEWS
    staged = pl.pallas_call(
        body,
        out_shape=(
            pltpu.VMEM((2, ROWS, PROTOS), F32),
            pltpu.VMEM((1, 128), F32),
            pltpu.VMEM((views, ROWS, DIM), F32),
            pltpu.VMEM((PROTOS, DIM), F32),
        ),
        in_specs=[vmem, hbm, hbm, hbm, hbm],
        out_specs=(vmem, vmem, vmem, vmem),
        scratch_shapes=[
            pltpu.VMEM((2, views, NROW, 128), BF16),
            pltpu.VMEM((2, views, ROWS, 128), BF16),
            pltpu.VMEM((2, PROTOS, 128), BF16),
            pltpu.VMEM((views, OWN, NROW), F32),
            pltpu.VMEM((KEPT, views * ROWS, PC), F32),
            pltpu.VMEM((2, OWN, 128), F32),
            pltpu.VMEM((DEVS, 2, 1, OWN), F32),
            pltpu.VMEM((ITERS, DEVS, 1, 2 * NROW), F32),
            pltpu.VMEM((DEVS, views, 1, 128), F32),
            pltpu.VMEM((DEVS, 1, 128), F32),
            pltpu.VMEM((DEVS, 1, 128), F32),
            pltpu.VMEM((1, NROW), F32),
            pltpu.VMEM((2, 1, NROW), F32),
            pltpu.VMEM((views, 1, NROW), F32),
            pltpu.VMEM((128, 128), F32),
            pltpu.VMEM((128, 128), F32),
            pltpu.VMEM((views + 2, ROWS, 128), F32),
            pltpu.VMEM((views * ROWS, 128), F32),
            dma((2,)), dma((12,)),
            dma((7, 5)), dma((7, 5)),
            dma((ITERS, DEVS)), dma((ITERS, DEVS)),
            dma((DEVS,)), dma((DEVS,)),
            dma((DEVS,)), dma((DEVS,)),
            dma((2, DEVS)), dma((2, DEVS)),
            dma((6, NCH)), dma((6, NCH)),
        ],
        compiler_params=pltpu.CompilerParams(
            collective_id=0, has_side_effects=True, vmem_limit_bytes=50 * 1024 * 1024),
        name="swav_step",
    )(live_mask.reshape(1, ROWS), z_one, z_two, z_small, protos)
    q_one, q_two, loss, dz_one, dz_two, dz_small, d_protos = pl.pallas_call(
        write_out,
        out_shape=(
            jax.ShapeDtypeStruct((ROWS, PROTOS), F32),
            jax.ShapeDtypeStruct((ROWS, PROTOS), F32),
            jax.ShapeDtypeStruct((1, 1), F32),
            jax.ShapeDtypeStruct((ROWS, DIM), F32),
            jax.ShapeDtypeStruct((ROWS, DIM), F32),
            jax.ShapeDtypeStruct((views - 2, ROWS, DIM), F32),
            jax.ShapeDtypeStruct((PROTOS, DIM), F32),
        ),
        in_specs=[vmem] * 4,
        out_specs=(hbm, hbm, pl.BlockSpec(memory_space=pltpu.SMEM), hbm, hbm, hbm, hbm),
        scratch_shapes=[dma((19,))],
        compiler_params=pltpu.CompilerParams(vmem_limit_bytes=1024 * 1024),
        name="write_out",
    )(*staged)
    return q_one, q_two, loss[0, 0], dz_one, dz_two, dz_small, d_protos


def solution(mesh):
    row_spec = P("data", None)
    crop_spec = P(None, "data", None)
    return jax.shard_map(local_step, mesh=mesh,
                         in_specs=(row_spec, row_spec, crop_spec, P(None, None), P("data")),
                         out_specs=(row_spec, row_spec, P(), row_spec, row_spec, crop_spec, P(None, None)),
                         check_vma=False)
```

```python
import functools
import math

import jax
import jax.numpy as jnp
from jax import lax
from jax.experimental import pallas as pl
from jax.experimental.pallas import tpu as pltpu
from jax.sharding import PartitionSpec as P

EPS = 0.05
TAU = 0.1
ITERS = 3
DEVS = 8
ROWS = 64
NROW = ROWS * DEVS
PROTOS = 8192
DIM = 256
VIEWS = 12
OWN = PROTOS // DEVS
KC = 256
NCH = OWN // KC
KEPT = 8
PC = 512
MESH = pl.DeviceIdType.MESH
F32 = jnp.float32
BF16 = jnp.bfloat16
UNITS = ((0, 1), (1, 1), (2, 5), (7, 3), (10, 2))
EC = 512


def nt_dot(a, b):
    return lax.dot_general(a, b, (((1,), (1,)), ((), ())), preferred_element_type=F32)


def body(mask_hbm, z1_hbm, z2_hbm, zs_hbm, c_hbm,
         q_out, loss_ref, dz_out, dcv,
         zall, zown, cv, et, sst, vb, vx, rx, lx, mx, px,
         mvec, wvec, acf, cf, ct, ab, lacc,
         mask_ref, csem, isem, zsend, zrecv, rsend, rrecv, lsend, lrecv, vsend, vrecv, psend, precv,
         asend, arecv):
    me = lax.axis_index("data")
    core = me % 2
    xpos = (me // 2) % 2
    ypos = me // 4
    partner = me + 1 - 2 * core
    xn = me + 2 - 4 * xpos
    yn = me + 4 - 8 * ypos
    dg = xn + 4 - 8 * ypos

    def other(d):
        return d + 1 - 2 * core

    my_rows = pl.ds(pl.multiple_of(me * ROWS, ROWS), ROWS)
    small = pl.ds(2, VIEWS - 2)
    own_copies = []
    for h in range(2):
        half = pl.ds(h * 128, 128)
        for src, dst in ((z1_hbm.at[:, half], zown.at[h, 0]),
                         (z2_hbm.at[:, half], zown.at[h, 1]),
                         (zs_hbm.at[:, :, half], zown.at[h, small]),
                         (z1_hbm.at[:, half], zall.at[h, 0, my_rows]),
                         (z2_hbm.at[:, half], zall.at[h, 1, my_rows]),
                         (zs_hbm.at[:, :, half], zall.at[h, small, my_rows])):
            own_copies.append(pltpu.make_async_copy(src, dst, isem.at[len(own_copies)]))
            own_copies[-1].start()
    own0 = pl.multiple_of(me * OWN, OWN)
    own_copies.append(pltpu.make_async_copy(mask_hbm, mask_ref, isem.at[12]))
    own_copies[-1].start()
    c_copies = []
    for h in range(2):
        c_copies.append(pltpu.make_async_copy(c_hbm.at[:, pl.ds(h * 128, 128)], cv.at[h], csem.at[h]))
        c_copies[-1].start()

    def halves(x0, x1):
        return jnp.concatenate([x0, x1], axis=1)

    def protos_at(rows):
        return halves(cv[0, rows], cv[1, rows])

    def view_rows(view):
        return halves(zall[0, view], zall[1, view])

    def own_rows():
        return halves(zown[0].reshape(VIEWS * ROWS, 128), zown[1].reshape(VIEWS * ROWS, 128))

    barrier = pltpu.get_barrier_semaphore()
    for off in range(1, DEVS):
        pl.semaphore_signal(barrier, inc=1, device_id=((me + off) % DEVS,), device_id_type=MESH)

    def zdst(unit, dev):
        lo, cnt = UNITS[unit]
        rows = pl.ds(pl.multiple_of(dev * ROWS, ROWS), ROWS)
        if cnt == 1:
            return zall.at[:, lo, rows]
        return zall.at[:, pl.ds(lo, cnt), rows]

    def zsrc(unit):
        lo, cnt = UNITS[unit]
        return zown.at[:, lo] if cnt == 1 else zown.at[:, pl.ds(lo, cnt)]

    peers = (partner, xn, yn, dg)

    def zcopy(unit, kind):
        if kind < 4:
            return pltpu.make_async_remote_copy(
                src_ref=zsrc(unit), dst_ref=zdst(unit, me), send_sem=zsend.at[kind, unit],
                recv_sem=zrecv.at[kind, unit], device_id=(peers[kind],), device_id_type=MESH)
        dev = peers[kind - 3]
        return pltpu.make_async_remote_copy(
            src_ref=zdst(unit, dev), dst_ref=zdst(unit, dev), send_sem=zsend.at[kind, unit],
            recv_sem=zrecv.at[kind, unit], device_id=(partner,), device_id_type=MESH)

    def zwait(unit, kind):
        dev = peers[kind] if kind < 4 else other(peers[kind - 3])
        pltpu.make_async_remote_copy(
            src_ref=zsrc(unit), dst_ref=zdst(unit, dev), send_sem=zsend.at[kind, unit],
            recv_sem=zrecv.at[kind, unit], device_id=(partner,), device_id_type=MESH).wait_recv()

    def zstart(unit):
        for kind in (1, 2, 3, 0):
            zcopy(unit, kind).start()

    def zforward(units):
        for kind in (1, 2, 3):
            for unit in units:
                zwait(unit, kind)
                zcopy(unit, kind + 3).start()

    def zfinish(units):
        for unit in units:
            zwait(unit, 0)
        for kind in (4, 5, 6):
            for unit in units:
                zwait(unit, kind)

    def bcast(ref_of, send_sem, recv_sem, wait):
        for off in range(1, DEVS):
            dev = (me + off) % DEVS
            slot = dev if wait else me
            copy = pltpu.make_async_remote_copy(
                src_ref=ref_of(slot), dst_ref=ref_of(slot), send_sem=send_sem(off),
                recv_sem=recv_sem(slot), device_id=(dev,), device_id_type=MESH)
            if wait:
                copy.wait_recv()
            else:
                copy.start()

    def bcast_drain(ref_of, send_sem, recv_sem):
        for off in range(1, DEVS):
            pltpu.make_async_remote_copy(
                src_ref=ref_of(me), dst_ref=ref_of(me), send_sem=send_sem(off),
                recv_sem=recv_sem(me), device_id=((me + off) % DEVS,), device_id_type=MESH).wait_send()

    m_args = (lambda d: mx.at[d], lambda o: psend.at[1, o], lambda d: precv.at[1, d])
    p_args = (lambda d: px.at[d], lambda o: psend.at[0, o], lambda d: precv.at[0, d])
    v_args = (lambda d: vx.at[d], lambda o: vsend.at[o], lambda d: vrecv.at[d])

    def r_args(step):
        return (lambda d: rx.at[step, d], lambda o: rsend.at[step, o], lambda d: rrecv.at[step, d])

    l_args = (lambda d: lx.at[d], lambda o: lsend.at[o], lambda d: lrecv.at[d])

    for copy in own_copies:
        copy.wait()

    mrow = mask_ref[...].astype(F32)
    sel = (lax.broadcasted_iota(jnp.int32, (ROWS, 128), 1)
           == lax.broadcasted_iota(jnp.int32, (ROWS, 128), 0) + ROWS * core)
    mplaced = jnp.dot(jnp.broadcast_to(mrow, (8, ROWS)).astype(BF16), sel.astype(BF16),
                      preferred_element_type=F32)
    mx[me] = mplaced[0:1, :]

    pl.semaphore_wait(barrier, DEVS - 1)
    zstart(0)
    zstart(1)
    bcast(*m_args, wait=False)
    zstart(2)

    def fold(x):
        return jnp.sum(x.reshape(x.shape[0] // 8, 8, x.shape[1]), axis=0)

    def lane_fold(x):
        out = x[:, 0:128]
        for i in range(1, x.shape[1] // 128):
            out = out + x[:, i * 128:(i + 1) * 128]
        return out

    lacc[...] = jnp.zeros_like(lacc)
    for copy in c_copies:
        copy.wait()

    def sum_chunk(ch, carry, keep=False):
        cc = protos_at(pl.ds(pl.multiple_of(ch * PC, PC), PC))
        scores = nt_dot(own_rows(), cc)
        lacc[...] += lane_fold(jnp.exp(scores * (1.0 / TAU)))
        if keep:
            sst[ch - (PROTOS // PC - KEPT)] = scores
        return carry
    def row_sums_out():
        for view in range(VIEWS):
            la = lacc[view * ROWS:(view + 1) * ROWS]
            lx[me, view] = jnp.sum(jnp.concatenate([la, la], axis=0).T, axis=0, keepdims=True)
        bcast(*l_args, wait=False)

    def exp_block(view, ch, base):
        rows = pl.ds(pl.multiple_of(ch * EC, EC), EC)
        scores = nt_dot(protos_at(pl.ds(pl.multiple_of(base + ch * EC, EC), EC)), view_rows(view))
        e = jnp.exp(scores * (1.0 / TAU))
        et[view, rows] = e
        return rows, e

    def exp_views(lo, hi, base=own0):
        def step(view, carry):
            for ch in range(OWN // EC):
                exp_block(view, ch, base)
            return carry
        lax.fori_loop(lo, hi, step, 0)

    lax.fori_loop(0, 6, sum_chunk, 0)
    zforward((0, 1))
    lax.fori_loop(6, 8, sum_chunk, 0)
    bcast(*m_args, wait=True)
    zfinish((0, 1))
    for q in range(NROW // 128):
        mvec[:, q * 128:(q + 1) * 128] = mx[2 * q] + mx[2 * q + 1]
    live_total = jnp.sum(mvec[...], axis=1, keepdims=True)

    SB = 128

    exp_views(0, 2)

    def sink_pass(it):
        scale = (1.0 if it == 0 else live_total) * (1.0 / PROTOS)

        def step(blk, accs):
            rows = pl.ds(pl.multiple_of(blk * SB, SB), SB)
            out = []
            for view in range(2):
                e = et[view, rows]
                a = e * e
                w = mvec[...] if it == 0 else wvec[view]
                colsum = jnp.sum(a * w, axis=1, keepdims=True)
                v = scale / colsum
                if it == ITERS - 1:
                    vb[view, rows] = jnp.broadcast_to(v, (SB, 128))
                out.append(accs[view] + fold(a * v))
            return tuple(out)
        zero = jnp.zeros((8, NROW), F32)
        accs = lax.fori_loop(0, OWN // SB, step, (zero, zero))
        for view in range(2):
            rx[it, me, :, view * NROW:(view + 1) * NROW] = jnp.sum(accs[view], axis=0, keepdims=True)
        bcast(*r_args(it), wait=False)

    def sink_close(it):
        bcast(*r_args(it), wait=True)
        tot = rx[it, 0]
        for d in range(1, DEVS):
            tot = tot + rx[it, d]
        for view in range(2):
            wvec[view] = mvec[...] / tot[:, view * NROW:(view + 1) * NROW]

    sink_pass(0)
    zstart(3)
    lax.fori_loop(PROTOS // PC - KEPT, PROTOS // PC, functools.partial(sum_chunk, keep=True), 0)
    zforward((2,))
    sink_close(0)
    sink_pass(1)
    row_sums_out()
    zstart(4)
    zfinish((2,))
    exp_views(2, 7)
    zforward((3,))
    sink_close(1)
    sink_pass(2)
    bcast(*l_args, wait=True)
    grad_scale = 1.0 / (TAU * live_total * (2 + 2 * (VIEWS - 2)))
    log_sum = jnp.zeros((1, NROW), F32)
    low = lax.broadcasted_iota(jnp.int32, (1, 128), 1) < ROWS
    for view in range(VIEWS):
        tot = jnp.concatenate([jnp.where(low, lx[2 * q, view], lx[2 * q + 1, view])
                               for q in range(NROW // 128)], axis=1)
        mult = 1.0 if view < 2 else 2.0
        acf[view] = (mult * grad_scale) * mvec[...] / tot
        log_sum = log_sum + mult * jnp.log(tot)
    log_sum = jnp.sum(log_sum * mvec[...], axis=1, keepdims=True)
    for view in range(2):
        for blk in range(OWN // 128):
            vt = vb[view, blk * 128:(blk + 1) * 128].T
            vx[me, view, :, blk * 128:(blk + 1) * 128] = vt[0:1, :]
    bcast(*v_args, wait=False)
    zfinish((3,))
    exp_views(7, 10)
    zforward((4,))
    zfinish((4,))
    exp_views(10, 12)
    sink_close(2)

    def rows_of(dev, ch):
        return pl.ds(pl.multiple_of(dev * OWN + ch * KC, KC), KC)

    def acopy(dev, ch, to, kind):
        rows = rows_of(dev, ch)
        return pltpu.make_async_remote_copy(
            src_ref=dcv.at[rows], dst_ref=dcv.at[rows], send_sem=asend.at[kind, ch],
            recv_sem=arecv.at[kind, ch], device_id=(to,), device_id_type=MESH)

    def dc_chunk(dev, ch):
        rows = pl.ds(pl.multiple_of(ch * KC, KC), KC)
        gq = []
        for view in range(2):
            v = jnp.concatenate([vb[view, rows]] * (NROW // 128), axis=1)
            e = et[view, rows]
            gq.append((wvec[view] * grad_scale) * (v * (e * e)))
        sub = [gq[1], gq[0]] + [gq[0] + gq[1]] * (VIEWS - 2)
        acc = None
        for view in range(VIEWS):
            g = (acf[view] * et[view, rows] - sub[view]).astype(BF16)
            part = jnp.dot(g, view_rows(view), preferred_element_type=F32)
            acc = part if acc is None else acc + part
        dcv[rows_of(dev, ch)] = acc

    def dc_own(ch, carry):
        dc_chunk(me, ch)
        acopy(me, ch, xn, 0).start()
        acopy(me, ch, yn, 1).start()
        acopy(me, ch, partner, 2).start()
        return carry
    lax.fori_loop(0, NCH, dc_own, 0)

    def dc_far(ch, carry):
        dc_chunk(dg, ch)
        acopy(dg, ch, partner, 5).start()
        return carry

    def forward(ch):
        for dev, kind in ((xn, 0), (yn, 1)):
            acopy(dev, ch, dev, kind).wait_recv()
            acopy(dev, ch, partner, 3 + kind).start()

    bcast(*v_args, wait=True)
    for view in range(2):
        for blk in range(OWN // 128):
            lanes = slice(blk * 128, (blk + 1) * 128)
            vb[view, lanes] = jnp.broadcast_to(vx[dg, view, :, lanes], (128, 128)).T
    exp_views(0, VIEWS, dg * OWN)
    lax.fori_loop(0, NCH, dc_far, 0)
    forward(0)
    forward(1)

    lanes = pl.ds(pl.multiple_of((me // 2) * 128, 128), 128)
    for view in range(VIEWS):
        cf[view:view + 1, :] = acf[view, :, lanes]
    for view in range(2):
        cf[VIEWS + view:VIEWS + view + 1, :] = wvec[view, :, lanes]
    ct[...] = cf[...].T
    own_cf = ct[pl.ds(pl.multiple_of(core * ROWS, ROWS), ROWS), :]
    for j in range(VIEWS + 2):
        ab[j] = jnp.broadcast_to(own_cf[:, j:j + 1], (ROWS, 128))

    dz_out[...] = jnp.zeros_like(dz_out)

    def wide(x):
        return jnp.concatenate([x] * (PC // 128), axis=1)

    def row_chunk(ch, acc, kept=False):
        cols = pl.ds(pl.multiple_of(ch * PC, PC), PC)
        cc = protos_at(pl.ds(pl.multiple_of(ch * PC, PC), PC))
        if kept:
            def score(view):
                return sst[ch - (PROTOS // PC - KEPT), view * ROWS:(view + 1) * ROWS]
        else:
            scores = nt_dot(own_rows(), cc)

            def score(view):
                return scores[view * ROWS:(view + 1) * ROWS]
        dev = ch // (OWN // PC)
        half = pl.ds(pl.multiple_of((ch % (OWN // PC)) * PC, PC), PC)
        e_large, q_large = [], []
        for view in range(2):
            e = jnp.exp(score(view) * (1.0 / TAU))
            q = wide(ab[VIEWS + view]) * (vx[dev, view, :, half] * (e * e))
            q_out[view, :, cols] = q
            e_large.append(e)
            q_large.append(q)
        q_sum = q_large[0] + q_large[1]
        gq_sum = q_sum * grad_scale
        parts = [(wide(ab[0]) * e_large[0] - q_large[1] * grad_scale).astype(BF16),
                 (wide(ab[1]) * e_large[1] - q_large[0] * grad_scale).astype(BF16)]
        s_sum = None
        for view in range(2, VIEWS):
            s = score(view)
            s_sum = s if s_sum is None else s_sum + s
            parts.append((wide(ab[view]) * jnp.exp(s * (1.0 / TAU)) - gq_sum).astype(BF16))
        dot = q_large[1] * score(0) + q_large[0] * score(1) + q_sum * s_sum
        dz = jnp.dot(jnp.concatenate(parts, axis=0), cc, preferred_element_type=F32)
        dz_out[...] += dz.reshape(VIEWS, ROWS, DIM)
        return acc + fold(dot)
    acc = lax.fori_loop(0, PROTOS // PC - KEPT, row_chunk, jnp.zeros((8, PC), F32))
    forward(2)
    row_kept = functools.partial(row_chunk, kept=True)
    acc = lax.fori_loop(PROTOS // PC - KEPT, PROTOS // PC - 2, row_kept, acc)
    forward(3)
    acc = lax.fori_loop(PROTOS // PC - 2, PROTOS // PC, row_kept, acc)
    cross = jnp.sum(jnp.sum(acc, axis=0, keepdims=True), axis=1, keepdims=True)
    px[me] = jnp.broadcast_to(cross, (1, 128))
    bcast(*p_args, wait=False)

    bcast(*p_args, wait=True)
    tot = px[0]
    for d in range(1, DEVS):
        tot = tot + px[d]
    loss = -(tot[:, 0:1] * (1.0 / TAU) - log_sum) / (live_total * (2 + 2 * (VIEWS - 2)))
    loss_ref[...] = jnp.broadcast_to(loss, (1, 128))

    def drain(ch, carry):
        for kind, dev in ((2, me), (3, xn), (4, yn), (5, dg)):
            acopy(other(dev), ch, partner, kind).wait_recv()
        for kind, dev in ((0, me), (1, me), (2, me), (3, xn), (4, yn), (5, dg)):
            acopy(dev, ch, partner, kind).wait_send()
        return carry
    for unit in range(len(UNITS)):
        for kind in range(7):
            zcopy(unit, kind).wait_send()
    bcast_drain(*m_args)
    bcast_drain(*p_args)
    bcast_drain(*v_args)
    for it in range(ITERS):
        bcast_drain(*r_args(it))
    bcast_drain(*l_args)
    lax.fori_loop(0, NCH, drain, 0)


def write_out(q_ref, loss_in, dz_ref, dc_ref, q1_hbm, q2_hbm, loss_ref, dz1_hbm, dz2_hbm, dzs_hbm, dc_hbm, sem):
    copies = []
    pairs = []
    for i in range(8):
        rows = pl.ds(i * (PROTOS // 8), PROTOS // 8)
        pairs.append((dc_ref.at[rows], dc_hbm.at[rows]))
    for i in range(4):
        rows = pl.ds(i * (ROWS // 4), ROWS // 4)
        pairs.append((q_ref.at[0, rows], q1_hbm.at[rows]))
        pairs.append((q_ref.at[1, rows], q2_hbm.at[rows]))
    pairs += [(dz_ref.at[pl.ds(2, VIEWS - 2)], dzs_hbm), (dz_ref.at[0], dz1_hbm), (dz_ref.at[1], dz2_hbm)]
    for src, dst in pairs:
        copies.append(pltpu.make_async_copy(src, dst, sem.at[len(copies)]))
        copies[-1].start()
    loss_ref[0, 0] = jnp.max(loss_in[:, 0:1])
    for copy in copies:
        copy.wait()


def local_step(z_one, z_two, z_small, protos, live_mask):
    vmem = pl.BlockSpec(memory_space=pltpu.VMEM)
    hbm = pl.BlockSpec(memory_space=pl.ANY)
    dma = pltpu.SemaphoreType.DMA
    views = VIEWS
    staged = pl.pallas_call(
        body,
        out_shape=(
            pltpu.VMEM((2, ROWS, PROTOS), F32),
            pltpu.VMEM((1, 128), F32),
            pltpu.VMEM((views, ROWS, DIM), F32),
            pltpu.VMEM((PROTOS, DIM), F32),
        ),
        in_specs=[hbm] * 5,
        out_specs=(vmem, vmem, vmem, vmem),
        scratch_shapes=[
            pltpu.VMEM((2, views, NROW, 128), BF16),
            pltpu.VMEM((2, views, ROWS, 128), BF16),
            pltpu.VMEM((2, PROTOS, 128), BF16),
            pltpu.VMEM((views, OWN, NROW), F32),
            pltpu.VMEM((KEPT, views * ROWS, PC), F32),
            pltpu.VMEM((2, OWN, 128), F32),
            pltpu.VMEM((DEVS, 2, 1, OWN), F32),
            pltpu.VMEM((ITERS, DEVS, 1, 2 * NROW), F32),
            pltpu.VMEM((DEVS, views, 1, 128), F32),
            pltpu.VMEM((DEVS, 1, 128), F32),
            pltpu.VMEM((DEVS, 1, 128), F32),
            pltpu.VMEM((1, NROW), F32),
            pltpu.VMEM((2, 1, NROW), F32),
            pltpu.VMEM((views, 1, NROW), F32),
            pltpu.VMEM((128, 128), F32),
            pltpu.VMEM((128, 128), F32),
            pltpu.VMEM((views + 2, ROWS, 128), F32),
            pltpu.VMEM((views * ROWS, 128), F32),
            pltpu.VMEM((1, ROWS), jnp.int32),
            dma((2,)), dma((13,)),
            dma((7, 5)), dma((7, 5)),
            dma((ITERS, DEVS)), dma((ITERS, DEVS)),
            dma((DEVS,)), dma((DEVS,)),
            dma((DEVS,)), dma((DEVS,)),
            dma((2, DEVS)), dma((2, DEVS)),
            dma((6, NCH)), dma((6, NCH)),
        ],
        compiler_params=pltpu.CompilerParams(
            collective_id=0, has_side_effects=True, vmem_limit_bytes=50 * 1024 * 1024),
        name="swav_step",
    )(live_mask.reshape(1, ROWS), z_one, z_two, z_small, protos)
    q_one, q_two, loss, dz_one, dz_two, dz_small, d_protos = pl.pallas_call(
        write_out,
        out_shape=(
            jax.ShapeDtypeStruct((ROWS, PROTOS), F32),
            jax.ShapeDtypeStruct((ROWS, PROTOS), F32),
            jax.ShapeDtypeStruct((1, 1), F32),
            jax.ShapeDtypeStruct((ROWS, DIM), F32),
            jax.ShapeDtypeStruct((ROWS, DIM), F32),
            jax.ShapeDtypeStruct((views - 2, ROWS, DIM), F32),
            jax.ShapeDtypeStruct((PROTOS, DIM), F32),
        ),
        in_specs=[vmem] * 4,
        out_specs=(hbm, hbm, pl.BlockSpec(memory_space=pltpu.SMEM), hbm, hbm, hbm, hbm),
        scratch_shapes=[dma((19,))],
        compiler_params=pltpu.CompilerParams(vmem_limit_bytes=1024 * 1024),
        name="write_out",
    )(*staged)
    return q_one, q_two, loss[0, 0], dz_one, dz_two, dz_small, d_protos


def solution(mesh):
    row_spec = P("data", None)
    crop_spec = P(None, "data", None)
    return jax.shard_map(local_step, mesh=mesh,
                         in_specs=(row_spec, row_spec, crop_spec, P(None, None), P("data")),
                         out_specs=(row_spec, row_spec, P(), row_spec, row_spec, crop_spec, P(None, None)),
                         check_vma=False)
```

```python
import functools
import math

import jax
import jax.numpy as jnp
from jax import lax
from jax.experimental import pallas as pl
from jax.experimental.pallas import tpu as pltpu
from jax.sharding import PartitionSpec as P

EPS = 0.05
TAU = 0.1
ITERS = 3
DEVS = 8
ROWS = 64
NROW = ROWS * DEVS
PROTOS = 8192
DIM = 256
VIEWS = 12
OWN = PROTOS // DEVS
KC = 256
NCH = OWN // KC
KEPT = 8
PC = 512
MESH = pl.DeviceIdType.MESH
F32 = jnp.float32
BF16 = jnp.bfloat16
UNITS = ((0, 1), (1, 1), (2, 5), (7, 3), (10, 2))
EC = 512


def nt_dot(a, b):
    return lax.dot_general(a, b, (((1,), (1,)), ((), ())), preferred_element_type=F32)


def body(mask_hbm, z1_hbm, z2_hbm, zs_hbm, c_hbm,
         q_out, loss_ref, dz_out, dcv,
         zall, zown, cv, et, sst, vb, vx, rx, lx, mx, px,
         mvec, wvec, acf, cf, ct, ab, lacc, gbuf,
         mask_ref, csem, isem, zsend, zrecv, rsend, rrecv, lsend, lrecv, vsend, vrecv, psend, precv,
         asend, arecv):
    me = lax.axis_index("data")
    core = me % 2
    xpos = (me // 2) % 2
    ypos = me // 4
    partner = me + 1 - 2 * core
    xn = me + 2 - 4 * xpos
    yn = me + 4 - 8 * ypos
    dg = xn + 4 - 8 * ypos

    def other(d):
        return d + 1 - 2 * core

    my_rows = pl.ds(pl.multiple_of(me * ROWS, ROWS), ROWS)
    small = pl.ds(2, VIEWS - 2)
    own_copies = []
    for h in range(2):
        half = pl.ds(h * 128, 128)
        for src, dst in ((z1_hbm.at[:, half], zown.at[h, 0]),
                         (z2_hbm.at[:, half], zown.at[h, 1]),
                         (zs_hbm.at[:, :, half], zown.at[h, small]),
                         (z1_hbm.at[:, half], zall.at[h, 0, my_rows]),
                         (z2_hbm.at[:, half], zall.at[h, 1, my_rows]),
                         (zs_hbm.at[:, :, half], zall.at[h, small, my_rows])):
            own_copies.append(pltpu.make_async_copy(src, dst, isem.at[len(own_copies)]))
            own_copies[-1].start()
    own0 = pl.multiple_of(me * OWN, OWN)
    own_copies.append(pltpu.make_async_copy(mask_hbm, mask_ref, isem.at[12]))
    own_copies[-1].start()
    c_copies = []
    for h in range(2):
        c_copies.append(pltpu.make_async_copy(c_hbm.at[:, pl.ds(h * 128, 128)], cv.at[h], csem.at[h]))
        c_copies[-1].start()

    def halves(x0, x1):
        return jnp.concatenate([x0, x1], axis=1)

    def protos_at(rows):
        return halves(cv[0, rows], cv[1, rows])

    def view_rows(view):
        return halves(zall[0, view], zall[1, view])

    def own_rows():
        return halves(zown[0].reshape(VIEWS * ROWS, 128), zown[1].reshape(VIEWS * ROWS, 128))

    barrier = pltpu.get_barrier_semaphore()
    for off in range(1, DEVS):
        pl.semaphore_signal(barrier, inc=1, device_id=((me + off) % DEVS,), device_id_type=MESH)

    def zdst(unit, dev):
        lo, cnt = UNITS[unit]
        rows = pl.ds(pl.multiple_of(dev * ROWS, ROWS), ROWS)
        if cnt == 1:
            return zall.at[:, lo, rows]
        return zall.at[:, pl.ds(lo, cnt), rows]

    def zsrc(unit):
        lo, cnt = UNITS[unit]
        return zown.at[:, lo] if cnt == 1 else zown.at[:, pl.ds(lo, cnt)]

    peers = (partner, xn, yn, dg)

    def zcopy(unit, kind):
        if kind < 4:
            return pltpu.make_async_remote_copy(
                src_ref=zsrc(unit), dst_ref=zdst(unit, me), send_sem=zsend.at[kind, unit],
                recv_sem=zrecv.at[kind, unit], device_id=(peers[kind],), device_id_type=MESH)
        dev = peers[kind - 3]
        return pltpu.make_async_remote_copy(
            src_ref=zdst(unit, dev), dst_ref=zdst(unit, dev), send_sem=zsend.at[kind, unit],
            recv_sem=zrecv.at[kind, unit], device_id=(partner,), device_id_type=MESH)

    def zwait(unit, kind):
        dev = peers[kind] if kind < 4 else other(peers[kind - 3])
        pltpu.make_async_remote_copy(
            src_ref=zsrc(unit), dst_ref=zdst(unit, dev), send_sem=zsend.at[kind, unit],
            recv_sem=zrecv.at[kind, unit], device_id=(partner,), device_id_type=MESH).wait_recv()

    def zstart(unit):
        for kind in (1, 2, 3, 0):
            zcopy(unit, kind).start()

    def zforward(units):
        for kind in (1, 2, 3):
            for unit in units:
                zwait(unit, kind)
                zcopy(unit, kind + 3).start()

    def zfinish(units):
        for unit in units:
            zwait(unit, 0)
        for kind in (4, 5, 6):
            for unit in units:
                zwait(unit, kind)

    def bcast(ref_of, send_sem, recv_sem, wait):
        for off in range(1, DEVS):
            dev = (me + off) % DEVS
            slot = dev if wait else me
            copy = pltpu.make_async_remote_copy(
                src_ref=ref_of(slot), dst_ref=ref_of(slot), send_sem=send_sem(off),
                recv_sem=recv_sem(slot), device_id=(dev,), device_id_type=MESH)
            if wait:
                copy.wait_recv()
            else:
                copy.start()

    def bcast_drain(ref_of, send_sem, recv_sem):
        for off in range(1, DEVS):
            pltpu.make_async_remote_copy(
                src_ref=ref_of(me), dst_ref=ref_of(me), send_sem=send_sem(off),
                recv_sem=recv_sem(me), device_id=((me + off) % DEVS,), device_id_type=MESH).wait_send()

    m_args = (lambda d: mx.at[d], lambda o: psend.at[1, o], lambda d: precv.at[1, d])
    p_args = (lambda d: px.at[d], lambda o: psend.at[0, o], lambda d: precv.at[0, d])
    v_args = (lambda d: vx.at[d], lambda o: vsend.at[o], lambda d: vrecv.at[d])

    def r_args(step):
        return (lambda d: rx.at[step, d], lambda o: rsend.at[step, o], lambda d: rrecv.at[step, d])

    l_args = (lambda d: lx.at[d], lambda o: lsend.at[o], lambda d: lrecv.at[d])

    for copy in own_copies:
        copy.wait()

    mrow = mask_ref[...].astype(F32)
    sel = (lax.broadcasted_iota(jnp.int32, (ROWS, 128), 1)
           == lax.broadcasted_iota(jnp.int32, (ROWS, 128), 0) + ROWS * core)
    mplaced = jnp.dot(jnp.broadcast_to(mrow, (8, ROWS)).astype(BF16), sel.astype(BF16),
                      preferred_element_type=F32)
    mx[me] = mplaced[0:1, :]

    pl.semaphore_wait(barrier, DEVS - 1)
    zstart(0)
    zstart(1)
    bcast(*m_args, wait=False)
    zstart(2)

    def fold(x):
        return jnp.sum(x.reshape(x.shape[0] // 8, 8, x.shape[1]), axis=0)

    def lane_fold(x):
        out = x[:, 0:128]
        for i in range(1, x.shape[1] // 128):
            out = out + x[:, i * 128:(i + 1) * 128]
        return out

    lacc[...] = jnp.zeros_like(lacc)
    for copy in c_copies:
        copy.wait()

    def sum_chunk(ch, carry, keep=False):
        cc = protos_at(pl.ds(pl.multiple_of(ch * PC, PC), PC))
        scores = nt_dot(own_rows(), cc)
        lacc[...] += lane_fold(jnp.exp(scores * (1.0 / TAU)))
        if keep:
            sst[ch - (PROTOS // PC - KEPT)] = scores
        return carry
    def row_sums_out():
        for view in range(VIEWS):
            la = lacc[view * ROWS:(view + 1) * ROWS]
            lx[me, view] = jnp.sum(jnp.concatenate([la, la], axis=0).T, axis=0, keepdims=True)
        bcast(*l_args, wait=False)

    def exp_block(view, ch, base):
        rows = pl.ds(pl.multiple_of(ch * EC, EC), EC)
        scores = nt_dot(protos_at(pl.ds(pl.multiple_of(base + ch * EC, EC), EC)), view_rows(view))
        e = jnp.exp(scores * (1.0 / TAU))
        et[view, rows] = e
        return rows, e

    def exp_views(lo, hi, base=own0):
        def step(view, carry):
            for ch in range(OWN // EC):
                exp_block(view, ch, base)
            return carry
        lax.fori_loop(lo, hi, step, 0)

    lax.fori_loop(0, 6, sum_chunk, 0)
    zforward((0, 1))
    lax.fori_loop(6, 8, sum_chunk, 0)
    bcast(*m_args, wait=True)
    zfinish((0, 1))
    for q in range(NROW // 128):
        mvec[:, q * 128:(q + 1) * 128] = mx[2 * q] + mx[2 * q + 1]
    live_total = jnp.sum(mvec[...], axis=1, keepdims=True)

    SB = 128

    exp_views(0, 2)

    def sink_pass(it):
        scale = (1.0 if it == 0 else live_total) * (1.0 / PROTOS)

        def step(blk, accs):
            rows = pl.ds(pl.multiple_of(blk * SB, SB), SB)
            out = []
            for view in range(2):
                e = et[view, rows]
                a = e * e
                w = mvec[...] if it == 0 else wvec[view]
                colsum = jnp.sum(a * w, axis=1, keepdims=True)
                v = scale / colsum
                if it == ITERS - 1:
                    vb[view, rows] = jnp.broadcast_to(v, (SB, 128))
                out.append(accs[view] + fold(a * v))
            return tuple(out)
        zero = jnp.zeros((8, NROW), F32)
        accs = lax.fori_loop(0, OWN // SB, step, (zero, zero))
        for view in range(2):
            rx[it, me, :, view * NROW:(view + 1) * NROW] = jnp.sum(accs[view], axis=0, keepdims=True)
        bcast(*r_args(it), wait=False)

    def sink_close(it):
        bcast(*r_args(it), wait=True)
        tot = rx[it, 0]
        for d in range(1, DEVS):
            tot = tot + rx[it, d]
        for view in range(2):
            wvec[view] = mvec[...] / tot[:, view * NROW:(view + 1) * NROW]

    sink_pass(0)
    zstart(3)
    lax.fori_loop(PROTOS // PC - KEPT, PROTOS // PC, functools.partial(sum_chunk, keep=True), 0)
    zforward((2,))
    sink_close(0)
    sink_pass(1)
    row_sums_out()
    zstart(4)
    zfinish((2,))
    exp_views(2, 7)
    zforward((3,))
    sink_close(1)
    sink_pass(2)
    bcast(*l_args, wait=True)
    grad_scale = 1.0 / (TAU * live_total * (2 + 2 * (VIEWS - 2)))
    log_sum = jnp.zeros((1, NROW), F32)
    low = lax.broadcasted_iota(jnp.int32, (1, 128), 1) < ROWS
    for view in range(VIEWS):
        tot = jnp.concatenate([jnp.where(low, lx[2 * q, view], lx[2 * q + 1, view])
                               for q in range(NROW // 128)], axis=1)
        mult = 1.0 if view < 2 else 2.0
        acf[view] = (mult * grad_scale) * mvec[...] / tot
        log_sum = log_sum + mult * jnp.log(tot)
    log_sum = jnp.sum(log_sum * mvec[...], axis=1, keepdims=True)
    for view in range(2):
        for blk in range(OWN // 128):
            vt = vb[view, blk * 128:(blk + 1) * 128].T
            vx[me, view, :, blk * 128:(blk + 1) * 128] = vt[0:1, :]
    bcast(*v_args, wait=False)
    zfinish((3,))
    exp_views(7, 10)
    zforward((4,))
    zfinish((4,))
    exp_views(10, 12)
    sink_close(2)

    def rows_of(dev, ch):
        return pl.ds(pl.multiple_of(dev * OWN + ch * KC, KC), KC)

    def acopy(dev, ch, to, kind):
        rows = rows_of(dev, ch)
        return pltpu.make_async_remote_copy(
            src_ref=dcv.at[rows], dst_ref=dcv.at[rows], send_sem=asend.at[kind, ch],
            recv_sem=arecv.at[kind, ch], device_id=(to,), device_id_type=MESH)

    def dc_chunk(dev, ch):
        rows = pl.ds(pl.multiple_of(ch * KC, KC), KC)
        gq = []
        for view in range(2):
            v = jnp.concatenate([vb[view, rows]] * (NROW // 128), axis=1)
            e = et[view, rows]
            gq.append((wvec[view] * grad_scale) * (v * (e * e)))
        sub = [gq[1], gq[0]] + [gq[0] + gq[1]] * (VIEWS - 2)
        acc = None
        for view in range(VIEWS):
            g = (acf[view] * et[view, rows] - sub[view]).astype(BF16)
            part = jnp.dot(g, view_rows(view), preferred_element_type=F32)
            acc = part if acc is None else acc + part
        dcv[rows_of(dev, ch)] = acc

    def dc_own(ch, carry):
        dc_chunk(me, ch)
        acopy(me, ch, xn, 0).start()
        acopy(me, ch, yn, 1).start()
        acopy(me, ch, partner, 2).start()
        return carry
    lax.fori_loop(0, NCH, dc_own, 0)

    def dc_far(ch, carry):
        dc_chunk(dg, ch)
        acopy(dg, ch, partner, 5).start()
        return carry

    def forward(ch):
        for dev, kind in ((xn, 0), (yn, 1)):
            acopy(dev, ch, dev, kind).wait_recv()
            acopy(dev, ch, partner, 3 + kind).start()

    bcast(*v_args, wait=True)
    for view in range(2):
        for blk in range(OWN // 128):
            lanes = slice(blk * 128, (blk + 1) * 128)
            vb[view, lanes] = jnp.broadcast_to(vx[dg, view, :, lanes], (128, 128)).T
    exp_views(0, VIEWS, dg * OWN)
    lax.fori_loop(0, NCH, dc_far, 0)
    forward(0)
    forward(1)

    lanes = pl.ds(pl.multiple_of((me // 2) * 128, 128), 128)
    for view in range(VIEWS):
        cf[view:view + 1, :] = acf[view, :, lanes]
    for view in range(2):
        cf[VIEWS + view:VIEWS + view + 1, :] = wvec[view, :, lanes]
    ct[...] = cf[...].T
    own_cf = ct[pl.ds(pl.multiple_of(core * ROWS, ROWS), ROWS), :]
    for j in range(VIEWS + 2):
        ab[j] = jnp.broadcast_to(own_cf[:, j:j + 1], (ROWS, 128))

    dz_out[...] = jnp.zeros_like(dz_out)

    def row_chunk(ch, acc, kept=False):
        cc = protos_at(pl.ds(pl.multiple_of(ch * PC, PC), PC))
        if not kept:
            scores = nt_dot(own_rows(), cc)

        def score(view, sub):
            rows, lanes = slice(view * ROWS, (view + 1) * ROWS), slice(sub * 128, (sub + 1) * 128)
            return sst[ch - (PROTOS // PC - KEPT), rows, lanes] if kept else scores[rows, lanes]
        dev = ch // (OWN // PC)
        for sub in range(PC // 128):
            lanes = pl.ds(pl.multiple_of((ch % (OWN // PC)) * PC + sub * 128, 128), 128)
            cols = pl.ds(pl.multiple_of(ch * PC + sub * 128, 128), 128)
            s0, s1 = score(0, sub), score(1, sub)
            e0, e1 = jnp.exp(s0 * (1.0 / TAU)), jnp.exp(s1 * (1.0 / TAU))
            q0 = ab[VIEWS] * (vx[dev, 0, :, lanes] * (e0 * e0))
            q1 = ab[VIEWS + 1] * (vx[dev, 1, :, lanes] * (e1 * e1))
            q_out[0, :, cols] = q0
            q_out[1, :, cols] = q1
            gbuf[sub, 0:ROWS] = (ab[0] * e0 - q1 * grad_scale).astype(BF16)
            gbuf[sub, ROWS:2 * ROWS] = (ab[1] * e1 - q0 * grad_scale).astype(BF16)
            cross = q1 * s0 + q0 * s1
            q_sum = q0 + q1
            gq_sum = q_sum * grad_scale
            s_sum = None
            for view in range(2, VIEWS):
                s = score(view, sub)
                s_sum = s if s_sum is None else s_sum + s
                gbuf[sub, view * ROWS:(view + 1) * ROWS] = (
                    ab[view] * jnp.exp(s * (1.0 / TAU)) - gq_sum).astype(BF16)
            acc = acc + fold(cross + q_sum * s_sum)
        g = jnp.concatenate([gbuf[sub] for sub in range(PC // 128)], axis=1)
        dz = jnp.dot(g, cc, preferred_element_type=F32)
        dz_out[...] += dz.reshape(VIEWS, ROWS, DIM)
        return acc
    acc = lax.fori_loop(0, PROTOS // PC - KEPT, row_chunk, jnp.zeros((8, 128), F32))
    forward(2)
    row_kept = functools.partial(row_chunk, kept=True)
    acc = lax.fori_loop(PROTOS // PC - KEPT, PROTOS // PC - 2, row_kept, acc)
    forward(3)
    acc = lax.fori_loop(PROTOS // PC - 2, PROTOS // PC, row_kept, acc)
    cross = jnp.sum(jnp.sum(acc, axis=0, keepdims=True), axis=1, keepdims=True)
    px[me] = jnp.broadcast_to(cross, (1, 128))
    bcast(*p_args, wait=False)

    bcast(*p_args, wait=True)
    tot = px[0]
    for d in range(1, DEVS):
        tot = tot + px[d]
    loss = -(tot[:, 0:1] * (1.0 / TAU) - log_sum) / (live_total * (2 + 2 * (VIEWS - 2)))
    loss_ref[...] = jnp.broadcast_to(loss, (1, 128))

    def drain(ch, carry):
        for kind, dev in ((2, me), (3, xn), (4, yn), (5, dg)):
            acopy(other(dev), ch, partner, kind).wait_recv()
        for kind, dev in ((0, me), (1, me), (2, me), (3, xn), (4, yn), (5, dg)):
            acopy(dev, ch, partner, kind).wait_send()
        return carry
    for unit in range(len(UNITS)):
        for kind in range(7):
            zcopy(unit, kind).wait_send()
    bcast_drain(*m_args)
    bcast_drain(*p_args)
    bcast_drain(*v_args)
    for it in range(ITERS):
        bcast_drain(*r_args(it))
    bcast_drain(*l_args)
    lax.fori_loop(0, NCH, drain, 0)


def write_out(q_ref, loss_in, dz_ref, dc_ref, q1_hbm, q2_hbm, loss_ref, dz1_hbm, dz2_hbm, dzs_hbm, dc_hbm, sem):
    copies = []
    pairs = []
    for i in range(8):
        rows = pl.ds(i * (PROTOS // 8), PROTOS // 8)
        pairs.append((dc_ref.at[rows], dc_hbm.at[rows]))
    for i in range(4):
        rows = pl.ds(i * (ROWS // 4), ROWS // 4)
        pairs.append((q_ref.at[0, rows], q1_hbm.at[rows]))
        pairs.append((q_ref.at[1, rows], q2_hbm.at[rows]))
    pairs += [(dz_ref.at[pl.ds(2, VIEWS - 2)], dzs_hbm), (dz_ref.at[0], dz1_hbm), (dz_ref.at[1], dz2_hbm)]
    for src, dst in pairs:
        copies.append(pltpu.make_async_copy(src, dst, sem.at[len(copies)]))
        copies[-1].start()
    loss_ref[0, 0] = jnp.max(loss_in[:, 0:1])
    for copy in copies:
        copy.wait()


def local_step(z_one, z_two, z_small, protos, live_mask):
    vmem = pl.BlockSpec(memory_space=pltpu.VMEM)
    hbm = pl.BlockSpec(memory_space=pl.ANY)
    dma = pltpu.SemaphoreType.DMA
    views = VIEWS
    staged = pl.pallas_call(
        body,
        out_shape=(
            pltpu.VMEM((2, ROWS, PROTOS), F32),
            pltpu.VMEM((1, 128), F32),
            pltpu.VMEM((views, ROWS, DIM), F32),
            pltpu.VMEM((PROTOS, DIM), F32),
        ),
        in_specs=[hbm] * 5,
        out_specs=(vmem, vmem, vmem, vmem),
        scratch_shapes=[
            pltpu.VMEM((2, views, NROW, 128), BF16),
            pltpu.VMEM((2, views, ROWS, 128), BF16),
            pltpu.VMEM((2, PROTOS, 128), BF16),
            pltpu.VMEM((views, OWN, NROW), F32),
            pltpu.VMEM((KEPT, views * ROWS, PC), F32),
            pltpu.VMEM((2, OWN, 128), F32),
            pltpu.VMEM((DEVS, 2, 1, OWN), F32),
            pltpu.VMEM((ITERS, DEVS, 1, 2 * NROW), F32),
            pltpu.VMEM((DEVS, views, 1, 128), F32),
            pltpu.VMEM((DEVS, 1, 128), F32),
            pltpu.VMEM((DEVS, 1, 128), F32),
            pltpu.VMEM((1, NROW), F32),
            pltpu.VMEM((2, 1, NROW), F32),
            pltpu.VMEM((views, 1, NROW), F32),
            pltpu.VMEM((128, 128), F32),
            pltpu.VMEM((128, 128), F32),
            pltpu.VMEM((views + 2, ROWS, 128), F32),
            pltpu.VMEM((views * ROWS, 128), F32),
            pltpu.VMEM((PC // 128, views * ROWS, 128), BF16),
            pltpu.VMEM((1, ROWS), jnp.int32),
            dma((2,)), dma((13,)),
            dma((7, 5)), dma((7, 5)),
            dma((ITERS, DEVS)), dma((ITERS, DEVS)),
            dma((DEVS,)), dma((DEVS,)),
            dma((DEVS,)), dma((DEVS,)),
            dma((2, DEVS)), dma((2, DEVS)),
            dma((6, NCH)), dma((6, NCH)),
        ],
        compiler_params=pltpu.CompilerParams(
            collective_id=0, has_side_effects=True, vmem_limit_bytes=50 * 1024 * 1024),
        name="swav_step",
    )(live_mask.reshape(1, ROWS), z_one, z_two, z_small, protos)
    q_one, q_two, loss, dz_one, dz_two, dz_small, d_protos = pl.pallas_call(
        write_out,
        out_shape=(
            jax.ShapeDtypeStruct((ROWS, PROTOS), F32),
            jax.ShapeDtypeStruct((ROWS, PROTOS), F32),
            jax.ShapeDtypeStruct((1, 1), F32),
            jax.ShapeDtypeStruct((ROWS, DIM), F32),
            jax.ShapeDtypeStruct((ROWS, DIM), F32),
            jax.ShapeDtypeStruct((views - 2, ROWS, DIM), F32),
            jax.ShapeDtypeStruct((PROTOS, DIM), F32),
        ),
        in_specs=[vmem] * 4,
        out_specs=(hbm, hbm, pl.BlockSpec(memory_space=pltpu.SMEM), hbm, hbm, hbm, hbm),
        scratch_shapes=[dma((19,))],
        compiler_params=pltpu.CompilerParams(vmem_limit_bytes=1024 * 1024),
        name="write_out",
    )(*staged)
    return q_one, q_two, loss[0, 0], dz_one, dz_two, dz_small, d_protos


def solution(mesh):
    row_spec = P("data", None)
    crop_spec = P(None, "data", None)
    return jax.shard_map(local_step, mesh=mesh,
                         in_specs=(row_spec, row_spec, crop_spec, P(None, None), P("data")),
                         out_specs=(row_spec, row_spec, P(), row_spec, row_spec, crop_spec, P(None, None)),
                         check_vma=False)
```

```python
import functools
import math

import jax
import jax.numpy as jnp
from jax import lax
from jax.experimental import pallas as pl
from jax.experimental.pallas import tpu as pltpu
from jax.sharding import PartitionSpec as P

EPS = 0.05
TAU = 0.1
ITERS = 3
DEVS = 8
ROWS = 64
NROW = ROWS * DEVS
PROTOS = 8192
DIM = 256
VIEWS = 12
OWN = PROTOS // DEVS
KC = 256
NCH = OWN // KC
KEPT = 8
PC = 512
MESH = pl.DeviceIdType.MESH
F32 = jnp.float32
BF16 = jnp.bfloat16
UNITS = ((0, 1), (1, 1), (2, 5), (7, 3), (10, 2))
EC = 512


def nt_dot(a, b):
    return lax.dot_general(a, b, (((1,), (1,)), ((), ())), preferred_element_type=F32)


def body(mask_hbm, z1_hbm, z2_hbm, zs_hbm, c_hbm,
         q_out, loss_ref, dz_out, dcv,
         zall, zown, cv, et, sst, vb, vx, rx, lx, mx, px,
         mvec, wvec, acf, cf, ct, ab, lacc,
         mask_ref, csem, isem, zsend, zrecv, rsend, rrecv, lsend, lrecv, vsend, vrecv, psend, precv,
         asend, arecv):
    me = lax.axis_index("data")
    core = me % 2
    xpos = (me // 2) % 2
    ypos = me // 4
    partner = me + 1 - 2 * core
    xn = me + 2 - 4 * xpos
    yn = me + 4 - 8 * ypos
    dg = xn + 4 - 8 * ypos

    def other(d):
        return d + 1 - 2 * core

    my_rows = pl.ds(pl.multiple_of(me * ROWS, ROWS), ROWS)
    small = pl.ds(2, VIEWS - 2)
    own_copies = []
    for h in range(2):
        half = pl.ds(h * 128, 128)
        for src, dst in ((z1_hbm.at[:, half], zown.at[h, 0]),
                         (z2_hbm.at[:, half], zown.at[h, 1]),
                         (zs_hbm.at[:, :, half], zown.at[h, small]),
                         (z1_hbm.at[:, half], zall.at[h, 0, my_rows]),
                         (z2_hbm.at[:, half], zall.at[h, 1, my_rows]),
                         (zs_hbm.at[:, :, half], zall.at[h, small, my_rows])):
            own_copies.append(pltpu.make_async_copy(src, dst, isem.at[len(own_copies)]))
            own_copies[-1].start()
    own0 = pl.multiple_of(me * OWN, OWN)
    own_copies.append(pltpu.make_async_copy(mask_hbm, mask_ref, isem.at[12]))
    own_copies[-1].start()
    c_copies = []
    for h in range(2):
        c_copies.append(pltpu.make_async_copy(c_hbm.at[:, pl.ds(h * 128, 128)], cv.at[h], csem.at[h]))
        c_copies[-1].start()

    def halves(x0, x1):
        return jnp.concatenate([x0, x1], axis=1)

    def protos_at(rows):
        return halves(cv[0, rows], cv[1, rows])

    def view_rows(view):
        return halves(zall[0, view], zall[1, view])

    def own_rows():
        return halves(zown[0].reshape(VIEWS * ROWS, 128), zown[1].reshape(VIEWS * ROWS, 128))

    barrier = pltpu.get_barrier_semaphore()
    for off in range(1, DEVS):
        pl.semaphore_signal(barrier, inc=1, device_id=((me + off) % DEVS,), device_id_type=MESH)

    def zdst(unit, dev):
        lo, cnt = UNITS[unit]
        rows = pl.ds(pl.multiple_of(dev * ROWS, ROWS), ROWS)
        if cnt == 1:
            return zall.at[:, lo, rows]
        return zall.at[:, pl.ds(lo, cnt), rows]

    def zsrc(unit):
        lo, cnt = UNITS[unit]
        return zown.at[:, lo] if cnt == 1 else zown.at[:, pl.ds(lo, cnt)]

    peers = (partner, xn, yn, dg)

    def zcopy(unit, kind):
        if kind < 4:
            return pltpu.make_async_remote_copy(
                src_ref=zsrc(unit), dst_ref=zdst(unit, me), send_sem=zsend.at[kind, unit],
                recv_sem=zrecv.at[kind, unit], device_id=(peers[kind],), device_id_type=MESH)
        dev = peers[kind - 3]
        return pltpu.make_async_remote_copy(
            src_ref=zdst(unit, dev), dst_ref=zdst(unit, dev), send_sem=zsend.at[kind, unit],
            recv_sem=zrecv.at[kind, unit], device_id=(partner,), device_id_type=MESH)

    def zwait(unit, kind):
        dev = peers[kind] if kind < 4 else other(peers[kind - 3])
        pltpu.make_async_remote_copy(
            src_ref=zsrc(unit), dst_ref=zdst(unit, dev), send_sem=zsend.at[kind, unit],
            recv_sem=zrecv.at[kind, unit], device_id=(partner,), device_id_type=MESH).wait_recv()

    def zstart(unit):
        for kind in (1, 2, 3, 0):
            zcopy(unit, kind).start()

    def zforward(units):
        for kind in (1, 2, 3):
            for unit in units:
                zwait(unit, kind)
                zcopy(unit, kind + 3).start()

    def zfinish(units):
        for unit in units:
            zwait(unit, 0)
        for kind in (4, 5, 6):
            for unit in units:
                zwait(unit, kind)

    def bcast(ref_of, send_sem, recv_sem, wait):
        for off in range(1, DEVS):
            dev = (me + off) % DEVS
            slot = dev if wait else me
            copy = pltpu.make_async_remote_copy(
                src_ref=ref_of(slot), dst_ref=ref_of(slot), send_sem=send_sem(off),
                recv_sem=recv_sem(slot), device_id=(dev,), device_id_type=MESH)
            if wait:
                copy.wait_recv()
            else:
                copy.start()

    def bcast_drain(ref_of, send_sem, recv_sem):
        for off in range(1, DEVS):
            pltpu.make_async_remote_copy(
                src_ref=ref_of(me), dst_ref=ref_of(me), send_sem=send_sem(off),
                recv_sem=recv_sem(me), device_id=((me + off) % DEVS,), device_id_type=MESH).wait_send()

    m_args = (lambda d: mx.at[d], lambda o: psend.at[1, o], lambda d: precv.at[1, d])
    p_args = (lambda d: px.at[d], lambda o: psend.at[0, o], lambda d: precv.at[0, d])
    v_args = (lambda d: vx.at[d], lambda o: vsend.at[o], lambda d: vrecv.at[d])

    def r_args(step):
        return (lambda d: rx.at[step, d], lambda o: rsend.at[step, o], lambda d: rrecv.at[step, d])

    l_args = (lambda d: lx.at[d], lambda o: lsend.at[o], lambda d: lrecv.at[d])

    for copy in own_copies:
        copy.wait()

    mrow = mask_ref[...].astype(F32)
    sel = (lax.broadcasted_iota(jnp.int32, (ROWS, 128), 1)
           == lax.broadcasted_iota(jnp.int32, (ROWS, 128), 0) + ROWS * core)
    mplaced = jnp.dot(jnp.broadcast_to(mrow, (8, ROWS)).astype(BF16), sel.astype(BF16),
                      preferred_element_type=F32)
    mx[me] = mplaced[0:1, :]

    pl.semaphore_wait(barrier, DEVS - 1)
    zstart(0)
    zstart(1)
    bcast(*m_args, wait=False)
    zstart(2)

    def fold(x):
        return jnp.sum(x.reshape(x.shape[0] // 8, 8, x.shape[1]), axis=0)

    def lane_fold(x):
        out = x[:, 0:128]
        for i in range(1, x.shape[1] // 128):
            out = out + x[:, i * 128:(i + 1) * 128]
        return out

    lacc[...] = jnp.zeros_like(lacc)
    for copy in c_copies:
        copy.wait()

    def sum_chunk(ch, carry, keep=False):
        cc = protos_at(pl.ds(pl.multiple_of(ch * PC, PC), PC))
        scores = nt_dot(own_rows(), cc)
        lacc[...] += lane_fold(jnp.exp(scores * (1.0 / TAU)))
        if keep:
            sst[ch - (PROTOS // PC - KEPT)] = scores
        return carry
    def row_sums_out():
        for view in range(VIEWS):
            la = lacc[view * ROWS:(view + 1) * ROWS]
            lx[me, view] = jnp.sum(jnp.concatenate([la, la], axis=0).T, axis=0, keepdims=True)
        bcast(*l_args, wait=False)

    def exp_block(view, ch, base):
        rows = pl.ds(pl.multiple_of(ch * EC, EC), EC)
        scores = nt_dot(protos_at(pl.ds(pl.multiple_of(base + ch * EC, EC), EC)), view_rows(view))
        e = jnp.exp(scores * (1.0 / TAU))
        et[view, rows] = e
        return rows, e

    def exp_views(lo, hi, base=own0):
        def step(view, carry):
            for ch in range(OWN // EC):
                exp_block(view, ch, base)
            return carry
        lax.fori_loop(lo, hi, step, 0)

    lax.fori_loop(0, 6, sum_chunk, 0)
    zforward((0, 1))
    lax.fori_loop(6, 8, sum_chunk, 0)
    bcast(*m_args, wait=True)
    zfinish((0, 1))
    for q in range(NROW // 128):
        mvec[:, q * 128:(q + 1) * 128] = mx[2 * q] + mx[2 * q + 1]
    live_total = jnp.sum(mvec[...], axis=1, keepdims=True)

    SB = 128

    exp_views(0, 2)

    def sink_pass(it):
        scale = (1.0 if it == 0 else live_total) * (1.0 / PROTOS)

        def step(blk, accs):
            rows = pl.ds(pl.multiple_of(blk * SB, SB), SB)
            out = []
            for view in range(2):
                e = et[view, rows]
                a = e * e
                w = mvec[...] if it == 0 else wvec[view]
                colsum = jnp.sum(a * w, axis=1, keepdims=True)
                v = scale / colsum
                if it == ITERS - 1:
                    vb[view, rows] = jnp.broadcast_to(v, (SB, 128))
                out.append(accs[view] + fold(a * v))
            return tuple(out)
        zero = jnp.zeros((8, NROW), F32)
        accs = lax.fori_loop(0, OWN // SB, step, (zero, zero))
        for view in range(2):
            rx[it, me, :, view * NROW:(view + 1) * NROW] = jnp.sum(accs[view], axis=0, keepdims=True)
        bcast(*r_args(it), wait=False)

    def sink_close(it):
        bcast(*r_args(it), wait=True)
        tot = rx[it, 0]
        for d in range(1, DEVS):
            tot = tot + rx[it, d]
        for view in range(2):
            wvec[view] = mvec[...] / tot[:, view * NROW:(view + 1) * NROW]

    sink_pass(0)
    zstart(3)
    lax.fori_loop(PROTOS // PC - KEPT, PROTOS // PC, functools.partial(sum_chunk, keep=True), 0)
    zforward((2,))
    sink_close(0)
    sink_pass(1)
    row_sums_out()
    zstart(4)
    zfinish((2,))
    exp_views(2, 7)
    zforward((3,))
    sink_close(1)
    sink_pass(2)
    bcast(*l_args, wait=True)
    grad_scale = 1.0 / (TAU * live_total * (2 + 2 * (VIEWS - 2)))
    log_sum = jnp.zeros((1, NROW), F32)
    low = lax.broadcasted_iota(jnp.int32, (1, 128), 1) < ROWS
    for view in range(VIEWS):
        tot = jnp.concatenate([jnp.where(low, lx[2 * q, view], lx[2 * q + 1, view])
                               for q in range(NROW // 128)], axis=1)
        mult = 1.0 if view < 2 else 2.0
        acf[view] = (mult * grad_scale) * mvec[...] / tot
        log_sum = log_sum + mult * jnp.log(tot)
    log_sum = jnp.sum(log_sum * mvec[...], axis=1, keepdims=True)
    for view in range(2):
        for blk in range(OWN // 128):
            vt = vb[view, blk * 128:(blk + 1) * 128].T
            vx[me, view, :, blk * 128:(blk + 1) * 128] = vt[0:1, :]
    bcast(*v_args, wait=False)
    zfinish((3,))
    exp_views(7, 10)
    zforward((4,))
    zfinish((4,))
    exp_views(10, 12)
    sink_close(2)

    def rows_of(dev, ch):
        return pl.ds(pl.multiple_of(dev * OWN + ch * KC, KC), KC)

    def acopy(dev, ch, to, kind):
        rows = rows_of(dev, ch)
        return pltpu.make_async_remote_copy(
            src_ref=dcv.at[rows], dst_ref=dcv.at[rows], send_sem=asend.at[kind, ch],
            recv_sem=arecv.at[kind, ch], device_id=(to,), device_id_type=MESH)

    def dc_chunk(dev, ch):
        rows = pl.ds(pl.multiple_of(ch * KC, KC), KC)
        gq = []
        for view in range(2):
            v = jnp.concatenate([vb[view, rows]] * (NROW // 128), axis=1)
            e = et[view, rows]
            gq.append((wvec[view] * grad_scale) * (v * (e * e)))
        sub = [gq[1], gq[0]] + [gq[0] + gq[1]] * (VIEWS - 2)
        acc = None
        for view in range(VIEWS):
            g = (acf[view] * et[view, rows] - sub[view]).astype(BF16)
            part = jnp.dot(g, view_rows(view), preferred_element_type=F32)
            acc = part if acc is None else acc + part
        dcv[rows_of(dev, ch)] = acc

    def dc_own(ch, carry):
        dc_chunk(me, ch)
        acopy(me, ch, xn, 0).start()
        acopy(me, ch, yn, 1).start()
        acopy(me, ch, partner, 2).start()
        return carry
    lax.fori_loop(0, NCH, dc_own, 0)

    def dc_far(ch, carry):
        dc_chunk(dg, ch)
        acopy(dg, ch, partner, 5).start()
        return carry

    def forward(ch):
        for dev, kind in ((xn, 0), (yn, 1)):
            acopy(dev, ch, dev, kind).wait_recv()
            acopy(dev, ch, partner, 3 + kind).start()

    bcast(*v_args, wait=True)

    lanes = pl.ds(pl.multiple_of((me // 2) * 128, 128), 128)
    for view in range(VIEWS):
        cf[view:view + 1, :] = acf[view, :, lanes]
    for view in range(2):
        cf[VIEWS + view:VIEWS + view + 1, :] = wvec[view, :, lanes]
    ct[...] = cf[...].T
    own_cf = ct[pl.ds(pl.multiple_of(core * ROWS, ROWS), ROWS), :]
    for j in range(VIEWS + 2):
        ab[j] = jnp.broadcast_to(own_cf[:, j:j + 1], (ROWS, 128))

    dz_out[...] = jnp.zeros_like(dz_out)

    def wide(x):
        return jnp.concatenate([x] * (PC // 128), axis=1)

    def row_chunk(ch, acc, kept=False):
        cols = pl.ds(pl.multiple_of(ch * PC, PC), PC)
        cc = protos_at(pl.ds(pl.multiple_of(ch * PC, PC), PC))
        if kept:
            def score(view):
                return sst[ch - (PROTOS // PC - KEPT), view * ROWS:(view + 1) * ROWS]
        else:
            scores = nt_dot(own_rows(), cc)

            def score(view):
                return scores[view * ROWS:(view + 1) * ROWS]
        dev = ch // (OWN // PC)
        half = pl.ds(pl.multiple_of((ch % (OWN // PC)) * PC, PC), PC)
        e_large, q_large = [], []
        for view in range(2):
            e = jnp.exp(score(view) * (1.0 / TAU))
            q = wide(ab[VIEWS + view]) * (vx[dev, view, :, half] * (e * e))
            q_out[view, :, cols] = q
            e_large.append(e)
            q_large.append(q)
        q_sum = q_large[0] + q_large[1]
        gq_sum = q_sum * grad_scale
        parts = [(wide(ab[0]) * e_large[0] - q_large[1] * grad_scale).astype(BF16),
                 (wide(ab[1]) * e_large[1] - q_large[0] * grad_scale).astype(BF16)]
        s_sum = None
        for view in range(2, VIEWS):
            s = score(view)
            s_sum = s if s_sum is None else s_sum + s
            parts.append((wide(ab[view]) * jnp.exp(s * (1.0 / TAU)) - gq_sum).astype(BF16))
        dot = q_large[1] * score(0) + q_large[0] * score(1) + q_sum * s_sum
        dz = jnp.dot(jnp.concatenate(parts, axis=0), cc, preferred_element_type=F32)
        dz_out[...] += dz.reshape(VIEWS, ROWS, DIM)
        return acc + fold(dot)
    acc = lax.fori_loop(0, PROTOS // PC - KEPT, row_chunk, jnp.zeros((8, PC), F32))
    row_kept = functools.partial(row_chunk, kept=True)
    acc = lax.fori_loop(PROTOS // PC - KEPT, PROTOS // PC, row_kept, acc)
    cross = jnp.sum(jnp.sum(acc, axis=0, keepdims=True), axis=1, keepdims=True)
    px[me] = jnp.broadcast_to(cross, (1, 128))
    bcast(*p_args, wait=False)
    forward(0)
    for view in range(2):
        for blk in range(OWN // 128):
            lanes = slice(blk * 128, (blk + 1) * 128)
            vb[view, lanes] = jnp.broadcast_to(vx[dg, view, :, lanes], (128, 128)).T
    exp_views(0, VIEWS, dg * OWN)
    forward(1)
    lax.fori_loop(0, 2, dc_far, 0)
    forward(2)
    lax.fori_loop(2, NCH, dc_far, 0)
    forward(3)


    bcast(*p_args, wait=True)
    tot = px[0]
    for d in range(1, DEVS):
        tot = tot + px[d]
    loss = -(tot[:, 0:1] * (1.0 / TAU) - log_sum) / (live_total * (2 + 2 * (VIEWS - 2)))
    loss_ref[...] = jnp.broadcast_to(loss, (1, 128))

    def drain(ch, carry):
        for kind, dev in ((2, me), (3, xn), (4, yn), (5, dg)):
            acopy(other(dev), ch, partner, kind).wait_recv()
        for kind, dev in ((0, me), (1, me), (2, me), (3, xn), (4, yn), (5, dg)):
            acopy(dev, ch, partner, kind).wait_send()
        return carry
    for unit in range(len(UNITS)):
        for kind in range(7):
            zcopy(unit, kind).wait_send()
    bcast_drain(*m_args)
    bcast_drain(*p_args)
    bcast_drain(*v_args)
    for it in range(ITERS):
        bcast_drain(*r_args(it))
    bcast_drain(*l_args)
    lax.fori_loop(0, NCH, drain, 0)


def write_out(q_ref, loss_in, dz_ref, dc_ref, q1_hbm, q2_hbm, loss_ref, dz1_hbm, dz2_hbm, dzs_hbm, dc_hbm, sem):
    copies = []
    pairs = []
    for i in range(8):
        rows = pl.ds(i * (PROTOS // 8), PROTOS // 8)
        pairs.append((dc_ref.at[rows], dc_hbm.at[rows]))
    for i in range(4):
        rows = pl.ds(i * (ROWS // 4), ROWS // 4)
        pairs.append((q_ref.at[0, rows], q1_hbm.at[rows]))
        pairs.append((q_ref.at[1, rows], q2_hbm.at[rows]))
    pairs += [(dz_ref.at[pl.ds(2, VIEWS - 2)], dzs_hbm), (dz_ref.at[0], dz1_hbm), (dz_ref.at[1], dz2_hbm)]
    for src, dst in pairs:
        copies.append(pltpu.make_async_copy(src, dst, sem.at[len(copies)]))
        copies[-1].start()
    loss_ref[0, 0] = jnp.max(loss_in[:, 0:1])
    for copy in copies:
        copy.wait()


def local_step(z_one, z_two, z_small, protos, live_mask):
    vmem = pl.BlockSpec(memory_space=pltpu.VMEM)
    hbm = pl.BlockSpec(memory_space=pl.ANY)
    dma = pltpu.SemaphoreType.DMA
    views = VIEWS
    staged = pl.pallas_call(
        body,
        out_shape=(
            pltpu.VMEM((2, ROWS, PROTOS), F32),
            pltpu.VMEM((1, 128), F32),
            pltpu.VMEM((views, ROWS, DIM), F32),
            pltpu.VMEM((PROTOS, DIM), F32),
        ),
        in_specs=[hbm] * 5,
        out_specs=(vmem, vmem, vmem, vmem),
        scratch_shapes=[
            pltpu.VMEM((2, views, NROW, 128), BF16),
            pltpu.VMEM((2, views, ROWS, 128), BF16),
            pltpu.VMEM((2, PROTOS, 128), BF16),
            pltpu.VMEM((views, OWN, NROW), F32),
            pltpu.VMEM((KEPT, views * ROWS, PC), F32),
            pltpu.VMEM((2, OWN, 128), F32),
            pltpu.VMEM((DEVS, 2, 1, OWN), F32),
            pltpu.VMEM((ITERS, DEVS, 1, 2 * NROW), F32),
            pltpu.VMEM((DEVS, views, 1, 128), F32),
            pltpu.VMEM((DEVS, 1, 128), F32),
            pltpu.VMEM((DEVS, 1, 128), F32),
            pltpu.VMEM((1, NROW), F32),
            pltpu.VMEM((2, 1, NROW), F32),
            pltpu.VMEM((views, 1, NROW), F32),
            pltpu.VMEM((128, 128), F32),
            pltpu.VMEM((128, 128), F32),
            pltpu.VMEM((views + 2, ROWS, 128), F32),
            pltpu.VMEM((views * ROWS, 128), F32),
            pltpu.VMEM((1, ROWS), jnp.int32),
            dma((2,)), dma((13,)),
            dma((7, 5)), dma((7, 5)),
            dma((ITERS, DEVS)), dma((ITERS, DEVS)),
            dma((DEVS,)), dma((DEVS,)),
            dma((DEVS,)), dma((DEVS,)),
            dma((2, DEVS)), dma((2, DEVS)),
            dma((6, NCH)), dma((6, NCH)),
        ],
        compiler_params=pltpu.CompilerParams(
            collective_id=0, has_side_effects=True, vmem_limit_bytes=50 * 1024 * 1024),
        name="swav_step",
    )(live_mask.reshape(1, ROWS), z_one, z_two, z_small, protos)
    q_one, q_two, loss, dz_one, dz_two, dz_small, d_protos = pl.pallas_call(
        write_out,
        out_shape=(
            jax.ShapeDtypeStruct((ROWS, PROTOS), F32),
            jax.ShapeDtypeStruct((ROWS, PROTOS), F32),
            jax.ShapeDtypeStruct((1, 1), F32),
            jax.ShapeDtypeStruct((ROWS, DIM), F32),
            jax.ShapeDtypeStruct((ROWS, DIM), F32),
            jax.ShapeDtypeStruct((views - 2, ROWS, DIM), F32),
            jax.ShapeDtypeStruct((PROTOS, DIM), F32),
        ),
        in_specs=[vmem] * 4,
        out_specs=(hbm, hbm, pl.BlockSpec(memory_space=pltpu.SMEM), hbm, hbm, hbm, hbm),
        scratch_shapes=[dma((19,))],
        compiler_params=pltpu.CompilerParams(vmem_limit_bytes=1024 * 1024),
        name="write_out",
    )(*staged)
    return q_one, q_two, loss[0, 0], dz_one, dz_two, dz_small, d_protos


def solution(mesh):
    row_spec = P("data", None)
    crop_spec = P(None, "data", None)
    return jax.shard_map(local_step, mesh=mesh,
                         in_specs=(row_spec, row_spec, crop_spec, P(None, None), P("data")),
                         out_specs=(row_spec, row_spec, P(), row_spec, row_spec, crop_spec, P(None, None)),
                         check_vma=False)
```

```python
import functools
import math

import jax
import jax.numpy as jnp
from jax import lax
from jax.experimental import pallas as pl
from jax.experimental.pallas import tpu as pltpu
from jax.sharding import PartitionSpec as P

EPS = 0.05
TAU = 0.1
ITERS = 3
DEVS = 8
ROWS = 64
NROW = ROWS * DEVS
PROTOS = 8192
DIM = 256
VIEWS = 12
OWN = PROTOS // DEVS
KC = 256
NCH = OWN // KC
KEPT = 10
PC = 512
MESH = pl.DeviceIdType.MESH
F32 = jnp.float32
BF16 = jnp.bfloat16
UNITS = ((0, 1), (1, 1), (2, 5), (7, 3), (10, 2))
EC = 512


def nt_dot(a, b):
    return lax.dot_general(a, b, (((1,), (1,)), ((), ())), preferred_element_type=F32)


def body(mask_hbm, z1_hbm, z2_hbm, zs_hbm, c_hbm,
         q_out, loss_ref, dz_out, dcv,
         zall, zown, cv, et, sst, vb, vx, rx, lx, mx, px,
         mvec, wvec, acf, cf, ct, ab, lacc,
         mask_ref, csem, isem, zsend, zrecv, rsend, rrecv, lsend, lrecv, vsend, vrecv, psend, precv,
         asend, arecv):
    me = lax.axis_index("data")
    core = me % 2
    xpos = (me // 2) % 2
    ypos = me // 4
    partner = me + 1 - 2 * core
    xn = me + 2 - 4 * xpos
    yn = me + 4 - 8 * ypos
    dg = xn + 4 - 8 * ypos

    def other(d):
        return d + 1 - 2 * core

    my_rows = pl.ds(pl.multiple_of(me * ROWS, ROWS), ROWS)
    small = pl.ds(2, VIEWS - 2)
    own_copies = []
    for h in range(2):
        half = pl.ds(h * 128, 128)
        for src, dst in ((z1_hbm.at[:, half], zown.at[h, 0]),
                         (z2_hbm.at[:, half], zown.at[h, 1]),
                         (zs_hbm.at[:, :, half], zown.at[h, small]),
                         (z1_hbm.at[:, half], zall.at[h, 0, my_rows]),
                         (z2_hbm.at[:, half], zall.at[h, 1, my_rows]),
                         (zs_hbm.at[:, :, half], zall.at[h, small, my_rows])):
            own_copies.append(pltpu.make_async_copy(src, dst, isem.at[len(own_copies)]))
            own_copies[-1].start()
    own0 = pl.multiple_of(me * OWN, OWN)
    own_copies.append(pltpu.make_async_copy(mask_hbm, mask_ref, isem.at[12]))
    own_copies[-1].start()
    c_copies = []
    for h in range(2):
        c_copies.append(pltpu.make_async_copy(c_hbm.at[:, pl.ds(h * 128, 128)], cv.at[h], csem.at[h]))
        c_copies[-1].start()

    def halves(x0, x1):
        return jnp.concatenate([x0, x1], axis=1)

    def protos_at(rows):
        return halves(cv[0, rows], cv[1, rows])

    def view_rows(view):
        return halves(zall[0, view], zall[1, view])

    def own_rows():
        return halves(zown[0].reshape(VIEWS * ROWS, 128), zown[1].reshape(VIEWS * ROWS, 128))

    barrier = pltpu.get_barrier_semaphore()
    for off in range(1, DEVS):
        pl.semaphore_signal(barrier, inc=1, device_id=((me + off) % DEVS,), device_id_type=MESH)

    def zdst(unit, dev):
        lo, cnt = UNITS[unit]
        rows = pl.ds(pl.multiple_of(dev * ROWS, ROWS), ROWS)
        if cnt == 1:
            return zall.at[:, lo, rows]
        return zall.at[:, pl.ds(lo, cnt), rows]

    def zsrc(unit):
        lo, cnt = UNITS[unit]
        return zown.at[:, lo] if cnt == 1 else zown.at[:, pl.ds(lo, cnt)]

    peers = (partner, xn, yn, dg)

    def zcopy(unit, kind):
        if kind < 4:
            return pltpu.make_async_remote_copy(
                src_ref=zsrc(unit), dst_ref=zdst(unit, me), send_sem=zsend.at[kind, unit],
                recv_sem=zrecv.at[kind, unit], device_id=(peers[kind],), device_id_type=MESH)
        dev = peers[kind - 3]
        return pltpu.make_async_remote_copy(
            src_ref=zdst(unit, dev), dst_ref=zdst(unit, dev), send_sem=zsend.at[kind, unit],
            recv_sem=zrecv.at[kind, unit], device_id=(partner,), device_id_type=MESH)

    def zwait(unit, kind):
        dev = peers[kind] if kind < 4 else other(peers[kind - 3])
        pltpu.make_async_remote_copy(
            src_ref=zsrc(unit), dst_ref=zdst(unit, dev), send_sem=zsend.at[kind, unit],
            recv_sem=zrecv.at[kind, unit], device_id=(partner,), device_id_type=MESH).wait_recv()

    def zstart(unit):
        for kind in (1, 2, 3, 0):
            zcopy(unit, kind).start()

    def zforward(units):
        for kind in (1, 2, 3):
            for unit in units:
                zwait(unit, kind)
                zcopy(unit, kind + 3).start()

    def zfinish(units):
        for unit in units:
            zwait(unit, 0)
        for kind in (4, 5, 6):
            for unit in units:
                zwait(unit, kind)

    def bcast(ref_of, send_sem, recv_sem, wait):
        for off in range(1, DEVS):
            dev = (me + off) % DEVS
            slot = dev if wait else me
            copy = pltpu.make_async_remote_copy(
                src_ref=ref_of(slot), dst_ref=ref_of(slot), send_sem=send_sem(off),
                recv_sem=recv_sem(slot), device_id=(dev,), device_id_type=MESH)
            if wait:
                copy.wait_recv()
            else:
                copy.start()

    def bcast_drain(ref_of, send_sem, recv_sem):
        for off in range(1, DEVS):
            pltpu.make_async_remote_copy(
                src_ref=ref_of(me), dst_ref=ref_of(me), send_sem=send_sem(off),
                recv_sem=recv_sem(me), device_id=((me + off) % DEVS,), device_id_type=MESH).wait_send()

    m_args = (lambda d: mx.at[d], lambda o: psend.at[1, o], lambda d: precv.at[1, d])
    p_args = (lambda d: px.at[d], lambda o: psend.at[0, o], lambda d: precv.at[0, d])
    v_args = (lambda d: vx.at[d], lambda o: vsend.at[o], lambda d: vrecv.at[d])

    def r_args(step):
        return (lambda d: rx.at[step, d], lambda o: rsend.at[step, o], lambda d: rrecv.at[step, d])

    l_args = (lambda d: lx.at[d], lambda o: lsend.at[o], lambda d: lrecv.at[d])

    for copy in own_copies:
        copy.wait()

    mrow = mask_ref[...].astype(F32)
    sel = (lax.broadcasted_iota(jnp.int32, (ROWS, 128), 1)
           == lax.broadcasted_iota(jnp.int32, (ROWS, 128), 0) + ROWS * core)
    mplaced = jnp.dot(jnp.broadcast_to(mrow, (8, ROWS)).astype(BF16), sel.astype(BF16),
                      preferred_element_type=F32)
    mx[me] = mplaced[0:1, :]

    pl.semaphore_wait(barrier, DEVS - 1)
    zstart(0)
    zstart(1)
    bcast(*m_args, wait=False)
    zstart(2)

    def fold(x):
        return jnp.sum(x.reshape(x.shape[0] // 8, 8, x.shape[1]), axis=0)

    def lane_fold(x):
        out = x[:, 0:128]
        for i in range(1, x.shape[1] // 128):
            out = out + x[:, i * 128:(i + 1) * 128]
        return out

    lacc[...] = jnp.zeros_like(lacc)
    for copy in c_copies:
        copy.wait()

    def sum_chunk(ch, carry, keep=False):
        cc = protos_at(pl.ds(pl.multiple_of(ch * PC, PC), PC))
        scores = nt_dot(own_rows(), cc)
        lacc[...] += lane_fold(jnp.exp(scores * (1.0 / TAU)))
        if keep:
            sst[ch - (PROTOS // PC - KEPT)] = scores
        return carry
    def row_sums_out():
        for view in range(VIEWS):
            la = lacc[view * ROWS:(view + 1) * ROWS]
            lx[me, view] = jnp.sum(jnp.concatenate([la, la], axis=0).T, axis=0, keepdims=True)
        bcast(*l_args, wait=False)

    def exp_block(view, ch, base):
        rows = pl.ds(pl.multiple_of(ch * EC, EC), EC)
        scores = nt_dot(protos_at(pl.ds(pl.multiple_of(base + ch * EC, EC), EC)), view_rows(view))
        e = jnp.exp(scores * (1.0 / TAU))
        et[view, rows] = e
        return rows, e

    def exp_views(lo, hi, base=own0):
        def step(view, carry):
            for ch in range(OWN // EC):
                exp_block(view, ch, base)
            return carry
        lax.fori_loop(lo, hi, step, 0)

    lax.fori_loop(0, 6, sum_chunk, 0)
    zforward((0, 1))
    lax.fori_loop(6, 8, functools.partial(sum_chunk, keep=True), 0)
    bcast(*m_args, wait=True)
    zfinish((0, 1))
    for q in range(NROW // 128):
        mvec[:, q * 128:(q + 1) * 128] = mx[2 * q] + mx[2 * q + 1]
    live_total = jnp.sum(mvec[...], axis=1, keepdims=True)

    SB = 128

    exp_views(0, 2)

    def sink_pass(it):
        scale = (1.0 if it == 0 else live_total) * (1.0 / PROTOS)

        def step(blk, accs):
            rows = pl.ds(pl.multiple_of(blk * SB, SB), SB)
            out = []
            for view in range(2):
                e = et[view, rows]
                a = e * e
                w = mvec[...] if it == 0 else wvec[view]
                colsum = jnp.sum(a * w, axis=1, keepdims=True)
                v = scale / colsum
                if it == ITERS - 1:
                    vb[view, rows] = jnp.broadcast_to(v, (SB, 128))
                out.append(accs[view] + fold(a * v))
            return tuple(out)
        zero = jnp.zeros((8, NROW), F32)
        accs = lax.fori_loop(0, OWN // SB, step, (zero, zero))
        for view in range(2):
            rx[it, me, :, view * NROW:(view + 1) * NROW] = jnp.sum(accs[view], axis=0, keepdims=True)
        bcast(*r_args(it), wait=False)

    def sink_close(it):
        bcast(*r_args(it), wait=True)
        tot = rx[it, 0]
        for d in range(1, DEVS):
            tot = tot + rx[it, d]
        for view in range(2):
            wvec[view] = mvec[...] / tot[:, view * NROW:(view + 1) * NROW]

    sink_pass(0)
    zstart(3)
    lax.fori_loop(8, PROTOS // PC, functools.partial(sum_chunk, keep=True), 0)
    zforward((2,))
    sink_close(0)
    sink_pass(1)
    row_sums_out()
    zstart(4)
    zfinish((2,))
    exp_views(2, 7)
    zforward((3,))
    sink_close(1)
    sink_pass(2)
    bcast(*l_args, wait=True)
    grad_scale = 1.0 / (TAU * live_total * (2 + 2 * (VIEWS - 2)))
    log_sum = jnp.zeros((1, NROW), F32)
    low = lax.broadcasted_iota(jnp.int32, (1, 128), 1) < ROWS
    for view in range(VIEWS):
        tot = jnp.concatenate([jnp.where(low, lx[2 * q, view], lx[2 * q + 1, view])
                               for q in range(NROW // 128)], axis=1)
        mult = 1.0 if view < 2 else 2.0
        acf[view] = (mult * grad_scale) * mvec[...] / tot
        log_sum = log_sum + mult * jnp.log(tot)
    log_sum = jnp.sum(log_sum * mvec[...], axis=1, keepdims=True)
    for view in range(2):
        for blk in range(OWN // 128):
            vt = vb[view, blk * 128:(blk + 1) * 128].T
            vx[me, view, :, blk * 128:(blk + 1) * 128] = vt[0:1, :]
    bcast(*v_args, wait=False)
    zfinish((3,))
    exp_views(7, 10)
    zforward((4,))
    zfinish((4,))
    exp_views(10, 12)
    sink_close(2)

    def rows_of(dev, ch):
        return pl.ds(pl.multiple_of(dev * OWN + ch * KC, KC), KC)

    def acopy(dev, ch, to, kind):
        rows = rows_of(dev, ch)
        return pltpu.make_async_remote_copy(
            src_ref=dcv.at[rows], dst_ref=dcv.at[rows], send_sem=asend.at[kind, ch],
            recv_sem=arecv.at[kind, ch], device_id=(to,), device_id_type=MESH)

    def dc_chunk(dev, ch):
        rows = pl.ds(pl.multiple_of(ch * KC, KC), KC)
        gq = []
        for view in range(2):
            v = jnp.concatenate([vb[view, rows]] * (NROW // 128), axis=1)
            e = et[view, rows]
            gq.append((wvec[view] * grad_scale) * (v * (e * e)))
        sub = [gq[1], gq[0]] + [gq[0] + gq[1]] * (VIEWS - 2)
        acc = None
        for view in range(VIEWS):
            g = (acf[view] * et[view, rows] - sub[view]).astype(BF16)
            part = jnp.dot(g, view_rows(view), preferred_element_type=F32)
            acc = part if acc is None else acc + part
        dcv[rows_of(dev, ch)] = acc

    def dc_own(ch, carry):
        dc_chunk(me, ch)
        acopy(me, ch, xn, 0).start()
        acopy(me, ch, yn, 1).start()
        acopy(me, ch, partner, 2).start()
        return carry
    lax.fori_loop(0, NCH, dc_own, 0)

    def dc_far(ch, carry):
        dc_chunk(dg, ch)
        acopy(dg, ch, partner, 5).start()
        return carry

    def forward(ch):
        for dev, kind in ((xn, 0), (yn, 1)):
            acopy(dev, ch, dev, kind).wait_recv()
            acopy(dev, ch, partner, 3 + kind).start()

    bcast(*v_args, wait=True)

    lanes = pl.ds(pl.multiple_of((me // 2) * 128, 128), 128)
    for view in range(VIEWS):
        cf[view:view + 1, :] = acf[view, :, lanes]
    for view in range(2):
        cf[VIEWS + view:VIEWS + view + 1, :] = wvec[view, :, lanes]
    ct[...] = cf[...].T
    own_cf = ct[pl.ds(pl.multiple_of(core * ROWS, ROWS), ROWS), :]
    for j in range(VIEWS + 2):
        ab[j] = jnp.broadcast_to(own_cf[:, j:j + 1], (ROWS, 128))

    dz_out[...] = jnp.zeros_like(dz_out)

    def wide(x):
        return jnp.concatenate([x] * (PC // 128), axis=1)

    def row_chunk(ch, acc, kept=False):
        cols = pl.ds(pl.multiple_of(ch * PC, PC), PC)
        cc = protos_at(pl.ds(pl.multiple_of(ch * PC, PC), PC))
        if kept:
            def score(view):
                return sst[ch - (PROTOS // PC - KEPT), view * ROWS:(view + 1) * ROWS]
        else:
            scores = nt_dot(own_rows(), cc)

            def score(view):
                return scores[view * ROWS:(view + 1) * ROWS]
        dev = ch // (OWN // PC)
        half = pl.ds(pl.multiple_of((ch % (OWN // PC)) * PC, PC), PC)
        e_large, q_large = [], []
        for view in range(2):
            e = jnp.exp(score(view) * (1.0 / TAU))
            q = wide(ab[VIEWS + view]) * (vx[dev, view, :, half] * (e * e))
            q_out[view, :, cols] = q
            e_large.append(e)
            q_large.append(q)
        q_sum = q_large[0] + q_large[1]
        gq_sum = q_sum * grad_scale
        parts = [(wide(ab[0]) * e_large[0] - q_large[1] * grad_scale).astype(BF16),
                 (wide(ab[1]) * e_large[1] - q_large[0] * grad_scale).astype(BF16)]
        s_sum = None
        for view in range(2, VIEWS):
            s = score(view)
            s_sum = s if s_sum is None else s_sum + s
            parts.append((wide(ab[view]) * jnp.exp(s * (1.0 / TAU)) - gq_sum).astype(BF16))
        dot = q_large[1] * score(0) + q_large[0] * score(1) + q_sum * s_sum
        dz = jnp.dot(jnp.concatenate(parts, axis=0), cc, preferred_element_type=F32)
        dz_out[...] += dz.reshape(VIEWS, ROWS, DIM)
        return acc + fold(dot)
    acc = lax.fori_loop(0, PROTOS // PC - KEPT, row_chunk, jnp.zeros((8, PC), F32))
    row_kept = functools.partial(row_chunk, kept=True)
    acc = lax.fori_loop(PROTOS // PC - KEPT, PROTOS // PC, row_kept, acc)
    cross = jnp.sum(jnp.sum(acc, axis=0, keepdims=True), axis=1, keepdims=True)
    px[me] = jnp.broadcast_to(cross, (1, 128))
    bcast(*p_args, wait=False)
    forward(0)
    for view in range(2):
        for blk in range(OWN // 128):
            lanes = slice(blk * 128, (blk + 1) * 128)
            vb[view, lanes] = jnp.broadcast_to(vx[dg, view, :, lanes], (128, 128)).T
    exp_views(0, VIEWS, dg * OWN)
    forward(1)
    lax.fori_loop(0, 2, dc_far, 0)
    forward(2)
    lax.fori_loop(2, NCH, dc_far, 0)
    forward(3)


    bcast(*p_args, wait=True)
    tot = px[0]
    for d in range(1, DEVS):
        tot = tot + px[d]
    loss = -(tot[:, 0:1] * (1.0 / TAU) - log_sum) / (live_total * (2 + 2 * (VIEWS - 2)))
    loss_ref[...] = jnp.broadcast_to(loss, (1, 128))

    def drain(ch, carry):
        for kind, dev in ((2, me), (3, xn), (4, yn), (5, dg)):
            acopy(other(dev), ch, partner, kind).wait_recv()
        for kind, dev in ((0, me), (1, me), (2, me), (3, xn), (4, yn), (5, dg)):
            acopy(dev, ch, partner, kind).wait_send()
        return carry
    for unit in range(len(UNITS)):
        for kind in range(7):
            zcopy(unit, kind).wait_send()
    bcast_drain(*m_args)
    bcast_drain(*p_args)
    bcast_drain(*v_args)
    for it in range(ITERS):
        bcast_drain(*r_args(it))
    bcast_drain(*l_args)
    lax.fori_loop(0, NCH, drain, 0)


def write_out(q_ref, loss_in, dz_ref, dc_ref, q1_hbm, q2_hbm, loss_ref, dz1_hbm, dz2_hbm, dzs_hbm, dc_hbm, sem):
    copies = []
    pairs = []
    for i in range(8):
        rows = pl.ds(i * (PROTOS // 8), PROTOS // 8)
        pairs.append((dc_ref.at[rows], dc_hbm.at[rows]))
    for i in range(4):
        rows = pl.ds(i * (ROWS // 4), ROWS // 4)
        pairs.append((q_ref.at[0, rows], q1_hbm.at[rows]))
        pairs.append((q_ref.at[1, rows], q2_hbm.at[rows]))
    pairs += [(dz_ref.at[pl.ds(2, VIEWS - 2)], dzs_hbm), (dz_ref.at[0], dz1_hbm), (dz_ref.at[1], dz2_hbm)]
    for src, dst in pairs:
        copies.append(pltpu.make_async_copy(src, dst, sem.at[len(copies)]))
        copies[-1].start()
    loss_ref[0, 0] = jnp.max(loss_in[:, 0:1])
    for copy in copies:
        copy.wait()


def local_step(z_one, z_two, z_small, protos, live_mask):
    vmem = pl.BlockSpec(memory_space=pltpu.VMEM)
    hbm = pl.BlockSpec(memory_space=pl.ANY)
    dma = pltpu.SemaphoreType.DMA
    views = VIEWS
    staged = pl.pallas_call(
        body,
        out_shape=(
            pltpu.VMEM((2, ROWS, PROTOS), F32),
            pltpu.VMEM((1, 128), F32),
            pltpu.VMEM((views, ROWS, DIM), F32),
            pltpu.VMEM((PROTOS, DIM), F32),
        ),
        in_specs=[hbm] * 5,
        out_specs=(vmem, vmem, vmem, vmem),
        scratch_shapes=[
            pltpu.VMEM((2, views, NROW, 128), BF16),
            pltpu.VMEM((2, views, ROWS, 128), BF16),
            pltpu.VMEM((2, PROTOS, 128), BF16),
            pltpu.VMEM((views, OWN, NROW), F32),
            pltpu.VMEM((KEPT, views * ROWS, PC), F32),
            pltpu.VMEM((2, OWN, 128), F32),
            pltpu.VMEM((DEVS, 2, 1, OWN), F32),
            pltpu.VMEM((ITERS, DEVS, 1, 2 * NROW), F32),
            pltpu.VMEM((DEVS, views, 1, 128), F32),
            pltpu.VMEM((DEVS, 1, 128), F32),
            pltpu.VMEM((DEVS, 1, 128), F32),
            pltpu.VMEM((1, NROW), F32),
            pltpu.VMEM((2, 1, NROW), F32),
            pltpu.VMEM((views, 1, NROW), F32),
            pltpu.VMEM((128, 128), F32),
            pltpu.VMEM((128, 128), F32),
            pltpu.VMEM((views + 2, ROWS, 128), F32),
            pltpu.VMEM((views * ROWS, 128), F32),
            pltpu.VMEM((1, ROWS), jnp.int32),
            dma((2,)), dma((13,)),
            dma((7, 5)), dma((7, 5)),
            dma((ITERS, DEVS)), dma((ITERS, DEVS)),
            dma((DEVS,)), dma((DEVS,)),
            dma((DEVS,)), dma((DEVS,)),
            dma((2, DEVS)), dma((2, DEVS)),
            dma((6, NCH)), dma((6, NCH)),
        ],
        compiler_params=pltpu.CompilerParams(
            collective_id=0, has_side_effects=True, vmem_limit_bytes=51 * 1024 * 1024),
        name="swav_step",
    )(live_mask.reshape(1, ROWS), z_one, z_two, z_small, protos)
    q_one, q_two, loss, dz_one, dz_two, dz_small, d_protos = pl.pallas_call(
        write_out,
        out_shape=(
            jax.ShapeDtypeStruct((ROWS, PROTOS), F32),
            jax.ShapeDtypeStruct((ROWS, PROTOS), F32),
            jax.ShapeDtypeStruct((1, 1), F32),
            jax.ShapeDtypeStruct((ROWS, DIM), F32),
            jax.ShapeDtypeStruct((ROWS, DIM), F32),
            jax.ShapeDtypeStruct((views - 2, ROWS, DIM), F32),
            jax.ShapeDtypeStruct((PROTOS, DIM), F32),
        ),
        in_specs=[vmem] * 4,
        out_specs=(hbm, hbm, pl.BlockSpec(memory_space=pltpu.SMEM), hbm, hbm, hbm, hbm),
        scratch_shapes=[dma((19,))],
        compiler_params=pltpu.CompilerParams(vmem_limit_bytes=1024 * 1024),
        name="write_out",
    )(*staged)
    return q_one, q_two, loss[0, 0], dz_one, dz_two, dz_small, d_protos


def solution(mesh):
    row_spec = P("data", None)
    crop_spec = P(None, "data", None)
    return jax.shard_map(local_step, mesh=mesh,
                         in_specs=(row_spec, row_spec, crop_spec, P(None, None), P("data")),
                         out_specs=(row_spec, row_spec, P(), row_spec, row_spec, crop_spec, P(None, None)),
                         check_vma=False)
```
